512 devices in a mesh: cfg: 2 (over y), ta: 8 (over x), gz: 16 (over z), gy: 2 (over core).
Axes of the slice: x: 8, y: 2, z: 16, core: 2. Of those that a mesh axis runs over, the one named last changes fastest.
The devices are a block of a 8x8x16 slice.
Arguments:
- spatial_links: float32 [6, 2, 3, 3, 16, 16, 16, 128], P('cfg', None, None, None, 'ta', 'gz', 'gy'), parts along dimension 0, may hold values from -1 to 1, as said below
- time_links: float32 [4, 3, 3, 16, 16, 16, 128], P('cfg', None, None, 'ta', 'gz', 'gy'), parts along dimension 0, may hold values from -1 to 1, as said below
Outputs:
- polyakov: float32 [4, 16, 16, 128], P('cfg', 'gz', 'gy'), parts along dimension 0
- site_mean: float32 [4], P('cfg'), parts along dimension 0
The draws below stay inside these ranges and needn't reach their ends.
There are 2 independent parts, one for each index of `cfg`. The reference program is written for one: setup_inputs(seed, part) draws one part's arguments, and reference() takes and returns one part's arrays. A program takes and returns all parts, laid end to end along the dimension named above; each array names one. Nothing has to cross between parts.
Inputs may be any that keep to these rules, and one draw needn't show every extreme that they name: `spatial_links`: every 3x3 complex matrix (real part at index 0, imaginary at index 1 of its part dimension) is Proj, as defined in the reference program, of some complex matrix; it is special unitary where both of its first two rows had a squared norm of 0.25 or more before their division, and need not be elsewhere. `time_links`: every 3x3 complex matrix (real part at index 0, imaginary at index 1 of its part dimension) is Proj, as defined in the reference program, of some complex matrix; it is special unitary where both of its first two rows had a squared norm of 0.25 or more before their division, and need not be elsewhere.
All inputs are finite; a program needn't handle non-finite values.
Results may differ from the reference program's by a relative error of at most 0.0003.
Values sent between devices are 32-bit elements; how exact they have to be, the bound alone decides.
A program may use at most 64 MiB of HBM per device.

```python
from functools import partial
import jax
import jax.numpy as jnp
from jax import lax

NX = 128
ITERS = 3
NT = 16
NZ = 16
NY = 16


norm_floor = 0.25


def normalize_row_drawn(row_vec):
    weight = jnp.sum(row_vec[0] * row_vec[0] + row_vec[1] * row_vec[1], axis=0)
    return row_vec / jnp.sqrt(jnp.maximum(weight, norm_floor))


def project_drawn(matrix):
    first = normalize_row_drawn(matrix[:, 0])
    second_raw = matrix[:, 1]
    inner_re = jnp.sum(first[0] * second_raw[0] + first[1] * second_raw[1], axis=0)
    inner_im = jnp.sum(first[0] * second_raw[1] - first[1] * second_raw[0], axis=0)
    ortho = jnp.stack([second_raw[0] - (inner_re * first[0] - inner_im * first[1]), second_raw[1] - (inner_re * first[1] + inner_im * first[0])])
    second = normalize_row_drawn(ortho)
    first_one = jnp.roll(first, -1, axis=1)
    first_two = jnp.roll(first, -2, axis=1)
    second_one = jnp.roll(second, -1, axis=1)
    second_two = jnp.roll(second, -2, axis=1)
    cross_re = first_one[0] * second_two[0] - first_one[1] * second_two[1] - (first_two[0] * second_one[0] - first_two[1] * second_one[1])
    cross_im = first_one[0] * second_two[1] + first_one[1] * second_two[0] - (first_two[0] * second_one[1] + first_two[1] * second_one[0])
    third = jnp.stack([cross_re, -cross_im])
    return jnp.stack([first, second, third], axis=1)


def link_draw(key, leading):
    count_lead = len(leading)
    site_shape = (NT, NZ, NY, NX)
    full_shape = leading + (2, 3, 3) + site_shape
    key_noise = jax.random.fold_in(key, 1)
    key_spread = jax.random.fold_in(key, 2)
    z_share = (jnp.arange(NZ, dtype=jnp.float32) / NZ)[:, None, None]
    noise_part = jax.random.normal(key_noise, full_shape, jnp.float32)
    scale_z = 0.08 + 0.3 * z_share
    spread = jax.random.uniform(key_spread, leading + site_shape, jnp.float32, 0.5, 1.5)
    strength = jnp.expand_dims(scale_z * spread, (count_lead, count_lead + 1, count_lead + 2))
    unit_mat = jnp.stack([jnp.eye(3, dtype=jnp.float32), jnp.zeros((3, 3), jnp.float32)])
    unit_mat = unit_mat.reshape((1,) * count_lead + (2, 3, 3, 1, 1, 1, 1))
    matrix = unit_mat + strength * noise_part
    if count_lead:
        matrix = jnp.moveaxis(matrix, 0, -1)
        matrix = project_drawn(matrix)
        return jnp.moveaxis(matrix, -1, 0)
    return project_drawn(matrix)


def draw_spatial_links(key, part):
    return link_draw(jax.random.fold_in(key, 11), (3,))


def draw_time_links(key, part):
    return link_draw(jax.random.fold_in(key, 23), ())


def setup_inputs(seed: int = 0, part: int = 0) -> dict:
    arg_keys = jax.random.split(jax.random.key(seed), 3)
    part_splits = jax.random.split(jax.random.fold_in(arg_keys[2], part), 3)
    return {
        "spatial_links": draw_spatial_links(jax.random.fold_in(jax.random.fold_in(arg_keys[2], part), 71), part),
        "time_links": draw_time_links(jax.random.fold_in(jax.random.fold_in(arg_keys[2], part), 71), part),
    }


smear_weight = 0.5
norm_floor = 0.25
unit_steps = ((1, 0, 0), (0, 1, 0), (0, 0, 1))

def mat_product(lhs_mat, rhs_mat):
    lhs_re = lhs_mat[0][:, :, None]
    lhs_im = lhs_mat[1][:, :, None]
    rhs_re = rhs_mat[0][None]
    rhs_im = rhs_mat[1][None]
    real_part = lax.optimization_barrier(jnp.sum(lhs_re * rhs_re - lhs_im * rhs_im, axis=1))
    imag_part = lax.optimization_barrier(jnp.sum(lhs_re * rhs_im + lhs_im * rhs_re, axis=1))
    return jnp.stack([real_part, imag_part])

def dagger(matrix):
    return jnp.stack([jnp.swapaxes(matrix[0], 0, 1), -jnp.swapaxes(matrix[1], 0, 1)])

def normalize_row(row_vec):
    weight = lax.optimization_barrier(jnp.sum(row_vec[0] * row_vec[0] + row_vec[1] * row_vec[1], axis=0))
    return row_vec / jnp.sqrt(jnp.maximum(weight, norm_floor))

def project(matrix):
    first = normalize_row(matrix[:, 0])
    second_raw = matrix[:, 1]
    inner_re = lax.optimization_barrier(jnp.sum(first[0] * second_raw[0] + first[1] * second_raw[1], axis=0))
    inner_im = lax.optimization_barrier(jnp.sum(first[0] * second_raw[1] - first[1] * second_raw[0], axis=0))
    ortho = jnp.stack([second_raw[0] - (inner_re * first[0] - inner_im * first[1]), second_raw[1] - (inner_re * first[1] + inner_im * first[0])])
    second = normalize_row(ortho)
    first_one = jnp.roll(first, -1, axis=1)
    first_two = jnp.roll(first, -2, axis=1)
    second_one = jnp.roll(second, -1, axis=1)
    second_two = jnp.roll(second, -2, axis=1)
    cross_re = first_one[0] * second_two[0] - first_one[1] * second_two[1] - (first_two[0] * second_one[0] - first_two[1] * second_one[1])
    cross_im = first_one[0] * second_two[1] + first_one[1] * second_two[0] - (first_two[0] * second_one[1] + first_two[1] * second_one[0])
    third = jnp.stack([cross_re, -cross_im])
    return jnp.stack([first, second, third], axis=1)

def moved(offset, unit_vec, factor):
    return (offset[0] + factor * unit_vec[0], offset[1] + factor * unit_vec[1], offset[2] + factor * unit_vec[2])

def smear_spatial(neighbour):
    anchor = (0, 0, 0)
    result = []
    for mu_dir in range(3):
        staples = None
        for nu_dir in range(3):
            if nu_dir == mu_dir:
                continue
            forward = unit_steps[nu_dir]
            sideways = unit_steps[mu_dir]
            upper_staple = mat_product(mat_product(neighbour(nu_dir, anchor), neighbour(mu_dir, forward)), dagger(neighbour(nu_dir, sideways)))
            back_offset = moved(anchor, forward, -1)
            lower_staple = mat_product(mat_product(dagger(neighbour(nu_dir, back_offset)), neighbour(mu_dir, back_offset)), neighbour(nu_dir, moved(back_offset, sideways, 1)))
            if staples is None:
                staples = upper_staple + lower_staple
            else:
                staples = staples + upper_staple + lower_staple
        mixed_link = (1.0 - smear_weight) * neighbour(mu_dir, anchor) + smear_weight / 4.0 * staples
        result.append(project(mixed_link))
    return jnp.stack(result)

def smear_time(neighbour):
    anchor = (0, 0, 0)
    staples = None
    for nu_dir in range(3):
        forward = unit_steps[nu_dir]
        upper_staple = mat_product(mat_product(neighbour(nu_dir, anchor, 0), neighbour(3, forward, 0)), dagger(neighbour(nu_dir, anchor, 1)))
        back_offset = moved(anchor, forward, -1)
        lower_staple = mat_product(mat_product(dagger(neighbour(nu_dir, back_offset, 0)), neighbour(3, back_offset, 0)), neighbour(nu_dir, back_offset, 1))
        if staples is None:
            staples = upper_staple + lower_staple
        else:
            staples = staples + upper_staple + lower_staple
    mixed_link = (1.0 - smear_weight) * neighbour(3, anchor, 0) + smear_weight / 6.0 * staples
    return project(mixed_link)

def periodic(field, offset):
    return jnp.roll(field, (-offset[2], -offset[1], -offset[0]), axis=(-3, -2, -1))

def slice_neighbour(field, direction, offset):
    return periodic(field[direction], offset)

def time_neighbour(here_links, ahead_links, time_slice, direction, offset, later):
    if direction == 3:
        return periodic(time_slice, offset)
    if later:
        return periodic(ahead_links[direction], offset)
    return periodic(here_links[direction], offset)

def smear_slice(link_slice):
    for sweep_index in range(ITERS):
        current = link_slice
        link_slice = smear_spatial(partial(slice_neighbour, current))
    return link_slice

def smooth_slice(packed):
    return smear_time(partial(time_neighbour, packed[0], packed[1], packed[2]))

def reference(spatial_links, time_links):
    smeared = lax.map(smear_slice, jnp.moveaxis(spatial_links, 4, 0))
    following = jnp.roll(smeared, -1, axis=0)
    time_major = jnp.moveaxis(time_links, 3, 0)
    smoothed = lax.map(smooth_slice, (smeared, following, time_major))
    shape_rest = smoothed.shape[4:]
    unit_mat = jnp.stack([jnp.broadcast_to(jnp.eye(3, dtype=time_links.dtype)[:, :, None, None, None], (3, 3) + shape_rest), jnp.zeros((3, 3) + shape_rest, time_links.dtype)])

    def advance(carry, link_now):
        return (mat_product(carry, link_now), None)
    whole_prod, unused = lax.scan(advance, unit_mat, smoothed)
    polyakov = jnp.stack([whole_prod[0, 0, 0] + whole_prod[0, 1, 1] + whole_prod[0, 2, 2], whole_prod[1, 0, 0] + whole_prod[1, 1, 1] + whole_prod[1, 2, 2]]) / 3.0
    site_mean = lax.optimization_barrier(jnp.mean(polyakov, axis=(1, 2, 3)))
    return (polyakov, site_mean)
```

```python
import functools

import jax
import jax.numpy as jnp
from jax import lax
from jax.experimental import pallas as pl
from jax.experimental.pallas import tpu as pltpu
from jax.sharding import PartitionSpec as P

MESH = pl.DeviceIdType.MESH
F32 = jnp.float32
STEPS = 3
FLOOR = 0.25
FX, FY, FZ, FV = 0, 1, 2, 3


def third_row(m):
    (a_re, b_re), (a_im, b_im) = m[0][:2], m[1][:2]
    re, im = [], []
    for k in range(3):
        p, q = (k + 1) % 3, (k + 2) % 3
        re.append(
            a_re[p] * b_re[q] - a_im[p] * b_im[q] - (a_re[q] * b_re[p] - a_im[q] * b_im[p])
        )
        im.append(
            (a_re[q] * b_im[p] + a_im[q] * b_re[p]) - (a_re[p] * b_im[q] + a_im[p] * b_re[q])
        )
    return [m[0][0], m[0][1], re], [m[1][0], m[1][1], im]


def load(ref, lead, rows, count=3):
    return tuple(
        [[ref[(*lead, part, i, j, rows)] for j in range(3)] for i in range(count)]
        for part in range(2)
    )


def load2(ref, lead, rows):
    return third_row(load(ref, lead, rows, 2))


def store(ref, lead, rows, m):
    for part in range(2):
        for i, row in enumerate(m[part]):
            for j, v in enumerate(row):
                ref[(*lead, part, i, j, rows)] = v


def mapped(fn, *ms):
    return tuple(
        [[fn(*vs) for vs in zip(*rows)] for rows in zip(*[m[part] for m in ms])]
        for part in range(2)
    )


def add(*ms):
    return mapped(lambda *vs: functools.reduce(lambda a, b: a + b, vs), *ms)


def ahead_x(m):
    return mapped(lambda v: pltpu.roll(v, v.shape[-1] - 1, 1), m)


def back_x(m):
    return mapped(lambda v: pltpu.roll(v, 1, 1), m)


def mul(a, b, da=False, db=False, rows=3):
    out_re, out_im = [], []
    for i in range(rows):
        row_re, row_im = [], []
        for k in range(3):
            re = im = None
            for j in range(3):
                ar, ai = (a[0][j][i], a[1][j][i]) if da else (a[0][i][j], a[1][i][j])
                br, bi = (b[0][k][j], b[1][k][j]) if db else (b[0][j][k], b[1][j][k])
                rr, ii, ri, ir = ar * br, ai * bi, ar * bi, ai * br
                tr = rr + ii if da != db else rr - ii
                if da and db:
                    ti = -(ri + ir)
                elif da:
                    ti = ri - ir
                elif db:
                    ti = ir - ri
                else:
                    ti = ri + ir
                re = tr if re is None else re + tr
                im = ti if im is None else im + ti
            row_re.append(re)
            row_im.append(im)
        out_re.append(row_re)
        out_im.append(row_im)
    return out_re, out_im


def normalized(re, im):
    weight = sum(v * v for v in re) + sum(v * v for v in im)
    scale = lax.rsqrt(jnp.maximum(weight, FLOOR))
    return [v * scale for v in re], [v * scale for v in im]


def project(re, im):
    u_re, u_im = normalized(re[0], im[0])
    in_re = sum(u_re[j] * re[1][j] + u_im[j] * im[1][j] for j in range(3))
    in_im = sum(u_re[j] * im[1][j] - u_im[j] * re[1][j] for j in range(3))
    w_re = [re[1][j] - (in_re * u_re[j] - in_im * u_im[j]) for j in range(3)]
    w_im = [im[1][j] - (in_re * u_im[j] + in_im * u_re[j]) for j in range(3)]
    v_re, v_im = normalized(w_re, w_im)
    return third_row(([u_re, v_re], [u_im, v_im]))


def mixed(link, staples, weight):
    re = [[0.5 * link[0][i][j] + weight * staples[0][i][j] for j in range(3)] for i in range(2)]
    im = [[0.5 * link[1][i][j] + weight * staples[1][i][j] for j in range(3)] for i in range(2)]
    return project(re, im)


def kernel(
    ta, gz, half,
    sp, tl, pol, mean,
    F, T, H, TH, UP, S, L, AB, M, sm, ar, tree, pb, bc, zs,
    local_sem, send_sem, recv_sem, out_sem,
):
    j, z, h = lax.axis_index("ta"), lax.axis_index("gz"), lax.axis_index("gy")
    o = 1 - h
    zp, zm = lax.rem(z + 1, gz), lax.rem(z + gz - 1, gz)
    full = 2 * half
    nd = 2 * ta
    own = full // nd
    me = 2 * j + h
    mine = pl.ds(pl.multiple_of(h * half, half), half)
    halves = [pl.ds(k * half, half) for k in range(2)]

    sent = []
    n_sem = [0, 0]

    def remote(src, dst, recv_index, **where):
        k = n_sem[0]
        n_sem[0] += 1
        copy = pltpu.make_async_remote_copy(
            src_ref=src, dst_ref=dst, send_sem=send_sem.at[k], recv_sem=recv_sem.at[recv_index],
            device_id=where, device_id_type=MESH,
        )
        copy.start()
        sent.append(copy)

    def arrived(dst, recv_index):
        pltpu.make_async_remote_copy(
            src_ref=dst, dst_ref=dst, send_sem=send_sem.at[0], recv_sem=recv_sem.at[recv_index],
            device_id={"gy": o}, device_id_type=MESH,
        ).wait_recv()

    def new_recv(n=1):
        k = n_sem[1]
        n_sem[1] += n
        return k

    near = [
        pltpu.make_async_copy(sp.at[:, :, :, :, h, 0], F.at[0, 0:3, :, :, :, mine], local_sem.at[0]),
        pltpu.make_async_copy(tl.at[:, :, :, h, 0], T.at[:, :, :, mine], local_sem.at[1]),
    ]
    for copy in near:
        copy.start()

    barrier = pltpu.get_barrier_semaphore()
    count = 0
    for k in range(1, nd):
        d = lax.rem(me + k, nd)
        pl.semaphore_signal(
            barrier, inc=1, device_id={"ta": d // 2, "gy": lax.rem(d, 2)}, device_id_type=MESH
        )
        count += 1
    for k in range(1, gz):
        pl.semaphore_signal(
            barrier, inc=1, device_id={"gz": lax.rem(z + k, gz)}, device_id_type=MESH
        )
        count += 1
    for k in sorted({1 % gz, (gz - 1) % gz}):
        pl.semaphore_signal(
            barrier, inc=1, device_id={"gz": lax.rem(z + k, gz), "gy": o}, device_id_type=MESH
        )
        count += 1
    pl.semaphore_wait(barrier, count)

    r_v, r_x, r_y, r_t = new_recv(2), new_recv(4), new_recv(4), new_recv(4)
    r_own, r_ownt = new_recv(), new_recv()

    def plane(f, t):
        return sp.at[f, :, 0:2, :, t, 0] if f is not None else tl.at[:, 0:2, :, t, 0]

    def two(ref, *lead):
        return ref.at[(*lead, slice(None), slice(0, 2), slice(None), mine)]

    for t in range(2):
        remote(plane(FZ, t), two(F, 0, FV), r_v + h, gz=zp, gy=t)
    remote(sp.at[:, :, :, :, o, 0], F.at[0, 0:3, :, :, :, mine], r_own, gy=o)
    for f, r in ((FX, r_x), (FY, r_y)):
        for t in range(2):
            remote(plane(f, t), two(H, 0, 0, f), r + h, gz=zm, gy=t)
            remote(plane(f, t), two(H, 0, 1, f), r + 2 + h, gz=zp, gy=t)
    remote(tl.at[:, :, :, o, 0], T.at[:, :, :, mine], r_ownt, gy=o)
    for t in range(2):
        remote(plane(None, t), two(TH, 0), r_t + h, gz=zm, gy=t)
        remote(plane(None, t), two(TH, 1), r_t + 2 + h, gz=zp, gy=t)

    def each_half(body):
        def run(k, carry):
            r0 = pl.multiple_of(k * half, half)
            body(pl.ds(r0, half), pl.ds(r0 + 1, half))
            return carry

        lax.fori_loop(0, 2, run, 0)

    def wrap(ref, *lead):
        ref[(*lead, slice(None), slice(None), slice(None), pl.ds(full, 1))] = ref[
            (*lead, slice(None), slice(None), slice(None), pl.ds(0, 1))
        ]

    def unwrap(k):
        L[k, :, :, :, pl.ds(0, 1)] = L[k, :, :, :, pl.ds(full, 1)]

    def in_plane(s):
        def body(rows, up):
            ux, uy = load(F, (s, FX), rows), load(F, (s, FY), rows)
            uy_x, ux_y = ahead_x(uy), load(F, (s, FX), up)
            c, d = mul(ux, uy_x), mul(uy, ux_y)
            store(S, (FX,), rows, mul(d, uy_x, db=True, rows=2))
            store(L, (0,), up, mul(uy, c, da=True, rows=2))
            store(
                S, (FY,), rows,
                add(mul(c, ux_y, db=True, rows=2), back_x(mul(ux, d, da=True, rows=2))),
            )

        each_half(body)
        unwrap(0)

    def side(ref, s, f, rows, up):
        return ahead_x(load(ref, (s, f), rows)) if up is None else load(ref, (s, f), up)

    def across(s, f):
        def body(rows, up):
            up = None if f == FX else up
            uz, uz_f = load(F, (s, FZ), rows), side(F, s, FZ, rows, up)
            a = mul(uz, load2(H, (s, 0, f), rows))
            store(AB, (0,), rows, a)
            total = add(load(S, (f,), rows, 2), mul(a, uz_f, db=True, rows=2))
            uv, uv_f = load(F, (s, FV), rows), side(F, s, FV, rows, up)
            b = mul(load2(H, (s, 1, f), rows), uv_f)
            store(AB, (1,), rows, b)
            total = add(total, mul(uv, b, da=True, rows=2))
            if f == FX:
                total = add(total, load(L, (0,), rows, 2))
            store(F, (s + 1, f), rows, mixed(load(F, (s, f), rows, 2), total, 0.125))

        each_half(body)

    def z_staples(s, f):
        def body(rows, up):
            shift = None if f == FX else up
            uf = load(F, (s, f), rows)
            b = mul(uf, side(F, s, FZ, rows, shift), rows=2)
            upper = mul(b, load2(H, (s, 0, f), rows), db=True, rows=2)
            lower = mul(uf, load(AB, (0,), rows), da=True, rows=2)
            below = load2(H, (s, 1, f), rows)
            v_upper = mul(load(AB, (1,), rows), uf, db=True, rows=2)
            v_lower = mul(mul(below, load(F, (s, FV), rows), da=True, rows=2), uf, rows=2)
            if f == FX:
                store(S, (FZ,), rows, add(upper, back_x(lower)))
                store(S, (FV,), rows, add(v_upper, back_x(v_lower)))
            else:
                store(L, (1,), up, lower)
                store(L, (2,), up, v_lower)
                store(S, (FZ,), rows, add(load(S, (FZ,), rows, 2), upper))
                store(S, (FV,), rows, add(load(S, (FV,), rows, 2), v_upper))

        each_half(body)
        if f == FY:
            unwrap(1)
            unwrap(2)

    def z_links(s):
        def body(rows, up):
            for f, k in ((FZ, 1), (FV, 2)):
                total = add(load(S, (f,), rows, 2), load(L, (k,), rows, 2))
                store(F, (s + 1, f), rows, mixed(load(F, (s, f), rows, 2), total, 0.125))

        each_half(body)
        wrap(F, s + 1, FZ)
        wrap(F, s + 1, FV)

    for copy in near:
        copy.wait()
    other = pl.ds(pl.multiple_of(o * half, half), half)
    arrived(F.at[0, 0:3, :, :, :, other], r_own)
    wrap(F, 0, FX)
    wrap(F, 0, FZ)
    in_plane(0)
    for k in range(2):
        arrived(F.at[0, FV, :, 0:2, :, halves[k]], r_v + k)

    def complete(rows, up):
        store(F, (0, FV), rows, load2(F, (0, FV), rows))

    each_half(complete)
    wrap(F, 0, FV)

    r_next = new_recv(4)

    def onward(s, f):
        remote(
            F.at[s, f, :, 0:2, :, 0:full], UP.at[f], r_next + f,
            ta=lax.rem(j + h + ta - 1, ta), gy=o,
        )

    for s in range(STEPS):
        last = s == STEPS - 1
        sems = {}
        for f in (FX, FY):
            if s == 0:
                for side_k in range(2):
                    for k in range(2):
                        arrived(
                            H.at[0, side_k, f, :, :, :, halves[k]],
                            (r_x, r_y)[f] + 2 * side_k + k,
                        )
            else:
                for side_k in range(2):
                    arrived(H.at[s, side_k, f], r_now[f] + side_k)
            across(s, f)
            if f == FX:
                wrap(F, s + 1, FX)
            if last:
                onward(s + 1, f)
            else:
                sems[f] = new_recv(2)
                out = F.at[s + 1, f, :, 0:2, :, 0:full]
                remote(out, H.at[s + 1, 0, f], sems[f], gz=zm)
                remote(out, H.at[s + 1, 1, f], sems[f] + 1, gz=zp)
            z_staples(s, f)
        r_now = sems
        z_links(s)
        if last:
            onward(s + 1, FZ)
            onward(s + 1, FV)
        else:
            in_plane(s + 1)

    n = STEPS
    arrived(T.at[:, :, :, other], r_ownt)
    wrap(T)
    for side_k in range(2):
        for k in range(2):
            arrived(TH.at[side_k, :, :, :, halves[k]], r_t + 2 * side_k + k)

    def before(rows, up):
        t = load(T, (), rows)
        ux, uy = load(F, (n, FX), rows), load(F, (n, FY), rows)
        store(M, (0,), rows, mul(ux, ahead_x(t), rows=2))
        store(M, (1,), rows, mul(ux, t, da=True, rows=2))
        store(M, (2,), rows, mul(uy, load(T, (), up), rows=2))
        store(M, (3,), rows, mul(uy, t, da=True, rows=2))
        store(M, (4,), rows, mul(load(F, (n, FZ), rows), load2(TH, (0,), rows), rows=2))
        store(
            M, (5,), rows, mul(load(F, (n, FV), rows), load2(TH, (1,), rows), da=True, rows=2)
        )

    each_half(before)
    arrived(UP.at[FX], r_next + FX)
    arrived(UP.at[FY], r_next + FY)

    def along_xy(rows, up):
        ux, uy = load2(UP, (FX,), rows), load2(UP, (FY,), rows)
        total = add(
            mul(load(M, (0,), rows, 2), ux, db=True, rows=2),
            back_x(mul(load(M, (1,), rows, 2), ux, rows=2)),
            mul(load(M, (2,), rows, 2), uy, db=True, rows=2),
        )
        store(S, (0,), rows, total)
        store(L, (0,), up, mul(load(M, (3,), rows, 2), uy, rows=2))

    each_half(along_xy)
    unwrap(0)
    arrived(UP.at[FZ], r_next + FZ)
    arrived(UP.at[FV], r_next + FV)

    def finish(k, carry):
        r0 = pl.multiple_of(k * half, half)
        rows = pl.ds(r0, half)
        uz, uv = load2(UP, (FZ,), rows), load2(UP, (FV,), rows)
        total = add(
            load(S, (0,), rows, 2),
            load(L, (0,), rows, 2),
            mul(load(M, (4,), rows, 2), uz, db=True, rows=2),
            mul(load(M, (5,), rows, 2), uv, rows=2),
        )
        done = mixed(load(T, (), rows, 2), total, 0.5 / 6.0)
        for part in range(2):
            for a in range(2):
                for b in range(3):
                    sm[pl.ds(r0 * 16 + part * 6 + a * 3 + b, half, 16), :] = done[part][a][b]
        return carry

    lax.fori_loop(0, 2, finish, 0)

    span = own * 16
    r_row = new_recv(nd)
    here = pl.ds(pl.multiple_of(me * span, 8), span)
    for k in range(1, nd):
        d = lax.rem(me + k, nd)
        remote(
            sm.at[pl.ds(pl.multiple_of(d * span, 8), span)], ar.at[here], r_row + me,
            ta=d // 2, gy=lax.rem(d, 2),
        )
    ar[here, :] = sm[here, :]
    for k in range(1, nd):
        d = lax.rem(me + k, nd)
        arrived(ar.at[pl.ds(pl.multiple_of(d * span, 8), span)], r_row + d)

    def slices(start, stride, rows):
        at = lambda c: ar[pl.ds(start + c, rows, stride), :]
        return third_row(
            tuple([[at(part * 6 + a * 3 + b) for b in range(3)] for a in range(2)] for part in range(2))
        )

    for row in range(own):
        rows = nd // 2
        lhs, rhs = slices(row * 16, 2 * span, rows), slices(row * 16 + span, 2 * span, rows)
        while rows > 1:
            prod = mul(lhs, rhs)
            flat = [v for part in prod for line in part for v in line]
            for c, v in enumerate(flat):
                tree[pl.ds(c * 8, rows), :] = v
            rows //= 2
            pick = lambda first: [tree[pl.ds(c * 8 + first, rows, 2), :] for c in range(18)]
            grid = lambda vs: tuple(
                [[vs[part * 9 + a * 3 + b] for b in range(3)] for a in range(3)] for part in range(2)
            )
            lhs, rhs = grid(pick(0)), grid(pick(1))
        re = im = None
        for a in range(3):
            for b in range(3):
                lr, li, rr, ri = lhs[0][a][b], lhs[1][a][b], rhs[0][b][a], rhs[1][b][a]
                t_re, t_im = lr * rr - li * ri, lr * ri + li * rr
                re = t_re if re is None else re + t_re
                im = t_im if im is None else im + t_im
        pb[row, 0:1, :] = re / 3.0
        pb[row, 1:2, :] = im / 3.0

    r_out = new_recv(nd)
    home = pl.ds(me * own, own)
    for k in range(1, nd):
        d = lax.rem(me + k, nd)
        remote(pb, bc.at[home], r_out + me, ta=d // 2, gy=lax.rem(d, 2))
    bc[home] = pb[...]
    for k in range(1, nd):
        d = lax.rem(me + k, nd)
        arrived(bc.at[pl.ds(d * own, own)], r_out + d)

    sums = jnp.sum(bc[...], axis=0)
    zs[z] = sums
    r_sum = new_recv(gz)
    for k in range(1, gz):
        remote(zs.at[z], zs.at[z], r_sum + z, gz=lax.rem(z + k, gz))
    for k in range(half):
        pol[:, 0, k, :] = bc[h * half + k]
    for k in range(1, gz):
        d = lax.rem(z + k, gz)
        arrived(zs.at[d], r_sum + d)
    totals = jnp.sum(zs[...], axis=0)
    sites = float(full * gz * sp.shape[-1])
    for part in range(2):
        mean[part] = jnp.sum(totals[part : part + 1, :]) / sites

    for copy in sent:
        copy.wait_send()


def solution(mesh):
    ta, gz = mesh.shape["ta"], mesh.shape["gz"]

    def body(sp, tl):
        half, lanes = sp.shape[-2:]
        full = 2 * half
        pad = full + 8
        nd = 2 * ta
        own = full // nd

        def vmem(*dims):
            return pltpu.VMEM((*dims, lanes), F32)

        n_send = 2 + 1 + 8 + 1 + 4 + 4 * (STEPS - 1) + 4 + 2 * (nd - 1) + gz - 1
        n_recv = 2 + 4 + 4 + 4 + 2 + 4 + 4 * (STEPS - 1) + 2 * nd + gz
        return pl.pallas_call(
            functools.partial(kernel, ta, gz, half),
            out_shape=(
                jax.ShapeDtypeStruct((2, 1, half, lanes), F32),
                jax.ShapeDtypeStruct((2,), F32),
            ),
            in_specs=[pl.BlockSpec(memory_space=pl.ANY)] * 2,
            out_specs=(
                pl.BlockSpec(memory_space=pltpu.VMEM),
                pl.BlockSpec(memory_space=pltpu.SMEM),
            ),
            scratch_shapes=[
                vmem(STEPS + 1, 4, 2, 3, 3, pad),
                vmem(2, 3, 3, pad),
                vmem(STEPS, 2, 2, 2, 2, 3, full),
                vmem(2, 2, 2, 3, full),
                vmem(4, 2, 2, 3, full),
                vmem(4, 2, 2, 3, full),
                vmem(3, 2, 2, 3, pad),
                vmem(2, 2, 3, 3, full),
                vmem(6, 2, 2, 3, full),
                vmem(full * 16),
                vmem(full * 16),
                vmem(18 * 8),
                vmem(own, 2),
                vmem(full, 2),
                vmem(gz, 2),
                pltpu.SemaphoreType.DMA((2,)),
                pltpu.SemaphoreType.DMA((n_send,)),
                pltpu.SemaphoreType.DMA((n_recv,)),
                pltpu.SemaphoreType.DMA,
            ],
            compiler_params=pltpu.CompilerParams(
                collective_id=0, has_side_effects=True, vmem_limit_bytes=32 * 1024 * 1024
            ),
        )(sp, tl)

    return jax.shard_map(
        body,
        mesh=mesh,
        in_specs=(
            P("cfg", None, None, None, "ta", "gz", "gy", None),
            P("cfg", None, None, "ta", "gz", "gy", None),
        ),
        out_specs=(P("cfg", "gz", "gy", None), P("cfg")),
        check_vma=False,
    )
```

```python
import functools

import jax
import jax.numpy as jnp
from jax import lax
from jax.experimental import pallas as pl
from jax.experimental.pallas import tpu as pltpu
from jax.sharding import PartitionSpec as P

MESH = pl.DeviceIdType.MESH
F32 = jnp.float32
STEPS = 3
FLOOR = 0.25
FX, FY, FZ, FV = 0, 1, 2, 3


def third_row(m):
    (a_re, b_re), (a_im, b_im) = m[0][:2], m[1][:2]
    re, im = [], []
    for k in range(3):
        p, q = (k + 1) % 3, (k + 2) % 3
        re.append(
            a_re[p] * b_re[q] - a_im[p] * b_im[q] - (a_re[q] * b_re[p] - a_im[q] * b_im[p])
        )
        im.append(
            (a_re[q] * b_im[p] + a_im[q] * b_re[p]) - (a_re[p] * b_im[q] + a_im[p] * b_re[q])
        )
    return [m[0][0], m[0][1], re], [m[1][0], m[1][1], im]


def load(ref, lead, rows, count=3):
    return tuple(
        [[ref[(*lead, part, i, j, rows)] for j in range(3)] for i in range(count)]
        for part in range(2)
    )


def load2(ref, lead, rows):
    return third_row(load(ref, lead, rows, 2))


def store(ref, lead, rows, m):
    for part in range(2):
        for i, row in enumerate(m[part]):
            for j, v in enumerate(row):
                ref[(*lead, part, i, j, rows)] = v


def mapped(fn, *ms):
    return tuple(
        [[fn(*vs) for vs in zip(*rows)] for rows in zip(*[m[part] for m in ms])]
        for part in range(2)
    )


def add(*ms):
    return mapped(lambda *vs: functools.reduce(lambda a, b: a + b, vs), *ms)


def ahead_x(m):
    return mapped(lambda v: pltpu.roll(v, v.shape[-1] - 1, 1), m)


def back_x(m):
    return mapped(lambda v: pltpu.roll(v, 1, 1), m)


def mul(a, b, da=False, db=False, rows=3):
    out_re, out_im = [], []
    for i in range(rows):
        row_re, row_im = [], []
        for k in range(3):
            re = im = None
            for j in range(3):
                ar, ai = (a[0][j][i], a[1][j][i]) if da else (a[0][i][j], a[1][i][j])
                br, bi = (b[0][k][j], b[1][k][j]) if db else (b[0][j][k], b[1][j][k])
                rr, ii, ri, ir = ar * br, ai * bi, ar * bi, ai * br
                tr = rr + ii if da != db else rr - ii
                if da and db:
                    ti = -(ri + ir)
                elif da:
                    ti = ri - ir
                elif db:
                    ti = ir - ri
                else:
                    ti = ri + ir
                re = tr if re is None else re + tr
                im = ti if im is None else im + ti
            row_re.append(re)
            row_im.append(im)
        out_re.append(row_re)
        out_im.append(row_im)
    return out_re, out_im


def normalized(re, im):
    weight = sum(v * v for v in re) + sum(v * v for v in im)
    scale = lax.rsqrt(jnp.maximum(weight, FLOOR))
    return [v * scale for v in re], [v * scale for v in im]


def project(re, im):
    u_re, u_im = normalized(re[0], im[0])
    in_re = sum(u_re[j] * re[1][j] + u_im[j] * im[1][j] for j in range(3))
    in_im = sum(u_re[j] * im[1][j] - u_im[j] * re[1][j] for j in range(3))
    w_re = [re[1][j] - (in_re * u_re[j] - in_im * u_im[j]) for j in range(3)]
    w_im = [im[1][j] - (in_re * u_im[j] + in_im * u_re[j]) for j in range(3)]
    v_re, v_im = normalized(w_re, w_im)
    return third_row(([u_re, v_re], [u_im, v_im]))


def mixed(link, staples, weight):
    re = [[0.5 * link[0][i][j] + weight * staples[0][i][j] for j in range(3)] for i in range(2)]
    im = [[0.5 * link[1][i][j] + weight * staples[1][i][j] for j in range(3)] for i in range(2)]
    return project(re, im)


def kernel(
    ta, gz, half,
    sp, tl, pol, mean,
    F, T, H, TH, UP, S, L, AB, M, sm, ar, tree, pb, bc, zs,
    local_sem, send_sem, recv_sem, ready_sem,
):
    j, z, h = lax.axis_index("ta"), lax.axis_index("gz"), lax.axis_index("gy")
    o = 1 - h
    zp, zm = lax.rem(z + 1, gz), lax.rem(z + gz - 1, gz)
    full = 2 * half
    nd = 2 * ta
    own = full // nd
    me = 2 * j + h
    mine = pl.ds(pl.multiple_of(h * half, half), half)
    halves = [pl.ds(k * half, half) for k in range(2)]

    sent = []
    n_sem = [0, 0]

    def remote(src, dst, recv_index, **where):
        k = n_sem[0]
        n_sem[0] += 1
        copy = pltpu.make_async_remote_copy(
            src_ref=src, dst_ref=dst, send_sem=send_sem.at[k], recv_sem=recv_sem.at[recv_index],
            device_id=where, device_id_type=MESH,
        )
        copy.start()
        sent.append(copy)

    def arrived(dst, recv_index):
        pltpu.make_async_remote_copy(
            src_ref=dst, dst_ref=dst, send_sem=send_sem.at[0], recv_sem=recv_sem.at[recv_index],
            device_id={"gy": o}, device_id_type=MESH,
        ).wait_recv()

    def new_recv(n=1):
        k = n_sem[1]
        n_sem[1] += n
        return k

    near = [
        pltpu.make_async_copy(sp.at[:, :, :, :, h, 0], F.at[0, 0:3, :, :, :, mine], local_sem.at[0]),
        pltpu.make_async_copy(tl.at[:, :, :, h, 0], T.at[:, :, :, mine], local_sem.at[1]),
    ]
    for copy in near:
        copy.start()

    barrier = pltpu.get_barrier_semaphore()
    around = sorted({(0, 1 % gz), (0, (gz - 1) % gz), (1 % ta, 0), ((ta - 1) % ta, 0)} - {(0, 0)})

    def place(dx, dz):
        return {"ta": lax.rem(j + dx, ta), "gz": lax.rem(z + dz, gz)}

    def signal(sem, **where):
        pl.semaphore_signal(sem, inc=1, device_id=where, device_id_type=MESH)

    signal(barrier, gy=o)
    for dx, dz in around:
        for c in range(2):
            signal(barrier, **place(dx, dz), gy=c)
    pl.semaphore_wait(barrier, 1 + 2 * len(around))

    rounds = max(ta // 2, gz // 2) - 1
    heard = [0]

    def hear(count=1):
        for _ in range(count):
            if 0 < heard[0] <= rounds:
                pl.semaphore_wait(ready_sem.at[heard[0] - 1], len(around))
            heard[0] += 1
            if heard[0] <= rounds:
                for dx, dz in around:
                    signal(ready_sem.at[heard[0] - 1], **place(dx, dz))

    r_v, r_x, r_y, r_t = new_recv(2), new_recv(4), new_recv(4), new_recv(4)
    r_own, r_ownt = new_recv(), new_recv()

    def plane(f, t):
        return sp.at[f, :, 0:2, :, t, 0] if f is not None else tl.at[:, 0:2, :, t, 0]

    def two(ref, *lead):
        return ref.at[(*lead, slice(None), slice(0, 2), slice(None), mine)]

    for t in range(2):
        remote(plane(FZ, t), two(F, 0, FV), r_v + h, gz=zp, gy=t)
    remote(sp.at[:, :, :, :, o, 0], F.at[0, 0:3, :, :, :, mine], r_own, gy=o)
    for f, r in ((FX, r_x), (FY, r_y)):
        for t in range(2):
            remote(plane(f, t), two(H, 0, 0, f), r + h, gz=zm, gy=t)
            remote(plane(f, t), two(H, 0, 1, f), r + 2 + h, gz=zp, gy=t)
    remote(tl.at[:, :, :, o, 0], T.at[:, :, :, mine], r_ownt, gy=o)
    for t in range(2):
        remote(plane(None, t), two(TH, 0), r_t + h, gz=zm, gy=t)
    hear()

    def each_half(body):
        def run(k, carry):
            r0 = pl.multiple_of(k * half, half)
            body(pl.ds(r0, half), pl.ds(r0 + 1, half))
            return carry

        lax.fori_loop(0, 2, run, 0)

    def wrap(ref, *lead):
        ref[(*lead, slice(None), slice(None), slice(None), pl.ds(full, 1))] = ref[
            (*lead, slice(None), slice(None), slice(None), pl.ds(0, 1))
        ]

    def unwrap(k):
        L[k, :, :, :, pl.ds(0, 1)] = L[k, :, :, :, pl.ds(full, 1)]

    def in_plane(s):
        def body(rows, up):
            ux, uy = load(F, (s, FX), rows), load(F, (s, FY), rows)
            uy_x, ux_y = ahead_x(uy), load(F, (s, FX), up)
            c, d = mul(ux, uy_x), mul(uy, ux_y)
            store(S, (FX,), rows, mul(d, uy_x, db=True, rows=2))
            store(L, (0,), up, mul(uy, c, da=True, rows=2))
            store(
                S, (FY,), rows,
                add(mul(c, ux_y, db=True, rows=2), back_x(mul(ux, d, da=True, rows=2))),
            )

        each_half(body)
        unwrap(0)

    def side(ref, s, f, rows, up):
        return ahead_x(load(ref, (s, f), rows)) if up is None else load(ref, (s, f), up)

    def across(s, f):
        def body(rows, up):
            up = None if f == FX else up
            uz, uz_f = load(F, (s, FZ), rows), side(F, s, FZ, rows, up)
            a = mul(uz, load2(H, (s, 0, f), rows))
            store(AB, (0,), rows, a)
            total = add(load(S, (f,), rows, 2), mul(a, uz_f, db=True, rows=2))
            uv, uv_f = load(F, (s, FV), rows), side(F, s, FV, rows, up)
            b = mul(load2(H, (s, 1, f), rows), uv_f)
            store(AB, (1,), rows, b)
            total = add(total, mul(uv, b, da=True, rows=2))
            if f == FX:
                total = add(total, load(L, (0,), rows, 2))
            store(F, (s + 1, f), rows, mixed(load(F, (s, f), rows, 2), total, 0.125))

        each_half(body)

    def z_staples(s, f):
        def body(rows, up):
            shift = None if f == FX else up
            uf = load(F, (s, f), rows)
            b = mul(uf, side(F, s, FZ, rows, shift), rows=2)
            upper = mul(b, load2(H, (s, 0, f), rows), db=True, rows=2)
            lower = mul(uf, load(AB, (0,), rows), da=True, rows=2)
            below = load2(H, (s, 1, f), rows)
            v_upper = mul(load(AB, (1,), rows), uf, db=True, rows=2)
            v_lower = mul(mul(below, load(F, (s, FV), rows), da=True, rows=2), uf, rows=2)
            if f == FX:
                store(S, (FZ,), rows, add(upper, back_x(lower)))
                store(S, (FV,), rows, add(v_upper, back_x(v_lower)))
            else:
                store(L, (1,), up, lower)
                store(L, (2,), up, v_lower)
                store(S, (FZ,), rows, add(load(S, (FZ,), rows, 2), upper))
                store(S, (FV,), rows, add(load(S, (FV,), rows, 2), v_upper))

        each_half(body)
        if f == FY:
            unwrap(1)
            unwrap(2)

    def z_links(s):
        def body(rows, up):
            for f, k in ((FZ, 1), (FV, 2)):
                total = add(load(S, (f,), rows, 2), load(L, (k,), rows, 2))
                store(F, (s + 1, f), rows, mixed(load(F, (s, f), rows, 2), total, 0.125))

        each_half(body)
        wrap(F, s + 1, FZ)
        wrap(F, s + 1, FV)

    for copy in near:
        copy.wait()
    other = pl.ds(pl.multiple_of(o * half, half), half)
    arrived(F.at[0, 0:3, :, :, :, other], r_own)
    wrap(F, 0, FX)
    wrap(F, 0, FZ)
    in_plane(0)
    hear()
    for k in range(2):
        arrived(F.at[0, FV, :, 0:2, :, halves[k]], r_v + k)

    def complete(rows, up):
        store(F, (0, FV), rows, load2(F, (0, FV), rows))

    each_half(complete)
    wrap(F, 0, FV)

    r_next = new_recv(4)

    def onward(s, f):
        remote(
            F.at[s, f, :, 0:2, :, 0:full], UP.at[f], r_next + f,
            ta=lax.rem(j + h + ta - 1, ta), gy=o,
        )

    for s in range(STEPS):
        last = s == STEPS - 1
        sems = {}
        for f in (FX, FY):
            if s == 0:
                for side_k in range(2):
                    for k in range(2):
                        arrived(
                            H.at[0, side_k, f, :, :, :, halves[k]],
                            (r_x, r_y)[f] + 2 * side_k + k,
                        )
            else:
                for side_k in range(2):
                    arrived(H.at[s, side_k, f], r_now[f] + side_k)
            across(s, f)
            if f == FX:
                wrap(F, s + 1, FX)
            if last:
                onward(s + 1, f)
            else:
                sems[f] = new_recv(2)
                out = F.at[s + 1, f, :, 0:2, :, 0:full]
                remote(out, H.at[s + 1, 0, f], sems[f], gz=zm)
                remote(out, H.at[s + 1, 1, f], sems[f] + 1, gz=zp)
            hear()
            z_staples(s, f)
        r_now = sems
        if s == STEPS - 2:
            for t in range(2):
                remote(plane(None, t), two(TH, 1), r_t + 2 + h, gz=zp, gy=t)
        z_links(s)
        if last:
            onward(s + 1, FZ)
            onward(s + 1, FV)
        else:
            hear()
            in_plane(s + 1)
    while heard[0] <= rounds:
        hear()

    n = STEPS
    arrived(T.at[:, :, :, other], r_ownt)
    wrap(T)
    for side_k in range(2):
        for k in range(2):
            arrived(TH.at[side_k, :, :, :, halves[k]], r_t + 2 * side_k + k)

    def before(rows, up):
        t = load(T, (), rows)
        ux, uy = load(F, (n, FX), rows), load(F, (n, FY), rows)
        store(M, (0,), rows, mul(ux, ahead_x(t), rows=2))
        store(M, (1,), rows, mul(ux, t, da=True, rows=2))
        store(M, (2,), rows, mul(uy, load(T, (), up), rows=2))
        store(M, (3,), rows, mul(uy, t, da=True, rows=2))
        store(M, (4,), rows, mul(load(F, (n, FZ), rows), load2(TH, (0,), rows), rows=2))
        store(
            M, (5,), rows, mul(load(F, (n, FV), rows), load2(TH, (1,), rows), da=True, rows=2)
        )

    each_half(before)
    arrived(UP.at[FX], r_next + FX)
    arrived(UP.at[FY], r_next + FY)

    def along_xy(rows, up):
        ux, uy = load2(UP, (FX,), rows), load2(UP, (FY,), rows)
        total = add(
            mul(load(M, (0,), rows, 2), ux, db=True, rows=2),
            back_x(mul(load(M, (1,), rows, 2), ux, rows=2)),
            mul(load(M, (2,), rows, 2), uy, db=True, rows=2),
        )
        store(S, (0,), rows, total)
        store(L, (0,), up, mul(load(M, (3,), rows, 2), uy, rows=2))

    each_half(along_xy)
    unwrap(0)
    arrived(UP.at[FZ], r_next + FZ)
    arrived(UP.at[FV], r_next + FV)

    def finish(k, carry):
        r0 = pl.multiple_of(k * half, half)
        rows = pl.ds(r0, half)
        uz, uv = load2(UP, (FZ,), rows), load2(UP, (FV,), rows)
        total = add(
            load(S, (0,), rows, 2),
            load(L, (0,), rows, 2),
            mul(load(M, (4,), rows, 2), uz, db=True, rows=2),
            mul(load(M, (5,), rows, 2), uv, rows=2),
        )
        done = mixed(load(T, (), rows, 2), total, 0.5 / 6.0)
        for part in range(2):
            for a in range(2):
                for b in range(3):
                    sm[pl.ds(r0 * 16 + part * 6 + a * 3 + b, half, 16), :] = done[part][a][b]
        return carry

    lax.fori_loop(0, 2, finish, 0)

    span = own * 16
    r_row = new_recv(nd)
    offsets = sorted(range(1, nd), key=lambda k: -min(k // 2, ta - k // 2))
    here = pl.ds(pl.multiple_of(me * span, 8), span)
    for k in offsets:
        d = 2 * lax.rem(j + k // 2, ta) + lax.rem(h + k, 2)
        remote(
            sm.at[pl.ds(pl.multiple_of(d * span, 8), span)], ar.at[here], r_row + me,
            ta=d // 2, gy=lax.rem(d, 2),
        )
    ar[here, :] = sm[here, :]
    for k in range(1, nd):
        d = lax.rem(me + k, nd)
        arrived(ar.at[pl.ds(pl.multiple_of(d * span, 8), span)], r_row + d)

    def slices(start, stride, rows):
        at = lambda c: ar[pl.ds(start + c, rows, stride), :]
        return third_row(
            tuple([[at(part * 6 + a * 3 + b) for b in range(3)] for a in range(2)] for part in range(2))
        )

    for row in range(own):
        rows = nd // 2
        lhs, rhs = slices(row * 16, 2 * span, rows), slices(row * 16 + span, 2 * span, rows)
        while rows > 1:
            prod = mul(lhs, rhs)
            flat = [v for part in prod for line in part for v in line]
            for c, v in enumerate(flat):
                tree[pl.ds(c * 8, rows), :] = v
            rows //= 2
            pick = lambda first: [tree[pl.ds(c * 8 + first, rows, 2), :] for c in range(18)]
            grid = lambda vs: tuple(
                [[vs[part * 9 + a * 3 + b] for b in range(3)] for a in range(3)] for part in range(2)
            )
            lhs, rhs = grid(pick(0)), grid(pick(1))
        re = im = None
        for a in range(3):
            for b in range(3):
                lr, li, rr, ri = lhs[0][a][b], lhs[1][a][b], rhs[0][b][a], rhs[1][b][a]
                t_re, t_im = lr * rr - li * ri, lr * ri + li * rr
                re = t_re if re is None else re + t_re
                im = t_im if im is None else im + t_im
        pb[row, 0:1, :] = re / 3.0
        pb[row, 1:2, :] = im / 3.0

    r_out = new_recv(nd)
    home = pl.ds(me * own, own)
    for k in offsets:
        d = 2 * lax.rem(j + k // 2, ta) + lax.rem(h + k, 2)
        remote(pb, bc.at[home], r_out + me, ta=d // 2, gy=lax.rem(d, 2))
    bc[home] = pb[...]
    for k in range(1, nd):
        d = lax.rem(me + k, nd)
        arrived(bc.at[pl.ds(d * own, own)], r_out + d)

    sums = jnp.sum(bc[...], axis=0)
    zs[z] = sums
    r_sum = new_recv(gz)
    for k in sorted(range(1, gz), key=lambda k: -min(k, gz - k)):
        remote(zs.at[z], zs.at[z], r_sum + z, gz=lax.rem(z + k, gz))
    for k in range(half):
        pol[:, 0, k, :] = bc[h * half + k]
    for k in range(1, gz):
        d = lax.rem(z + k, gz)
        arrived(zs.at[d], r_sum + d)
    totals = jnp.sum(zs[...], axis=0)
    sites = float(full * gz * sp.shape[-1])
    for part in range(2):
        mean[part] = jnp.sum(totals[part : part + 1, :]) / sites

    for copy in sent:
        copy.wait_send()


def solution(mesh):
    ta, gz = mesh.shape["ta"], mesh.shape["gz"]

    def body(sp, tl):
        half, lanes = sp.shape[-2:]
        full = 2 * half
        pad = full + 8
        nd = 2 * ta
        own = full // nd

        def vmem(*dims):
            return pltpu.VMEM((*dims, lanes), F32)

        n_send = 2 + 1 + 8 + 1 + 4 + 4 * (STEPS - 1) + 4 + 2 * (nd - 1) + gz - 1
        n_recv = 2 + 4 + 4 + 4 + 2 + 4 + 4 * (STEPS - 1) + 2 * nd + gz
        return pl.pallas_call(
            functools.partial(kernel, ta, gz, half),
            out_shape=(
                jax.ShapeDtypeStruct((2, 1, half, lanes), F32),
                jax.ShapeDtypeStruct((2,), F32),
            ),
            in_specs=[pl.BlockSpec(memory_space=pl.ANY)] * 2,
            out_specs=(
                pl.BlockSpec(memory_space=pltpu.VMEM),
                pl.BlockSpec(memory_space=pltpu.SMEM),
            ),
            scratch_shapes=[
                vmem(STEPS + 1, 4, 2, 3, 3, pad),
                vmem(2, 3, 3, pad),
                vmem(STEPS, 2, 2, 2, 2, 3, full),
                vmem(2, 2, 2, 3, full),
                vmem(4, 2, 2, 3, full),
                vmem(4, 2, 2, 3, full),
                vmem(3, 2, 2, 3, pad),
                vmem(2, 2, 3, 3, full),
                vmem(6, 2, 2, 3, full),
                vmem(full * 16),
                vmem(full * 16),
                vmem(18 * 8),
                vmem(own, 2),
                vmem(full, 2),
                vmem(gz, 2),
                pltpu.SemaphoreType.DMA((2,)),
                pltpu.SemaphoreType.DMA((n_send,)),
                pltpu.SemaphoreType.DMA((n_recv,)),
                pltpu.SemaphoreType.REGULAR((max(ta // 2, gz // 2),)),
            ],
            compiler_params=pltpu.CompilerParams(
                collective_id=0, has_side_effects=True, vmem_limit_bytes=63 * 1024 * 1024
            ),
        )(sp, tl)

    return jax.shard_map(
        body,
        mesh=mesh,
        in_specs=(
            P("cfg", None, None, None, "ta", "gz", "gy", None),
            P("cfg", None, None, "ta", "gz", "gy", None),
        ),
        out_specs=(P("cfg", "gz", "gy", None), P("cfg")),
        check_vma=False,
    )
```

```python
import functools

import jax
import jax.numpy as jnp
from jax import lax
from jax.experimental import pallas as pl
from jax.experimental.pallas import tpu as pltpu
from jax.sharding import PartitionSpec as P

MESH = pl.DeviceIdType.MESH
F32 = jnp.float32
STEPS = 3
FLOOR = 0.25
FX, FY, FZ, FV = 0, 1, 2, 3


def third_row(m):
    (a_re, b_re), (a_im, b_im) = m[0][:2], m[1][:2]
    re, im = [], []
    for k in range(3):
        p, q = (k + 1) % 3, (k + 2) % 3
        re.append(
            a_re[p] * b_re[q] - a_im[p] * b_im[q] - (a_re[q] * b_re[p] - a_im[q] * b_im[p])
        )
        im.append(
            (a_re[q] * b_im[p] + a_im[q] * b_re[p]) - (a_re[p] * b_im[q] + a_im[p] * b_re[q])
        )
    return [m[0][0], m[0][1], re], [m[1][0], m[1][1], im]


def load(ref, lead, rows, count=3):
    return tuple(
        [[ref[(*lead, part, i, j, rows)] for j in range(3)] for i in range(count)]
        for part in range(2)
    )


def load2(ref, lead, rows):
    return third_row(load(ref, lead, rows, 2))


def store(ref, lead, rows, m):
    for part in range(2):
        for i, row in enumerate(m[part]):
            for j, v in enumerate(row):
                ref[(*lead, part, i, j, rows)] = v


def mapped(fn, *ms):
    return tuple(
        [[fn(*vs) for vs in zip(*rows)] for rows in zip(*[m[part] for m in ms])]
        for part in range(2)
    )


def add(*ms):
    return mapped(lambda *vs: functools.reduce(lambda a, b: a + b, vs), *ms)


def ahead_x(m):
    return mapped(lambda v: pltpu.roll(v, v.shape[-1] - 1, 1), m)


def back_x(m):
    return mapped(lambda v: pltpu.roll(v, 1, 1), m)


def mul(a, b, da=False, db=False, rows=3):
    out_re, out_im = [], []
    for i in range(rows):
        row_re, row_im = [], []
        for k in range(3):
            re = im = None
            for j in range(3):
                ar, ai = (a[0][j][i], a[1][j][i]) if da else (a[0][i][j], a[1][i][j])
                br, bi = (b[0][k][j], b[1][k][j]) if db else (b[0][j][k], b[1][j][k])
                rr, ii, ri, ir = ar * br, ai * bi, ar * bi, ai * br
                tr = rr + ii if da != db else rr - ii
                if da and db:
                    ti = -(ri + ir)
                elif da:
                    ti = ri - ir
                elif db:
                    ti = ir - ri
                else:
                    ti = ri + ir
                re = tr if re is None else re + tr
                im = ti if im is None else im + ti
            row_re.append(re)
            row_im.append(im)
        out_re.append(row_re)
        out_im.append(row_im)
    return out_re, out_im


def normalized(re, im):
    weight = sum(v * v for v in re) + sum(v * v for v in im)
    scale = lax.rsqrt(jnp.maximum(weight, FLOOR))
    return [v * scale for v in re], [v * scale for v in im]


def project(re, im):
    u_re, u_im = normalized(re[0], im[0])
    in_re = sum(u_re[j] * re[1][j] + u_im[j] * im[1][j] for j in range(3))
    in_im = sum(u_re[j] * im[1][j] - u_im[j] * re[1][j] for j in range(3))
    w_re = [re[1][j] - (in_re * u_re[j] - in_im * u_im[j]) for j in range(3)]
    w_im = [im[1][j] - (in_re * u_im[j] + in_im * u_re[j]) for j in range(3)]
    v_re, v_im = normalized(w_re, w_im)
    return third_row(([u_re, v_re], [u_im, v_im]))


def mixed(link, staples, weight):
    re = [[0.5 * link[0][i][j] + weight * staples[0][i][j] for j in range(3)] for i in range(2)]
    im = [[0.5 * link[1][i][j] + weight * staples[1][i][j] for j in range(3)] for i in range(2)]
    return project(re, im)


def kernel(
    ta, gz, half,
    sp, tl, pol, mean,
    F, T, H, TH, UP, S, L, AB, M, sm, ar, tree, pb, bc, zs,
    local_sem, send_sem, recv_sem, ready_x, ready_z,
):
    def wrapped(v, n):
        return jnp.where(v >= n, v - n, v)

    j, z, h = lax.axis_index("ta"), lax.axis_index("gz"), lax.axis_index("gy")
    o = 1 - h
    zp, zm = wrapped(z + 1, gz), wrapped(z + gz - 1, gz)
    full = 2 * half
    nd = 2 * ta
    own = full // nd
    me = 2 * j + h
    mine = pl.ds(pl.multiple_of(h * half, half), half)
    halves = [pl.ds(k * half, half) for k in range(2)]

    sent = []
    n_sem = [0, 0]

    def remote(src, dst, recv_index, **where):
        k = n_sem[0]
        n_sem[0] += 1
        copy = pltpu.make_async_remote_copy(
            src_ref=src, dst_ref=dst, send_sem=send_sem.at[k], recv_sem=recv_sem.at[recv_index],
            device_id=where, device_id_type=MESH,
        )
        copy.start()
        sent.append(copy)

    def arrived(dst, recv_index):
        pltpu.make_async_remote_copy(
            src_ref=dst, dst_ref=dst, send_sem=send_sem.at[0], recv_sem=recv_sem.at[recv_index],
            device_id={"gy": o}, device_id_type=MESH,
        ).wait_recv()

    def new_recv(n=1):
        k = n_sem[1]
        n_sem[1] += n
        return k

    near = [
        pltpu.make_async_copy(sp.at[:, :, :, :, h, 0], F.at[0, 0:3, :, :, :, mine], local_sem.at[0]),
        pltpu.make_async_copy(tl.at[:, :, :, h, 0], T.at[:, :, :, mine], local_sem.at[1]),
    ]
    for copy in near:
        copy.start()

    barrier = pltpu.get_barrier_semaphore()
    around = sorted({(0, 1 % gz), (0, (gz - 1) % gz), (1 % ta, 0), ((ta - 1) % ta, 0)} - {(0, 0)})

    def place(dx, dz):
        return {"ta": wrapped(j + dx, ta), "gz": wrapped(z + dz, gz)}

    def signal(sem, **where):
        pl.semaphore_signal(sem, inc=1, device_id=where, device_id_type=MESH)

    signal(barrier, gy=o)
    for dx, dz in around:
        for c in range(2):
            signal(barrier, **place(dx, dz), gy=c)
    pl.semaphore_wait(barrier, 1 + 2 * len(around))

    def relay(sem, rounds, sides):
        done = [0]

        def go(last=False):
            while True:
                if 0 < done[0] <= rounds:
                    pl.semaphore_wait(sem.at[done[0] - 1], len(sides))
                done[0] += 1
                if done[0] <= rounds:
                    for where in sides:
                        signal(sem.at[done[0] - 1], **where)
                if not last or done[0] > rounds:
                    return

        return go

    hear_x = relay(
        ready_x, ta // 2 - 1, [{"ta": wrapped(j + k, ta)} for k in sorted({1 % ta, ta - 1} - {0})]
    )
    hear_z = relay(
        ready_z, gz // 2 - STEPS, [{"gz": wrapped(z + k, gz)} for k in sorted({1 % gz, gz - 1} - {0})]
    )

    r_v, r_x, r_y, r_t = new_recv(2), new_recv(4), new_recv(4), new_recv(4)
    r_own, r_ownt = new_recv(), new_recv()

    def plane(f, t):
        return sp.at[f, :, 0:2, :, t, 0] if f is not None else tl.at[:, 0:2, :, t, 0]

    def two(ref, *lead):
        return ref.at[(*lead, slice(None), slice(0, 2), slice(None), mine)]

    for t in range(2):
        remote(plane(FZ, t), two(F, 0, FV), r_v + h, gz=zp, gy=t)
    remote(sp.at[:, :, :, :, o, 0], F.at[0, 0:3, :, :, :, mine], r_own, gy=o)
    for f, r in ((FX, r_x), (FY, r_y)):
        for t in range(2):
            remote(plane(f, t), two(H, 0, 0, f), r + h, gz=zm, gy=t)
            remote(plane(f, t), two(H, 0, 1, f), r + 2 + h, gz=zp, gy=t)
    remote(tl.at[:, :, :, o, 0], T.at[:, :, :, mine], r_ownt, gy=o)
    for t in range(2):
        remote(plane(None, t), two(TH, 0), r_t + h, gz=zm, gy=t)
    hear_x()

    def each_half(body):
        def run(k, carry):
            r0 = pl.multiple_of(k * half, half)
            body(pl.ds(r0, half), pl.ds(r0 + 1, half))
            return carry

        lax.fori_loop(0, 2, run, 0)

    def wrap(ref, *lead):
        ref[(*lead, slice(None), slice(None), slice(None), pl.ds(full, 1))] = ref[
            (*lead, slice(None), slice(None), slice(None), pl.ds(0, 1))
        ]

    def unwrap(k):
        L[k, :, :, :, pl.ds(0, 1)] = L[k, :, :, :, pl.ds(full, 1)]

    def in_plane(s):
        def body(rows, up):
            ux, uy = load(F, (s, FX), rows), load(F, (s, FY), rows)
            uy_x, ux_y = ahead_x(uy), load(F, (s, FX), up)
            c, d = mul(ux, uy_x), mul(uy, ux_y)
            store(S, (FX,), rows, mul(d, uy_x, db=True, rows=2))
            store(L, (0,), up, mul(uy, c, da=True, rows=2))
            store(
                S, (FY,), rows,
                add(mul(c, ux_y, db=True, rows=2), back_x(mul(ux, d, da=True, rows=2))),
            )

        each_half(body)
        unwrap(0)

    def side(ref, s, f, rows, up):
        return ahead_x(load(ref, (s, f), rows)) if up is None else load(ref, (s, f), up)

    def across(s, f):
        def body(rows, up):
            up = None if f == FX else up
            uz, uz_f = load(F, (s, FZ), rows), side(F, s, FZ, rows, up)
            a = mul(uz, load2(H, (s, 0, f), rows))
            store(AB, (0,), rows, a)
            total = add(load(S, (f,), rows, 2), mul(a, uz_f, db=True, rows=2))
            uv, uv_f = load(F, (s, FV), rows), side(F, s, FV, rows, up)
            b = mul(load2(H, (s, 1, f), rows), uv_f)
            store(AB, (1,), rows, b)
            total = add(total, mul(uv, b, da=True, rows=2))
            if f == FX:
                total = add(total, load(L, (0,), rows, 2))
            store(F, (s + 1, f), rows, mixed(load(F, (s, f), rows, 2), total, 0.125))

        each_half(body)

    def z_staples(s, f):
        def body(rows, up):
            shift = None if f == FX else up
            uf = load(F, (s, f), rows)
            b = mul(uf, side(F, s, FZ, rows, shift), rows=2)
            upper = mul(b, load2(H, (s, 0, f), rows), db=True, rows=2)
            lower = mul(uf, load(AB, (0,), rows), da=True, rows=2)
            below = load2(H, (s, 1, f), rows)
            v_upper = mul(load(AB, (1,), rows), uf, db=True, rows=2)
            v_lower = mul(mul(below, load(F, (s, FV), rows), da=True, rows=2), uf, rows=2)
            if f == FX:
                store(S, (FZ,), rows, add(upper, back_x(lower)))
                store(S, (FV,), rows, add(v_upper, back_x(v_lower)))
            else:
                store(L, (1,), up, lower)
                store(L, (2,), up, v_lower)
                store(S, (FZ,), rows, add(load(S, (FZ,), rows, 2), upper))
                store(S, (FV,), rows, add(load(S, (FV,), rows, 2), v_upper))

        each_half(body)
        if f == FY:
            unwrap(1)
            unwrap(2)

    def z_links(s):
        def body(rows, up):
            for f, k in ((FZ, 1), (FV, 2)):
                total = add(load(S, (f,), rows, 2), load(L, (k,), rows, 2))
                store(F, (s + 1, f), rows, mixed(load(F, (s, f), rows, 2), total, 0.125))

        each_half(body)
        wrap(F, s + 1, FZ)
        wrap(F, s + 1, FV)

    for copy in near:
        copy.wait()
    other = pl.ds(pl.multiple_of(o * half, half), half)
    arrived(F.at[0, 0:3, :, :, :, other], r_own)
    wrap(F, 0, FX)
    wrap(F, 0, FZ)
    in_plane(0)
    for k in range(2):
        arrived(F.at[0, FV, :, 0:2, :, halves[k]], r_v + k)

    def complete(rows, up):
        store(F, (0, FV), rows, load2(F, (0, FV), rows))

    each_half(complete)
    wrap(F, 0, FV)

    r_next = new_recv(4)

    def onward(s, f):
        remote(
            F.at[s, f, :, 0:2, :, 0:full], UP.at[f], r_next + f,
            ta=wrapped(j + h + ta - 1, ta), gy=o,
        )

    for s in range(STEPS):
        last = s == STEPS - 1
        sems = {}
        for f in (FX, FY):
            if s == 0:
                for side_k in range(2):
                    for k in range(2):
                        arrived(
                            H.at[0, side_k, f, :, :, :, halves[k]],
                            (r_x, r_y)[f] + 2 * side_k + k,
                        )
            else:
                for side_k in range(2):
                    arrived(H.at[s, side_k, f], r_now[f] + side_k)
            across(s, f)
            if f == FX:
                wrap(F, s + 1, FX)
            if last:
                onward(s + 1, f)
            else:
                sems[f] = new_recv(2)
                out = F.at[s + 1, f, :, 0:2, :, 0:full]
                remote(out, H.at[s + 1, 0, f], sems[f], gz=zm)
                remote(out, H.at[s + 1, 1, f], sems[f] + 1, gz=zp)
            if f == FY:
                hear_x(last)
            if last:
                hear_z()
            z_staples(s, f)
        r_now = sems
        if s == STEPS - 2:
            for t in range(2):
                remote(plane(None, t), two(TH, 1), r_t + 2 + h, gz=zp, gy=t)
        z_links(s)
        if last:
            onward(s + 1, FZ)
            onward(s + 1, FV)
        else:
            in_plane(s + 1)

    n = STEPS
    arrived(T.at[:, :, :, other], r_ownt)
    wrap(T)
    for side_k in range(2):
        for k in range(2):
            arrived(TH.at[side_k, :, :, :, halves[k]], r_t + 2 * side_k + k)

    def before(rows, up):
        t = load(T, (), rows)
        ux, uy = load(F, (n, FX), rows), load(F, (n, FY), rows)
        store(M, (0,), rows, mul(ux, ahead_x(t), rows=2))
        store(M, (1,), rows, mul(ux, t, da=True, rows=2))
        store(M, (2,), rows, mul(uy, load(T, (), up), rows=2))
        store(M, (3,), rows, mul(uy, t, da=True, rows=2))
        store(M, (4,), rows, mul(load(F, (n, FZ), rows), load2(TH, (0,), rows), rows=2))
        store(
            M, (5,), rows, mul(load(F, (n, FV), rows), load2(TH, (1,), rows), da=True, rows=2)
        )

    each_half(before)
    hear_z()
    arrived(UP.at[FX], r_next + FX)
    arrived(UP.at[FY], r_next + FY)

    def along_xy(rows, up):
        ux, uy = load2(UP, (FX,), rows), load2(UP, (FY,), rows)
        total = add(
            mul(load(M, (0,), rows, 2), ux, db=True, rows=2),
            back_x(mul(load(M, (1,), rows, 2), ux, rows=2)),
            mul(load(M, (2,), rows, 2), uy, db=True, rows=2),
        )
        store(S, (0,), rows, total)
        store(L, (0,), up, mul(load(M, (3,), rows, 2), uy, rows=2))

    each_half(along_xy)
    hear_z()
    unwrap(0)
    arrived(UP.at[FZ], r_next + FZ)
    arrived(UP.at[FV], r_next + FV)

    def finish(k, carry):
        r0 = pl.multiple_of(k * half, half)
        rows = pl.ds(r0, half)
        uz, uv = load2(UP, (FZ,), rows), load2(UP, (FV,), rows)
        total = add(
            load(S, (0,), rows, 2),
            load(L, (0,), rows, 2),
            mul(load(M, (4,), rows, 2), uz, db=True, rows=2),
            mul(load(M, (5,), rows, 2), uv, rows=2),
        )
        done = mixed(load(T, (), rows, 2), total, 0.5 / 6.0)
        for part in range(2):
            for a in range(2):
                for b in range(3):
                    sm[pl.ds(r0 * 16 + part * 6 + a * 3 + b, half, 16), :] = done[part][a][b]
        return carry

    lax.fori_loop(0, 2, finish, 0)

    span = own * 16
    sm3, ar3 = sm.reshape(full, 16, sm.shape[-1]), ar.reshape(full, 16, sm.shape[-1])
    r_row = new_recv(nd)
    offsets = sorted(range(1, nd), key=lambda k: -min(k // 2, ta - k // 2))
    here = pl.ds(me * own, own)

    def part_of(ref, d):
        return ref.at[pl.ds(d * own, own), 0:12]

    for k in offsets:
        dj, dh = wrapped(j + k // 2, ta), (h if k % 2 == 0 else o)
        remote(part_of(sm3, 2 * dj + dh), part_of(ar3, me), r_row + me, ta=dj, gy=dh)
    hear_z()
    ar3[here] = sm3[here]
    for k in range(1, nd):
        d = wrapped(me + k, nd)
        arrived(part_of(ar3, d), r_row + d)

    def slices(start, stride, rows):
        at = lambda c: ar[pl.ds(start + c, rows, stride), :]
        return third_row(
            tuple([[at(part * 6 + a * 3 + b) for b in range(3)] for a in range(2)] for part in range(2))
        )

    for row in range(own):
        rows = nd // 2
        lhs, rhs = slices(row * 16, 2 * span, rows), slices(row * 16 + span, 2 * span, rows)
        while rows > 1:
            prod = mul(lhs, rhs)
            flat = [v for part in prod for line in part for v in line]
            for c, v in enumerate(flat):
                tree[pl.ds(c * 8, rows), :] = v
            rows //= 2
            pick = lambda first: [tree[pl.ds(c * 8 + first, rows, 2), :] for c in range(18)]
            grid = lambda vs: tuple(
                [[vs[part * 9 + a * 3 + b] for b in range(3)] for a in range(3)] for part in range(2)
            )
            lhs, rhs = grid(pick(0)), grid(pick(1))
        re = im = None
        for a in range(3):
            for b in range(3):
                lr, li, rr, ri = lhs[0][a][b], lhs[1][a][b], rhs[0][b][a], rhs[1][b][a]
                t_re, t_im = lr * rr - li * ri, lr * ri + li * rr
                re = t_re if re is None else re + t_re
                im = t_im if im is None else im + t_im
        pb[row, 0:1, :] = re / 3.0
        pb[row, 1:2, :] = im / 3.0

    hear_z(True)
    r_out = new_recv(nd)
    home = pl.ds(me * own, own)
    for k in offsets:
        remote(
            pb, bc.at[home], r_out + me, ta=wrapped(j + k // 2, ta), gy=h if k % 2 == 0 else o
        )
    bc[home] = pb[...]
    for k in range(1, nd):
        d = wrapped(me + k, nd)
        arrived(bc.at[pl.ds(d * own, own)], r_out + d)

    sums = jnp.sum(bc[...], axis=0)
    zs[z] = sums
    r_sum = new_recv(gz)
    for k in sorted(range(1, gz), key=lambda k: -min(k, gz - k)):
        remote(zs.at[z], zs.at[z], r_sum + z, gz=wrapped(z + k, gz))
    for k in range(half):
        pol[:, 0, k, :] = bc[h * half + k]
    for k in range(1, gz):
        d = wrapped(z + k, gz)
        arrived(zs.at[d], r_sum + d)
    totals = jnp.sum(zs[...], axis=0)
    sites = float(full * gz * sp.shape[-1])
    mean[...] = jnp.broadcast_to(jnp.sum(totals, axis=1, keepdims=True) / sites, totals.shape)

    for copy in sent:
        copy.wait_send()


def solution(mesh):
    ta, gz = mesh.shape["ta"], mesh.shape["gz"]

    def body(sp, tl):
        half, lanes = sp.shape[-2:]
        full = 2 * half
        pad = full + 8
        nd = 2 * ta
        own = full // nd

        def vmem(*dims):
            return pltpu.VMEM((*dims, lanes), F32)

        n_send = 2 + 1 + 8 + 1 + 4 + 4 * (STEPS - 1) + 4 + 2 * (nd - 1) + gz - 1
        n_recv = 2 + 4 + 4 + 4 + 2 + 4 + 4 * (STEPS - 1) + 2 * nd + gz
        polyakov, means = pl.pallas_call(
            functools.partial(kernel, ta, gz, half),
            out_shape=(
                jax.ShapeDtypeStruct((2, 1, half, lanes), F32),
                jax.ShapeDtypeStruct((2, lanes), F32),
            ),
            in_specs=[pl.BlockSpec(memory_space=pltpu.HBM)] * 2,
            out_specs=(pl.BlockSpec(memory_space=pltpu.VMEM),) * 2,
            scratch_shapes=[
                vmem(STEPS + 1, 4, 2, 3, 3, pad),
                vmem(2, 3, 3, pad),
                vmem(STEPS, 2, 2, 2, 2, 3, full),
                vmem(2, 2, 2, 3, full),
                vmem(4, 2, 2, 3, full),
                vmem(4, 2, 2, 3, full),
                vmem(3, 2, 2, 3, pad),
                vmem(2, 2, 3, 3, full),
                vmem(6, 2, 2, 3, full),
                vmem(full * 16),
                vmem(full * 16),
                vmem(18 * 8),
                vmem(own, 2),
                vmem(full, 2),
                vmem(gz, 2),
                pltpu.SemaphoreType.DMA((2,)),
                pltpu.SemaphoreType.DMA((n_send,)),
                pltpu.SemaphoreType.DMA((n_recv,)),
                pltpu.SemaphoreType.REGULAR((max(ta // 2, 1),)),
                pltpu.SemaphoreType.REGULAR((max(gz // 2, 1),)),
            ],
            compiler_params=pltpu.CompilerParams(
                collective_id=0, has_side_effects=True, vmem_limit_bytes=56_450_000
            ),
        )(sp, tl)
        return polyakov, means[:, 0]

    return jax.shard_map(
        body,
        mesh=mesh,
        in_specs=(
            P("cfg", None, None, None, "ta", "gz", "gy", None),
            P("cfg", None, None, "ta", "gz", "gy", None),
        ),
        out_specs=(P("cfg", "gz", "gy", None), P("cfg")),
        check_vma=False,
    )
```

```python
import functools

import jax
import jax.numpy as jnp
from jax import lax
from jax.experimental import pallas as pl
from jax.experimental.pallas import tpu as pltpu
from jax.sharding import PartitionSpec as P

MESH = pl.DeviceIdType.MESH
F32 = jnp.float32
STEPS = 3
FLOOR = 0.25
FX, FY, FZ, FV = 0, 1, 2, 3


def third_row(m):
    (a_re, b_re), (a_im, b_im) = m[0][:2], m[1][:2]
    re, im = [], []
    for k in range(3):
        p, q = (k + 1) % 3, (k + 2) % 3
        re.append(
            a_re[p] * b_re[q] - a_im[p] * b_im[q] - (a_re[q] * b_re[p] - a_im[q] * b_im[p])
        )
        im.append(
            (a_re[q] * b_im[p] + a_im[q] * b_re[p]) - (a_re[p] * b_im[q] + a_im[p] * b_re[q])
        )
    return [m[0][0], m[0][1], re], [m[1][0], m[1][1], im]


def load(ref, lead, rows, count=3):
    return tuple(
        [[ref[(*lead, part, i, j, rows)] for j in range(3)] for i in range(count)]
        for part in range(2)
    )


def load2(ref, lead, rows):
    return third_row(load(ref, lead, rows, 2))


def store(ref, lead, rows, m):
    for part in range(2):
        for i, row in enumerate(m[part]):
            for j, v in enumerate(row):
                ref[(*lead, part, i, j, rows)] = v


def mapped(fn, *ms):
    return tuple(
        [[fn(*vs) for vs in zip(*rows)] for rows in zip(*[m[part] for m in ms])]
        for part in range(2)
    )


def add(*ms):
    return mapped(lambda *vs: functools.reduce(lambda a, b: a + b, vs), *ms)


def ahead_x(m):
    return mapped(lambda v: pltpu.roll(v, v.shape[-1] - 1, 1), m)


def back_x(m):
    return mapped(lambda v: pltpu.roll(v, 1, 1), m)


def mul(a, b, da=False, db=False, rows=3):
    out_re, out_im = [], []
    for i in range(rows):
        row_re, row_im = [], []
        for k in range(3):
            re = im = None
            for j in range(3):
                ar, ai = (a[0][j][i], a[1][j][i]) if da else (a[0][i][j], a[1][i][j])
                br, bi = (b[0][k][j], b[1][k][j]) if db else (b[0][j][k], b[1][j][k])
                rr, ii, ri, ir = ar * br, ai * bi, ar * bi, ai * br
                tr = rr + ii if da != db else rr - ii
                if da and db:
                    ti = -(ri + ir)
                elif da:
                    ti = ri - ir
                elif db:
                    ti = ir - ri
                else:
                    ti = ri + ir
                re = tr if re is None else re + tr
                im = ti if im is None else im + ti
            row_re.append(re)
            row_im.append(im)
        out_re.append(row_re)
        out_im.append(row_im)
    return out_re, out_im


def normalized(re, im):
    weight = sum(v * v for v in re) + sum(v * v for v in im)
    scale = lax.rsqrt(jnp.maximum(weight, FLOOR))
    return [v * scale for v in re], [v * scale for v in im]


def project(re, im):
    u_re, u_im = normalized(re[0], im[0])
    in_re = sum(u_re[j] * re[1][j] + u_im[j] * im[1][j] for j in range(3))
    in_im = sum(u_re[j] * im[1][j] - u_im[j] * re[1][j] for j in range(3))
    w_re = [re[1][j] - (in_re * u_re[j] - in_im * u_im[j]) for j in range(3)]
    w_im = [im[1][j] - (in_re * u_im[j] + in_im * u_re[j]) for j in range(3)]
    v_re, v_im = normalized(w_re, w_im)
    return third_row(([u_re, v_re], [u_im, v_im]))


def mixed(link, staples, weight):
    re = [[0.5 * link[0][i][j] + weight * staples[0][i][j] for j in range(3)] for i in range(2)]
    im = [[0.5 * link[1][i][j] + weight * staples[1][i][j] for j in range(3)] for i in range(2)]
    return project(re, im)


def kernel(
    ta, gz, half,
    sp, tl, pol, mean,
    SP, TL, F, T, H, TH, UP, S, L, AB, M, sm, ar, tree, pb, bc, zs,
    local_sem, send_sem, recv_sem, ready_x, ready_z,
):
    def wrapped(v, n):
        return jnp.where(v >= n, v - n, v)

    j, z, h = lax.axis_index("ta"), lax.axis_index("gz"), lax.axis_index("gy")
    o = 1 - h
    zp, zm = wrapped(z + 1, gz), wrapped(z + gz - 1, gz)
    full = 2 * half
    nd = 2 * ta
    own = full // nd
    me = 2 * j + h
    mine = pl.ds(pl.multiple_of(h * half, half), half)
    halves = [pl.ds(k * half, half) for k in range(2)]

    sent = []
    n_sem = [0, 0]

    def remote(src, dst, recv_index, **where):
        k = n_sem[0]
        n_sem[0] += 1
        copy = pltpu.make_async_remote_copy(
            src_ref=src, dst_ref=dst, send_sem=send_sem.at[k], recv_sem=recv_sem.at[recv_index],
            device_id=where, device_id_type=MESH,
        )
        copy.start()
        sent.append(copy)

    def arrived(dst, recv_index):
        pltpu.make_async_remote_copy(
            src_ref=dst, dst_ref=dst, send_sem=send_sem.at[0], recv_sem=recv_sem.at[recv_index],
            device_id={"gy": o}, device_id_type=MESH,
        ).wait_recv()

    def new_recv(n=1):
        k = n_sem[1]
        n_sem[1] += n
        return k

    near = [
        pltpu.make_async_copy(sp, SP, local_sem.at[2]),
        pltpu.make_async_copy(tl, TL, local_sem.at[3]),
        pltpu.make_async_copy(sp.at[:, :, :, :, h, 0], F.at[0, 0:3, :, :, :, mine], local_sem.at[0]),
        pltpu.make_async_copy(tl.at[:, :, :, h, 0], T.at[:, :, :, mine], local_sem.at[1]),
    ]
    for copy in near:
        copy.start()

    barrier = pltpu.get_barrier_semaphore()
    around = sorted({(0, 1 % gz), (0, (gz - 1) % gz), (1 % ta, 0), ((ta - 1) % ta, 0)} - {(0, 0)})

    def place(dx, dz):
        return {"ta": wrapped(j + dx, ta), "gz": wrapped(z + dz, gz)}

    def signal(sem, **where):
        pl.semaphore_signal(sem, inc=1, device_id=where, device_id_type=MESH)

    signal(barrier, gy=o)
    for dx, dz in around:
        for c in range(2):
            signal(barrier, **place(dx, dz), gy=c)
    near[0].wait()
    pl.semaphore_wait(barrier, 1 + 2 * len(around))

    def relay(sem, rounds, sides):
        done = [0]

        def go(last=False):
            while True:
                if 0 < done[0] <= rounds:
                    pl.semaphore_wait(sem.at[done[0] - 1], len(sides))
                done[0] += 1
                if done[0] <= rounds:
                    for where in sides:
                        signal(sem.at[done[0] - 1], **where)
                if not last or done[0] > rounds:
                    return

        return go

    hear_x = relay(
        ready_x, ta // 2 - 1, [{"ta": wrapped(j + k, ta)} for k in sorted({1 % ta, ta - 1} - {0})]
    )
    hear_z = relay(
        ready_z, gz // 2 - STEPS, [{"gz": wrapped(z + k, gz)} for k in sorted({1 % gz, gz - 1} - {0})]
    )

    r_v, r_x, r_y, r_t = new_recv(2), new_recv(4), new_recv(4), new_recv(4)
    r_own, r_ownt = new_recv(), new_recv()

    def plane(f, t):
        return SP.at[f, :, 0:2, :, t, 0] if f is not None else TL.at[:, 0:2, :, t, 0]

    def two(ref, *lead):
        return ref.at[(*lead, slice(None), slice(0, 2), slice(None), mine)]

    for t in range(2):
        remote(plane(FZ, t), two(F, 0, FV), r_v + h, gz=zp, gy=t)
    remote(SP.at[:, :, :, :, o, 0], F.at[0, 0:3, :, :, :, mine], r_own, gy=o)
    for f, r in ((FX, r_x), (FY, r_y)):
        for t in range(2):
            remote(plane(f, t), two(H, 0, 0, f), r + h, gz=zm, gy=t)
            remote(plane(f, t), two(H, 0, 1, f), r + 2 + h, gz=zp, gy=t)
    near[1].wait()
    remote(TL.at[:, :, :, o, 0], T.at[:, :, :, mine], r_ownt, gy=o)
    for t in range(2):
        remote(plane(None, t), two(TH, 0), r_t + h, gz=zm, gy=t)
    hear_x()

    def each_half(body):
        def run(k, carry):
            r0 = pl.multiple_of(k * half, half)
            body(pl.ds(r0, half), pl.ds(r0 + 1, half))
            return carry

        lax.fori_loop(0, 2, run, 0)

    def wrap(ref, *lead):
        ref[(*lead, slice(None), slice(None), slice(None), pl.ds(full, 1))] = ref[
            (*lead, slice(None), slice(None), slice(None), pl.ds(0, 1))
        ]

    def unwrap(k):
        L[k, :, :, :, pl.ds(0, 1)] = L[k, :, :, :, pl.ds(full, 1)]

    def in_plane(s):
        def body(rows, up):
            ux, uy = load(F, (s, FX), rows), load(F, (s, FY), rows)
            uy_x, ux_y = ahead_x(uy), load(F, (s, FX), up)
            c, d = mul(ux, uy_x), mul(uy, ux_y)
            store(S, (FX,), rows, mul(d, uy_x, db=True, rows=2))
            store(L, (0,), up, mul(uy, c, da=True, rows=2))
            store(
                S, (FY,), rows,
                add(mul(c, ux_y, db=True, rows=2), back_x(mul(ux, d, da=True, rows=2))),
            )

        each_half(body)
        unwrap(0)

    def side(ref, s, f, rows, up):
        return ahead_x(load(ref, (s, f), rows)) if up is None else load(ref, (s, f), up)

    def across(s, f, k):
        def body(rows, up):
            up = None if f == FX else up
            uz, uz_f = load(F, (s, FZ), rows), side(F, s, FZ, rows, up)
            a = mul(uz, load2(H, (s, 0, f), rows))
            store(AB, (0,), rows, a)
            total = add(load(S, (f,), rows, 2), mul(a, uz_f, db=True, rows=2))
            uv, uv_f = load(F, (s, FV), rows), side(F, s, FV, rows, up)
            b = mul(load2(H, (s, 1, f), rows), uv_f)
            store(AB, (1,), rows, b)
            total = add(total, mul(uv, b, da=True, rows=2))
            if f == FX:
                total = add(total, load(L, (0,), rows, 2))
            store(F, (s + 1, f), rows, mixed(load(F, (s, f), rows, 2), total, 0.125))

        body(halves[k], pl.ds(k * half + 1, half))

    def z_staples(s, f):
        def body(rows, up):
            shift = None if f == FX else up
            uf = load(F, (s, f), rows)
            b = mul(uf, side(F, s, FZ, rows, shift), rows=2)
            upper = mul(b, load2(H, (s, 0, f), rows), db=True, rows=2)
            lower = mul(uf, load(AB, (0,), rows), da=True, rows=2)
            below = load2(H, (s, 1, f), rows)
            v_upper = mul(load(AB, (1,), rows), uf, db=True, rows=2)
            v_lower = mul(mul(below, load(F, (s, FV), rows), da=True, rows=2), uf, rows=2)
            if f == FX:
                store(S, (FZ,), rows, add(upper, back_x(lower)))
                store(S, (FV,), rows, add(v_upper, back_x(v_lower)))
            else:
                store(L, (1,), up, lower)
                store(L, (2,), up, v_lower)
                store(S, (FZ,), rows, add(load(S, (FZ,), rows, 2), upper))
                store(S, (FV,), rows, add(load(S, (FV,), rows, 2), v_upper))

        each_half(body)
        if f == FY:
            unwrap(1)
            unwrap(2)

    def z_links(s, last):
        for f, k in ((FZ, 1), (FV, 2)):
            for part in range(2):
                rows = halves[part]
                total = add(load(S, (f,), rows, 2), load(L, (k,), rows, 2))
                store(F, (s + 1, f), rows, mixed(load(F, (s, f), rows, 2), total, 0.125))
                if last:
                    onward(s + 1, f, part)
        wrap(F, s + 1, FZ)
        wrap(F, s + 1, FV)

    for copy in near[2:]:
        copy.wait()
    other = pl.ds(pl.multiple_of(o * half, half), half)
    arrived(F.at[0, 0:3, :, :, :, other], r_own)
    wrap(F, 0, FX)
    wrap(F, 0, FZ)
    in_plane(0)
    for k in range(2):
        arrived(F.at[0, FV, :, 0:2, :, halves[k]], r_v + k)

    def complete(rows, up):
        store(F, (0, FV), rows, load2(F, (0, FV), rows))

    each_half(complete)
    wrap(F, 0, FV)

    r_next = new_recv(8)

    def onward(s, f, k):
        remote(
            F.at[s, f, :, 0:2, :, halves[k]], UP.at[f, :, :, :, halves[k]], r_next + 2 * f + k,
            ta=wrapped(j + h + ta - 1, ta), gy=o,
        )

    def next_arrived(f, k):
        arrived(UP.at[f, :, :, :, halves[k]], r_next + 2 * f + k)

    r_now = {FX: r_x, FY: r_y}
    for s in range(STEPS):
        last = s == STEPS - 1
        r_then = {f: new_recv(4) for f in (FX, FY)} if not last else {}
        for f in (FX, FY):
            for k in range(2):
                for side_k in range(2):
                    arrived(H.at[s, side_k, f, :, :, :, halves[k]], r_now[f] + 2 * side_k + k)
                across(s, f, k)
                if last:
                    onward(s + 1, f, k)
                else:
                    out = F.at[s + 1, f, :, 0:2, :, halves[k]]
                    for side_k, to in ((0, zm), (1, zp)):
                        remote(
                            out, H.at[s + 1, side_k, f, :, :, :, halves[k]],
                            r_then[f] + 2 * side_k + k, gz=to,
                        )
            if f == FX:
                wrap(F, s + 1, FX)
            else:
                hear_x(last)
            if last:
                hear_z()
            z_staples(s, f)
        r_now = r_then
        if s == STEPS - 2:
            for t in range(2):
                remote(plane(None, t), two(TH, 1), r_t + 2 + h, gz=zp, gy=t)
        z_links(s, last)
        if not last:
            in_plane(s + 1)

    n = STEPS
    arrived(T.at[:, :, :, other], r_ownt)
    wrap(T)
    for side_k in range(2):
        for k in range(2):
            arrived(TH.at[side_k, :, :, :, halves[k]], r_t + 2 * side_k + k)

    def before(rows, up):
        t = load(T, (), rows)
        ux, uy = load(F, (n, FX), rows), load(F, (n, FY), rows)
        store(M, (0,), rows, mul(ux, ahead_x(t), rows=2))
        store(M, (1,), rows, mul(ux, t, da=True, rows=2))
        store(M, (2,), rows, mul(uy, load(T, (), up), rows=2))
        store(M, (3,), rows, mul(uy, t, da=True, rows=2))
        store(M, (4,), rows, mul(load(F, (n, FZ), rows), load2(TH, (0,), rows), rows=2))
        store(
            M, (5,), rows, mul(load(F, (n, FV), rows), load2(TH, (1,), rows), da=True, rows=2)
        )

    each_half(before)
    hear_z()
    for k in range(2):
        next_arrived(FX, k)
    for k in range(2):
        next_arrived(FY, k)

    def along_xy(rows, up):
        ux, uy = load2(UP, (FX,), rows), load2(UP, (FY,), rows)
        total = add(
            mul(load(M, (0,), rows, 2), ux, db=True, rows=2),
            back_x(mul(load(M, (1,), rows, 2), ux, rows=2)),
            mul(load(M, (2,), rows, 2), uy, db=True, rows=2),
        )
        store(S, (0,), rows, total)
        store(L, (0,), up, mul(load(M, (3,), rows, 2), uy, rows=2))

    each_half(along_xy)
    hear_z()
    unwrap(0)
    for k in range(2):
        next_arrived(FZ, k)
    for k in range(2):
        next_arrived(FV, k)

    def finish(k, carry):
        r0 = pl.multiple_of(k * half, half)
        rows = pl.ds(r0, half)
        uz, uv = load2(UP, (FZ,), rows), load2(UP, (FV,), rows)
        total = add(
            load(S, (0,), rows, 2),
            load(L, (0,), rows, 2),
            mul(load(M, (4,), rows, 2), uz, db=True, rows=2),
            mul(load(M, (5,), rows, 2), uv, rows=2),
        )
        done = mixed(load(T, (), rows, 2), total, 0.5 / 6.0)
        for part in range(2):
            for a in range(2):
                for b in range(3):
                    sm[pl.ds(r0 * 16 + part * 6 + a * 3 + b, half, 16), :] = done[part][a][b]
        return carry

    lax.fori_loop(0, 2, finish, 0)

    span = own * 16
    sm3, ar3 = sm.reshape(full, 16, sm.shape[-1]), ar.reshape(full, 16, sm.shape[-1])
    r_row = new_recv(nd)
    offsets = sorted(range(1, nd), key=lambda k: -min(k // 2, ta - k // 2))
    here = pl.ds(me * own, own)

    def part_of(ref, d):
        return ref.at[pl.ds(d * own, own), 0:12]

    for k in offsets:
        dj, dh = wrapped(j + k // 2, ta), (h if k % 2 == 0 else o)
        remote(part_of(sm3, 2 * dj + dh), part_of(ar3, me), r_row + me, ta=dj, gy=dh)
    hear_z()
    ar3[here] = sm3[here]
    for k in range(1, nd):
        d = wrapped(me + k, nd)
        arrived(part_of(ar3, d), r_row + d)

    def slices(start, stride, rows):
        at = lambda c: ar[pl.ds(start + c, rows, stride), :]
        return third_row(
            tuple([[at(part * 6 + a * 3 + b) for b in range(3)] for a in range(2)] for part in range(2))
        )

    for row in range(own):
        rows = nd // 2
        lhs, rhs = slices(row * 16, 2 * span, rows), slices(row * 16 + span, 2 * span, rows)
        while rows > 1:
            prod = mul(lhs, rhs)
            flat = [v for part in prod for line in part for v in line]
            for c, v in enumerate(flat):
                tree[pl.ds(c * 8, rows), :] = v
            rows //= 2
            pick = lambda first: [tree[pl.ds(c * 8 + first, rows, 2), :] for c in range(18)]
            grid = lambda vs: tuple(
                [[vs[part * 9 + a * 3 + b] for b in range(3)] for a in range(3)] for part in range(2)
            )
            lhs, rhs = grid(pick(0)), grid(pick(1))
        re = im = None
        for a in range(3):
            for b in range(3):
                lr, li, rr, ri = lhs[0][a][b], lhs[1][a][b], rhs[0][b][a], rhs[1][b][a]
                t_re, t_im = lr * rr - li * ri, lr * ri + li * rr
                re = t_re if re is None else re + t_re
                im = t_im if im is None else im + t_im
        pb[row, 0:1, :] = re / 3.0
        pb[row, 1:2, :] = im / 3.0

    hear_z(True)
    r_out = new_recv(nd)
    home = pl.ds(me * own, own)
    for k in offsets:
        remote(
            pb, bc.at[home], r_out + me, ta=wrapped(j + k // 2, ta), gy=h if k % 2 == 0 else o
        )
    bc[home] = pb[...]
    for k in range(1, nd):
        d = wrapped(me + k, nd)
        arrived(bc.at[pl.ds(d * own, own)], r_out + d)

    sums = jnp.sum(bc[...], axis=0)
    zs[z] = sums
    r_sum = new_recv(gz)
    for k in sorted(range(1, gz), key=lambda k: -min(k, gz - k)):
        remote(zs.at[z], zs.at[z], r_sum + z, gz=wrapped(z + k, gz))
    for k in range(half):
        pol[:, 0, k, :] = bc[h * half + k]
    for k in range(1, gz):
        d = wrapped(z + k, gz)
        arrived(zs.at[d], r_sum + d)
    totals = jnp.sum(zs[...], axis=0)
    sites = float(full * gz * sp.shape[-1])
    mean[...] = jnp.broadcast_to(jnp.sum(totals, axis=1, keepdims=True) / sites, totals.shape)

    for copy in sent:
        copy.wait_send()


def solution(mesh):
    ta, gz = mesh.shape["ta"], mesh.shape["gz"]

    def body(sp, tl):
        half, lanes = sp.shape[-2:]
        full = 2 * half
        pad = full + 8
        nd = 2 * ta
        own = full // nd

        def vmem(*dims):
            return pltpu.VMEM((*dims, lanes), F32)

        n_send = 2 + 1 + 8 + 1 + 4 + 8 * (STEPS - 1) + 8 + 2 * (nd - 1) + gz - 1
        n_recv = 2 + 4 + 4 + 4 + 2 + 8 + 8 * (STEPS - 1) + 2 * nd + gz
        polyakov, means = pl.pallas_call(
            functools.partial(kernel, ta, gz, half),
            out_shape=(
                jax.ShapeDtypeStruct((2, 1, half, lanes), F32),
                jax.ShapeDtypeStruct((2, lanes), F32),
            ),
            in_specs=[pl.BlockSpec(memory_space=pltpu.HBM)] * 2,
            out_specs=(pl.BlockSpec(memory_space=pltpu.VMEM),) * 2,
            scratch_shapes=[
                pltpu.VMEM(sp.shape, F32),
                pltpu.VMEM(tl.shape, F32),
                vmem(STEPS + 1, 4, 2, 3, 3, pad),
                vmem(2, 3, 3, pad),
                vmem(STEPS, 2, 2, 2, 2, 3, full),
                vmem(2, 2, 2, 3, full),
                vmem(4, 2, 2, 3, full),
                vmem(4, 2, 2, 3, full),
                vmem(3, 2, 2, 3, pad),
                vmem(2, 2, 3, 3, full),
                vmem(6, 2, 2, 3, full),
                vmem(full * 16),
                vmem(full * 16),
                vmem(18 * 8),
                vmem(own, 2),
                vmem(full, 2),
                vmem(gz, 2),
                pltpu.SemaphoreType.DMA((4,)),
                pltpu.SemaphoreType.DMA((n_send,)),
                pltpu.SemaphoreType.DMA((n_recv,)),
                pltpu.SemaphoreType.REGULAR((max(ta // 2, 1),)),
                pltpu.SemaphoreType.REGULAR((max(gz // 2, 1),)),
            ],
            compiler_params=pltpu.CompilerParams(
                collective_id=0, has_side_effects=True, vmem_limit_bytes=56_450_000
            ),
        )(sp, tl)
        return polyakov, means[:, 0]

    return jax.shard_map(
        body,
        mesh=mesh,
        in_specs=(
            P("cfg", None, None, None, "ta", "gz", "gy", None),
            P("cfg", None, None, "ta", "gz", "gy", None),
        ),
        out_specs=(P("cfg", "gz", "gy", None), P("cfg")),
        check_vma=False,
    )
```

```python
import functools
import math

import jax
import jax.numpy as jnp
from jax import lax
from jax.experimental import pallas as pl
from jax.experimental.pallas import tpu as pltpu
from jax.sharding import PartitionSpec as P

MESH = pl.DeviceIdType.MESH
F32 = jnp.float32
STEPS = 3
FLOOR = 0.25
FX, FY, FZ, FV = 0, 1, 2, 3


def third_row(m):
    (a_re, b_re), (a_im, b_im) = m[0][:2], m[1][:2]
    re, im = [], []
    for k in range(3):
        p, q = (k + 1) % 3, (k + 2) % 3
        re.append(
            a_re[p] * b_re[q] - a_im[p] * b_im[q] - (a_re[q] * b_re[p] - a_im[q] * b_im[p])
        )
        im.append(
            (a_re[q] * b_im[p] + a_im[q] * b_re[p]) - (a_re[p] * b_im[q] + a_im[p] * b_re[q])
        )
    return [m[0][0], m[0][1], re], [m[1][0], m[1][1], im]


def load(ref, lead, rows, count=3):
    return tuple(
        [[ref[(*lead, part, i, j, rows)] for j in range(3)] for i in range(count)]
        for part in range(2)
    )


def load2(ref, lead, rows):
    return third_row(load(ref, lead, rows, 2))


def store(ref, lead, rows, m):
    for part in range(2):
        for i, row in enumerate(m[part]):
            for j, v in enumerate(row):
                ref[(*lead, part, i, j, rows)] = v


def mapped(fn, *ms):
    return tuple(
        [[fn(*vs) for vs in zip(*rows)] for rows in zip(*[m[part] for m in ms])]
        for part in range(2)
    )


def add(*ms):
    return mapped(lambda *vs: functools.reduce(lambda a, b: a + b, vs), *ms)


def ahead_x(m):
    return mapped(lambda v: pltpu.roll(v, v.shape[-1] - 1, 1), m)


def back_x(m):
    return mapped(lambda v: pltpu.roll(v, 1, 1), m)


def mul(a, b, da=False, db=False, rows=3):
    out_re, out_im = [], []
    for i in range(rows):
        row_re, row_im = [], []
        for k in range(3):
            re = im = None
            for j in range(3):
                ar, ai = (a[0][j][i], a[1][j][i]) if da else (a[0][i][j], a[1][i][j])
                br, bi = (b[0][k][j], b[1][k][j]) if db else (b[0][j][k], b[1][j][k])
                rr, ii, ri, ir = ar * br, ai * bi, ar * bi, ai * br
                tr = rr + ii if da != db else rr - ii
                if da and db:
                    ti = -(ri + ir)
                elif da:
                    ti = ri - ir
                elif db:
                    ti = ir - ri
                else:
                    ti = ri + ir
                re = tr if re is None else re + tr
                im = ti if im is None else im + ti
            row_re.append(re)
            row_im.append(im)
        out_re.append(row_re)
        out_im.append(row_im)
    return out_re, out_im


def normalized(re, im):
    weight = sum(v * v for v in re) + sum(v * v for v in im)
    scale = lax.rsqrt(jnp.maximum(weight, FLOOR))
    return [v * scale for v in re], [v * scale for v in im]


def project(re, im):
    u_re, u_im = normalized(re[0], im[0])
    in_re = sum(u_re[j] * re[1][j] + u_im[j] * im[1][j] for j in range(3))
    in_im = sum(u_re[j] * im[1][j] - u_im[j] * re[1][j] for j in range(3))
    w_re = [re[1][j] - (in_re * u_re[j] - in_im * u_im[j]) for j in range(3)]
    w_im = [im[1][j] - (in_re * u_im[j] + in_im * u_re[j]) for j in range(3)]
    v_re, v_im = normalized(w_re, w_im)
    return third_row(([u_re, v_re], [u_im, v_im]))


def mixed(link, staples, weight):
    re = [[0.5 * link[0][i][j] + weight * staples[0][i][j] for j in range(3)] for i in range(2)]
    im = [[0.5 * link[1][i][j] + weight * staples[1][i][j] for j in range(3)] for i in range(2)]
    return project(re, im)


def kernel(
    ta, gz, half,
    sp, tl, pol, mean,
    SP, TL, F, T, H, TH, UP, S, L, AB, M, sm, ar, tree, pb, bc, zs,
    local_sem, send_sem, recv_sem, ready_x, ready_z,
):
    def wrapped(v, n):
        return jnp.where(v >= n, v - n, v)

    j, z, h = lax.axis_index("ta"), lax.axis_index("gz"), lax.axis_index("gy")
    o = 1 - h
    zp, zm = wrapped(z + 1, gz), wrapped(z + gz - 1, gz)
    full = 2 * half
    nd = 2 * ta
    own = full // nd
    me = 2 * j + h
    mine = pl.ds(pl.multiple_of(h * half, half), half)
    halves = [pl.ds(k * half, half) for k in range(2)]

    rows_sent = [0]
    n_recv = [0]

    def remote(src, dst, recv_index, **where):
        pltpu.make_async_remote_copy(
            src_ref=src, dst_ref=dst, send_sem=send_sem, recv_sem=recv_sem.at[recv_index],
            device_id=where, device_id_type=MESH,
        ).start()
        rows_sent[0] += math.prod(src.shape[:-1])

    def arrived(dst, recv_index):
        pltpu.make_async_remote_copy(
            src_ref=dst, dst_ref=dst, send_sem=send_sem, recv_sem=recv_sem.at[recv_index],
            device_id={"gy": o}, device_id_type=MESH,
        ).wait_recv()

    def new_recv(n=1):
        k = n_recv[0]
        n_recv[0] += n
        return k

    near = [
        pltpu.make_async_copy(sp, SP, local_sem.at[2]),
        pltpu.make_async_copy(tl, TL, local_sem.at[3]),
        pltpu.make_async_copy(sp.at[:, :, :, :, h, 0], F.at[0, 0:3, :, :, :, mine], local_sem.at[0]),
        pltpu.make_async_copy(tl.at[:, :, :, h, 0], T.at[:, :, :, mine], local_sem.at[1]),
    ]
    for copy in near:
        copy.start()

    barrier = pltpu.get_barrier_semaphore()
    around = sorted({(0, 1 % gz), (0, gz - 1), (1 % ta, 0), (ta - 1, 0)} - {(0, 0)})

    def place(dx, dz):
        return {"ta": wrapped(j + dx, ta), "gz": wrapped(z + dz, gz)}

    def signal(sem, **where):
        pl.semaphore_signal(sem, inc=1, device_id=where, device_id_type=MESH)

    signal(barrier, gy=o)
    for dx, dz in around:
        for c in range(2):
            signal(barrier, **place(dx, dz), gy=c)
    near[0].wait()
    pl.semaphore_wait(barrier, 1 + 2 * len(around))

    def relay(sem, rounds, sides):
        done = [0]

        def go(last=False):
            while True:
                if 0 < done[0] <= rounds:
                    pl.semaphore_wait(sem.at[done[0] - 1], len(sides))
                done[0] += 1
                if done[0] <= rounds:
                    for where in sides:
                        signal(sem.at[done[0] - 1], **where)
                if not last or done[0] > rounds:
                    return

        return go

    hear_x = relay(
        ready_x, ta // 2 - 1, [{"ta": wrapped(j + k, ta)} for k in sorted({1 % ta, ta - 1} - {0})]
    )
    hear_z = relay(
        ready_z, gz // 2 - STEPS, [{"gz": wrapped(z + k, gz)} for k in sorted({1 % gz, gz - 1} - {0})]
    )

    r_v, r_x, r_y, r_t = new_recv(2), new_recv(2), new_recv(2), new_recv(2)
    r_own, r_ownt = new_recv(), new_recv()

    def plane(f, t):
        return SP.at[f, :, 0:2, :, t, 0] if f is not None else TL.at[:, 0:2, :, t, 0]

    def two(ref, *lead):
        return ref.at[(*lead, slice(None), slice(0, 2), slice(None), mine)]

    for t in range(2):
        remote(plane(FZ, t), two(F, 0, FV), r_v + h, gz=zp, gy=t)
    remote(SP.at[:, :, :, :, o, 0], F.at[0, 0:3, :, :, :, mine], r_own, gy=o)
    for f, r in ((FX, r_x), (FY, r_y)):
        for t in range(2):
            remote(plane(f, t), two(H, 0, 0, f), r + h, gz=zm, gy=t)
            remote(plane(f, t), two(H, 0, 1, f), r + h, gz=zp, gy=t)
    near[1].wait()
    remote(TL.at[:, :, :, o, 0], T.at[:, :, :, mine], r_ownt, gy=o)
    for t in range(2):
        remote(plane(None, t), two(TH, 0), r_t + h, gz=zm, gy=t)
    hear_x()

    def each_half(body):
        def run(k, carry):
            r0 = pl.multiple_of(k * half, half)
            body(pl.ds(r0, half), pl.ds(r0 + 1, half))
            return carry

        lax.fori_loop(0, 2, run, 0)

    def wrap(ref, *lead):
        ref[(*lead, slice(None), slice(None), slice(None), pl.ds(full, 1))] = ref[
            (*lead, slice(None), slice(None), slice(None), pl.ds(0, 1))
        ]

    def unwrap(k):
        L[k, :, :, :, pl.ds(0, 1)] = L[k, :, :, :, pl.ds(full, 1)]

    def in_plane(s):
        def body(rows, up):
            ux, uy = load(F, (s, FX), rows), load(F, (s, FY), rows)
            uy_x, ux_y = ahead_x(uy), load(F, (s, FX), up)
            c, d = mul(ux, uy_x), mul(uy, ux_y)
            store(S, (FX,), rows, mul(d, uy_x, db=True, rows=2))
            store(L, (0,), up, mul(uy, c, da=True, rows=2))
            store(
                S, (FY,), rows,
                add(mul(c, ux_y, db=True, rows=2), back_x(mul(ux, d, da=True, rows=2))),
            )

        each_half(body)
        unwrap(0)

    def side(ref, s, f, rows, up):
        return ahead_x(load(ref, (s, f), rows)) if up is None else load(ref, (s, f), up)

    def across(s, f, k):
        def body(rows, up):
            up = None if f == FX else up
            uz, uz_f = load(F, (s, FZ), rows), side(F, s, FZ, rows, up)
            a = mul(uz, load2(H, (s, 0, f), rows))
            store(AB, (0,), rows, a)
            total = add(load(S, (f,), rows, 2), mul(a, uz_f, db=True, rows=2))
            uv, uv_f = load(F, (s, FV), rows), side(F, s, FV, rows, up)
            b = mul(load2(H, (s, 1, f), rows), uv_f)
            store(AB, (1,), rows, b)
            total = add(total, mul(uv, b, da=True, rows=2))
            if f == FX:
                total = add(total, load(L, (0,), rows, 2))
            store(F, (s + 1, f), rows, mixed(load(F, (s, f), rows, 2), total, 0.125))

        body(halves[k], pl.ds(k * half + 1, half))

    def z_staples(s, f):
        def body(rows, up):
            shift = None if f == FX else up
            uf = load(F, (s, f), rows)
            b = mul(uf, side(F, s, FZ, rows, shift), rows=2)
            upper = mul(b, load2(H, (s, 0, f), rows), db=True, rows=2)
            lower = mul(uf, load(AB, (0,), rows), da=True, rows=2)
            below = load2(H, (s, 1, f), rows)
            v_upper = mul(load(AB, (1,), rows), uf, db=True, rows=2)
            v_lower = mul(mul(below, load(F, (s, FV), rows), da=True, rows=2), uf, rows=2)
            if f == FX:
                store(S, (FZ,), rows, add(upper, back_x(lower)))
                store(S, (FV,), rows, add(v_upper, back_x(v_lower)))
            else:
                store(L, (1,), up, lower)
                store(L, (2,), up, v_lower)
                store(S, (FZ,), rows, add(load(S, (FZ,), rows, 2), upper))
                store(S, (FV,), rows, add(load(S, (FV,), rows, 2), v_upper))

        each_half(body)
        if f == FY:
            unwrap(1)
            unwrap(2)

    def z_links(s, last):
        for f, k in ((FZ, 1), (FV, 2)):
            for part in range(2):
                rows = halves[part]
                total = add(load(S, (f,), rows, 2), load(L, (k,), rows, 2))
                store(F, (s + 1, f), rows, mixed(load(F, (s, f), rows, 2), total, 0.125))
                if last:
                    onward(s + 1, f, part)
        wrap(F, s + 1, FZ)
        wrap(F, s + 1, FV)

    for copy in near[2:]:
        copy.wait()
    other = pl.ds(pl.multiple_of(o * half, half), half)
    arrived(F.at[0, 0:3, :, :, :, other], r_own)
    wrap(F, 0, FX)
    wrap(F, 0, FZ)
    in_plane(0)
    for k in range(2):
        arrived(F.at[0, FV, :, 0:2, :, halves[k]], r_v + k)

    def complete(rows, up):
        store(F, (0, FV), rows, load2(F, (0, FV), rows))

    each_half(complete)
    wrap(F, 0, FV)

    r_next = new_recv(4)

    def onward(s, f, k):
        remote(
            F.at[s, f, :, 0:2, :, halves[k]], UP.at[f, :, :, :, halves[k]], r_next + f,
            ta=wrapped(j + h + ta - 1, ta), gy=o,
        )

    r_now = {FX: r_x, FY: r_y}
    for s in range(STEPS):
        last = s == STEPS - 1
        r_then = {f: new_recv(2) for f in (FX, FY)} if not last else {}
        for f in (FX, FY):
            for k in range(2):
                arrived(H.at[s, :, f, :, :, :, halves[k]], r_now[f] + k)
                across(s, f, k)
                if last:
                    onward(s + 1, f, k)
                else:
                    out = F.at[s + 1, f, :, 0:2, :, halves[k]]
                    for side_k, to in ((0, zm), (1, zp)):
                        remote(
                            out, H.at[s + 1, side_k, f, :, :, :, halves[k]],
                            r_then[f] + k, gz=to,
                        )
            if f == FX:
                wrap(F, s + 1, FX)
            else:
                hear_x(last)
            if last:
                hear_z()
            z_staples(s, f)
        r_now = r_then
        if s == STEPS - 2:
            for t in range(2):
                remote(plane(None, t), two(TH, 1), r_t + h, gz=zp, gy=t)
        z_links(s, last)
        if not last:
            in_plane(s + 1)

    n = STEPS
    arrived(T.at[:, :, :, other], r_ownt)
    wrap(T)
    for k in range(2):
        arrived(TH.at[:, :, :, :, halves[k]], r_t + k)

    def before(rows, up):
        t = load(T, (), rows)
        ux, uy = load(F, (n, FX), rows), load(F, (n, FY), rows)
        store(M, (0,), rows, mul(ux, ahead_x(t), rows=2))
        store(M, (1,), rows, mul(ux, t, da=True, rows=2))
        store(M, (2,), rows, mul(uy, load(T, (), up), rows=2))
        store(M, (3,), rows, mul(uy, t, da=True, rows=2))
        store(M, (4,), rows, mul(load(F, (n, FZ), rows), load2(TH, (0,), rows), rows=2))
        store(
            M, (5,), rows, mul(load(F, (n, FV), rows), load2(TH, (1,), rows), da=True, rows=2)
        )

    each_half(before)
    hear_z()
    arrived(UP.at[FX], r_next + FX)
    arrived(UP.at[FY], r_next + FY)

    def along_xy(rows, up):
        ux, uy = load2(UP, (FX,), rows), load2(UP, (FY,), rows)
        total = add(
            mul(load(M, (0,), rows, 2), ux, db=True, rows=2),
            back_x(mul(load(M, (1,), rows, 2), ux, rows=2)),
            mul(load(M, (2,), rows, 2), uy, db=True, rows=2),
        )
        store(S, (0,), rows, total)
        store(L, (0,), up, mul(load(M, (3,), rows, 2), uy, rows=2))

    each_half(along_xy)
    hear_z()
    unwrap(0)
    arrived(UP.at[FZ], r_next + FZ)
    arrived(UP.at[FV], r_next + FV)

    def finish(k, carry):
        r0 = pl.multiple_of(k * half, half)
        rows = pl.ds(r0, half)
        uz, uv = load2(UP, (FZ,), rows), load2(UP, (FV,), rows)
        total = add(
            load(S, (0,), rows, 2),
            load(L, (0,), rows, 2),
            mul(load(M, (4,), rows, 2), uz, db=True, rows=2),
            mul(load(M, (5,), rows, 2), uv, rows=2),
        )
        done = mixed(load(T, (), rows, 2), total, 0.5 / 6.0)
        for part in range(2):
            for a in range(2):
                for b in range(3):
                    sm[pl.ds(r0 * 16 + part * 6 + a * 3 + b, half, 16), :] = done[part][a][b]
        return carry

    lax.fori_loop(0, 2, finish, 0)

    span = own * 16
    sm3, ar3 = sm.reshape(full, 16, sm.shape[-1]), ar.reshape(full, 16, sm.shape[-1])
    r_row = new_recv()
    offsets = sorted(range(1, nd), key=lambda k: -min(k // 2, ta - k // 2))
    here = pl.ds(me * own, own)

    def part_of(ref, d):
        return ref.at[pl.ds(d * own, own), 0:12]

    for k in offsets:
        dj, dh = wrapped(j + k // 2, ta), (h if k % 2 == 0 else o)
        remote(part_of(sm3, 2 * dj + dh), part_of(ar3, me), r_row, ta=dj, gy=dh)
    hear_z()
    ar3[here] = sm3[here]
    arrived(ar3.at[pl.ds(0, full - own), 0:12], r_row)

    def slices(start, stride, rows):
        at = lambda c: ar[pl.ds(start + c, rows, stride), :]
        return third_row(
            tuple([[at(part * 6 + a * 3 + b) for b in range(3)] for a in range(2)] for part in range(2))
        )

    for row in range(own):
        rows = nd // 2
        lhs, rhs = slices(row * 16, 2 * span, rows), slices(row * 16 + span, 2 * span, rows)
        while rows > 1:
            prod = mul(lhs, rhs)
            flat = [v for part in prod for line in part for v in line]
            for c, v in enumerate(flat):
                tree[pl.ds(c * 8, rows), :] = v
            rows //= 2
            pick = lambda first: [tree[pl.ds(c * 8 + first, rows, 2), :] for c in range(18)]
            grid = lambda vs: tuple(
                [[vs[part * 9 + a * 3 + b] for b in range(3)] for a in range(3)] for part in range(2)
            )
            lhs, rhs = grid(pick(0)), grid(pick(1))
        re = im = None
        for a in range(3):
            for b in range(3):
                lr, li, rr, ri = lhs[0][a][b], lhs[1][a][b], rhs[0][b][a], rhs[1][b][a]
                t_re, t_im = lr * rr - li * ri, lr * ri + li * rr
                re = t_re if re is None else re + t_re
                im = t_im if im is None else im + t_im
        pb[row, 0:1, :] = re / 3.0
        pb[row, 1:2, :] = im / 3.0

    hear_z(True)
    r_out = new_recv()
    home = pl.ds(me * own, own)
    for k in offsets:
        remote(
            pb, bc.at[home], r_out, ta=wrapped(j + k // 2, ta), gy=h if k % 2 == 0 else o
        )
    bc[home] = pb[...]
    arrived(bc.at[pl.ds(0, full - own)], r_out)

    sums = jnp.sum(bc[...], axis=0)
    zs[z] = sums
    r_sum = new_recv()
    for k in sorted(range(1, gz), key=lambda k: -min(k, gz - k)):
        remote(zs.at[z], zs.at[z], r_sum, gz=wrapped(z + k, gz))
    for k in range(half):
        pol[:, 0, k, :] = bc[h * half + k]
    arrived(zs.at[pl.ds(0, gz - 1)], r_sum)
    totals = jnp.sum(zs[...], axis=0)
    sites = float(full * gz * sp.shape[-1])
    mean[...] = jnp.broadcast_to(jnp.sum(totals, axis=1, keepdims=True) / sites, totals.shape)

    lines = F.reshape(math.prod(F.shape[:-1]), F.shape[-1]).at[pl.ds(0, rows_sent[0])]
    pltpu.make_async_copy(lines, lines, send_sem).wait()


def solution(mesh):
    ta, gz = mesh.shape["ta"], mesh.shape["gz"]

    def body(sp, tl):
        half, lanes = sp.shape[-2:]
        full = 2 * half
        pad = full + 8
        nd = 2 * ta
        own = full // nd

        def vmem(*dims):
            return pltpu.VMEM((*dims, lanes), F32)

        n_recv = 2 + 2 + 2 + 2 + 2 + 4 + 4 * (STEPS - 1) + 3
        polyakov, means = pl.pallas_call(
            functools.partial(kernel, ta, gz, half),
            out_shape=(
                jax.ShapeDtypeStruct((2, 1, half, lanes), F32),
                jax.ShapeDtypeStruct((2, lanes), F32),
            ),
            in_specs=[pl.BlockSpec(memory_space=pltpu.HBM)] * 2,
            out_specs=(pl.BlockSpec(memory_space=pltpu.VMEM),) * 2,
            scratch_shapes=[
                pltpu.VMEM(sp.shape, F32),
                pltpu.VMEM(tl.shape, F32),
                vmem(STEPS + 1, 4, 2, 3, 3, pad),
                vmem(2, 3, 3, pad),
                vmem(STEPS, 2, 2, 2, 2, 3, full),
                vmem(2, 2, 2, 3, full),
                vmem(4, 2, 2, 3, full),
                vmem(4, 2, 2, 3, full),
                vmem(3, 2, 2, 3, pad),
                vmem(2, 2, 3, 3, full),
                vmem(6, 2, 2, 3, full),
                vmem(full * 16),
                vmem(full * 16),
                vmem(18 * 8),
                vmem(own, 2),
                vmem(full, 2),
                vmem(gz, 2),
                pltpu.SemaphoreType.DMA((4,)),
                pltpu.SemaphoreType.DMA,
                pltpu.SemaphoreType.DMA((n_recv,)),
                pltpu.SemaphoreType.REGULAR((max(ta // 2, 1),)),
                pltpu.SemaphoreType.REGULAR((max(gz // 2, 1),)),
            ],
            compiler_params=pltpu.CompilerParams(
                collective_id=0, has_side_effects=True, vmem_limit_bytes=56_450_000
            ),
        )(sp, tl)
        return polyakov, means[:, 0]

    return jax.shard_map(
        body,
        mesh=mesh,
        in_specs=(
            P("cfg", None, None, None, "ta", "gz", "gy", None),
            P("cfg", None, None, "ta", "gz", "gy", None),
        ),
        out_specs=(P("cfg", "gz", "gy", None), P("cfg")),
        check_vma=False,
    )
```

```python
import functools
import math

import jax
import jax.numpy as jnp
from jax import lax
from jax.experimental import pallas as pl
from jax.experimental.pallas import tpu as pltpu
from jax.sharding import PartitionSpec as P

MESH = pl.DeviceIdType.MESH
F32 = jnp.float32
STEPS = 3
FLOOR = 0.25
FX, FY, FZ, FV = 0, 1, 2, 3


def third_row(m):
    (a_re, b_re), (a_im, b_im) = m[0][:2], m[1][:2]
    re, im = [], []
    for k in range(3):
        p, q = (k + 1) % 3, (k + 2) % 3
        re.append(
            a_re[p] * b_re[q] - a_im[p] * b_im[q] - (a_re[q] * b_re[p] - a_im[q] * b_im[p])
        )
        im.append(
            (a_re[q] * b_im[p] + a_im[q] * b_re[p]) - (a_re[p] * b_im[q] + a_im[p] * b_re[q])
        )
    return [m[0][0], m[0][1], re], [m[1][0], m[1][1], im]


def load(ref, lead, rows, count=3):
    return tuple(
        [[ref[(*lead, part, i, j, rows)] for j in range(3)] for i in range(count)]
        for part in range(2)
    )


def load2(ref, lead, rows):
    return third_row(load(ref, lead, rows, 2))


def store(ref, lead, rows, m):
    for part in range(2):
        for i, row in enumerate(m[part]):
            for j, v in enumerate(row):
                ref[(*lead, part, i, j, rows)] = v


def mapped(fn, *ms):
    return tuple(
        [[fn(*vs) for vs in zip(*rows)] for rows in zip(*[m[part] for m in ms])]
        for part in range(2)
    )


def add(*ms):
    return mapped(lambda *vs: functools.reduce(lambda a, b: a + b, vs), *ms)


def ahead_x(m):
    return mapped(lambda v: pltpu.roll(v, v.shape[-1] - 1, 1), m)


def back_x(m):
    return mapped(lambda v: pltpu.roll(v, 1, 1), m)


def mul(a, b, da=False, db=False, rows=3):
    out_re, out_im = [], []
    for i in range(rows):
        row_re, row_im = [], []
        for k in range(3):
            re = im = None
            for j in range(3):
                ar, ai = (a[0][j][i], a[1][j][i]) if da else (a[0][i][j], a[1][i][j])
                br, bi = (b[0][k][j], b[1][k][j]) if db else (b[0][j][k], b[1][j][k])
                rr, ii, ri, ir = ar * br, ai * bi, ar * bi, ai * br
                tr = rr + ii if da != db else rr - ii
                if da and db:
                    ti = -(ri + ir)
                elif da:
                    ti = ri - ir
                elif db:
                    ti = ir - ri
                else:
                    ti = ri + ir
                re = tr if re is None else re + tr
                im = ti if im is None else im + ti
            row_re.append(re)
            row_im.append(im)
        out_re.append(row_re)
        out_im.append(row_im)
    return out_re, out_im


def normalized(re, im):
    weight = sum(v * v for v in re) + sum(v * v for v in im)
    scale = lax.rsqrt(jnp.maximum(weight, FLOOR))
    return [v * scale for v in re], [v * scale for v in im]


def project(re, im):
    u_re, u_im = normalized(re[0], im[0])
    in_re = sum(u_re[j] * re[1][j] + u_im[j] * im[1][j] for j in range(3))
    in_im = sum(u_re[j] * im[1][j] - u_im[j] * re[1][j] for j in range(3))
    w_re = [re[1][j] - (in_re * u_re[j] - in_im * u_im[j]) for j in range(3)]
    w_im = [im[1][j] - (in_re * u_im[j] + in_im * u_re[j]) for j in range(3)]
    v_re, v_im = normalized(w_re, w_im)
    return third_row(([u_re, v_re], [u_im, v_im]))


def mixed(link, staples, weight):
    re = [[0.5 * link[0][i][j] + weight * staples[0][i][j] for j in range(3)] for i in range(2)]
    im = [[0.5 * link[1][i][j] + weight * staples[1][i][j] for j in range(3)] for i in range(2)]
    return project(re, im)


def kernel(
    ta, gz, half,
    sp, tl, pol, mean,
    SP, TL, F, T, H, TH, UP, S, L, AB, M, sm, ar, tree, pb, bc, zs,
    local_sem, send_sem, recv_sem, ready_x, ready_z,
):
    def wrapped(v, n):
        return jnp.where(v >= n, v - n, v)

    j, z, h = lax.axis_index("ta"), lax.axis_index("gz"), lax.axis_index("gy")
    o = 1 - h
    zp, zm = wrapped(z + 1, gz), wrapped(z + gz - 1, gz)
    full = 2 * half
    nd = 2 * ta
    own = full // ta
    me = 2 * j + h
    mine = pl.ds(pl.multiple_of(h * half, half), half)
    halves = [pl.ds(k * half, half) for k in range(2)]

    rows_sent = [0, 0]
    n_recv = [0]

    def remote(src, dst, recv_index, cores=(0, 1), **where):
        pltpu.make_async_remote_copy(
            src_ref=src, dst_ref=dst, send_sem=send_sem, recv_sem=recv_sem.at[recv_index],
            device_id=where, device_id_type=MESH,
        ).start()
        for c in cores:
            rows_sent[c] += math.prod(src.shape[:-1])

    def arrived(dst, recv_index):
        pltpu.make_async_remote_copy(
            src_ref=dst, dst_ref=dst, send_sem=send_sem, recv_sem=recv_sem.at[recv_index],
            device_id={"gy": o}, device_id_type=MESH,
        ).wait_recv()

    def new_recv(n=1):
        k = n_recv[0]
        n_recv[0] += n
        return k

    near = [
        pltpu.make_async_copy(sp, SP, local_sem.at[2]),
        pltpu.make_async_copy(tl, TL, local_sem.at[3]),
        pltpu.make_async_copy(sp.at[:, :, :, :, h, 0], F.at[0, 0:3, :, :, :, mine], local_sem.at[0]),
        pltpu.make_async_copy(tl.at[:, :, :, h, 0], T.at[:, :, :, mine], local_sem.at[1]),
    ]
    for copy in near:
        copy.start()

    barrier = pltpu.get_barrier_semaphore()
    around = sorted({(0, 1 % gz), (0, gz - 1), (1 % ta, 0), (ta - 1, 0)} - {(0, 0)})

    def place(dx, dz):
        return {"ta": wrapped(j + dx, ta), "gz": wrapped(z + dz, gz)}

    def signal(sem, **where):
        pl.semaphore_signal(sem, inc=1, device_id=where, device_id_type=MESH)

    signal(barrier, gy=o)
    for dx, dz in around:
        for c in range(2):
            signal(barrier, **place(dx, dz), gy=c)
    near[0].wait()
    pl.semaphore_wait(barrier, 1 + 2 * len(around))

    def relay(sem, rounds, sides):
        done = [0]

        def go(last=False):
            while True:
                if 0 < done[0] <= rounds:
                    pl.semaphore_wait(sem.at[done[0] - 1], len(sides))
                done[0] += 1
                if done[0] <= rounds:
                    for where in sides:
                        signal(sem.at[done[0] - 1], **where)
                if not last or done[0] > rounds:
                    return

        return go

    hear_x = relay(
        ready_x, ta // 2 - 1, [{"ta": wrapped(j + k, ta)} for k in sorted({1 % ta, ta - 1} - {0})]
    )
    hear_z = relay(
        ready_z, gz // 2 - STEPS, [{"gz": wrapped(z + k, gz)} for k in sorted({1 % gz, gz - 1} - {0})]
    )

    r_v, r_x, r_y, r_t = new_recv(2), new_recv(2), new_recv(2), new_recv(2)
    r_own, r_ownt = new_recv(), new_recv()

    def plane(f, t):
        return SP.at[f, :, 0:2, :, t, 0] if f is not None else TL.at[:, 0:2, :, t, 0]

    def two(ref, *lead):
        return ref.at[(*lead, slice(None), slice(0, 2), slice(None), mine)]

    for t in range(2):
        remote(plane(FZ, t), two(F, 0, FV), r_v + h, gz=zp, gy=t)
    remote(SP.at[:, :, :, :, o, 0], F.at[0, 0:3, :, :, :, mine], r_own, gy=o)
    for f, r in ((FX, r_x), (FY, r_y)):
        for t in range(2):
            remote(plane(f, t), two(H, 0, 0, f), r + h, gz=zm, gy=t)
            remote(plane(f, t), two(H, 0, 1, f), r + h, gz=zp, gy=t)
    near[1].wait()
    remote(TL.at[:, :, :, o, 0], T.at[:, :, :, mine], r_ownt, gy=o)
    for t in range(2):
        remote(plane(None, t), two(TH, 0), r_t + h, gz=zm, gy=t)
    hear_x()

    def each_half(body):
        def run(k, carry):
            r0 = pl.multiple_of(k * half, half)
            body(pl.ds(r0, half), pl.ds(r0 + 1, half))
            return carry

        lax.fori_loop(0, 2, run, 0)

    def wrap(ref, *lead):
        ref[(*lead, slice(None), slice(None), slice(None), pl.ds(full, 1))] = ref[
            (*lead, slice(None), slice(None), slice(None), pl.ds(0, 1))
        ]

    def unwrap(k):
        L[k, :, :, :, pl.ds(0, 1)] = L[k, :, :, :, pl.ds(full, 1)]

    def in_plane(s):
        def body(rows, up):
            ux, uy = load(F, (s, FX), rows), load(F, (s, FY), rows)
            uy_x, ux_y = ahead_x(uy), load(F, (s, FX), up)
            c, d = mul(ux, uy_x), mul(uy, ux_y)
            store(S, (FX,), rows, mul(d, uy_x, db=True, rows=2))
            store(L, (0,), up, mul(uy, c, da=True, rows=2))
            store(
                S, (FY,), rows,
                add(mul(c, ux_y, db=True, rows=2), back_x(mul(ux, d, da=True, rows=2))),
            )

        each_half(body)
        unwrap(0)

    def side(ref, s, f, rows, up):
        return ahead_x(load(ref, (s, f), rows)) if up is None else load(ref, (s, f), up)

    def across(s, f, k):
        def body(rows, up):
            up = None if f == FX else up
            uz, uz_f = load(F, (s, FZ), rows), side(F, s, FZ, rows, up)
            a = mul(uz, load2(H, (s, 0, f), rows))
            store(AB, (0,), rows, a)
            total = add(load(S, (f,), rows, 2), mul(a, uz_f, db=True, rows=2))
            uv, uv_f = load(F, (s, FV), rows), side(F, s, FV, rows, up)
            b = mul(load2(H, (s, 1, f), rows), uv_f)
            store(AB, (1,), rows, b)
            total = add(total, mul(uv, b, da=True, rows=2))
            if f == FX:
                total = add(total, load(L, (0,), rows, 2))
            store(F, (s + 1, f), rows, mixed(load(F, (s, f), rows, 2), total, 0.125))

        body(halves[k], pl.ds(k * half + 1, half))

    def z_staples(s, f):
        def body(rows, up):
            shift = None if f == FX else up
            uf = load(F, (s, f), rows)
            b = mul(uf, side(F, s, FZ, rows, shift), rows=2)
            upper = mul(b, load2(H, (s, 0, f), rows), db=True, rows=2)
            lower = mul(uf, load(AB, (0,), rows), da=True, rows=2)
            below = load2(H, (s, 1, f), rows)
            v_upper = mul(load(AB, (1,), rows), uf, db=True, rows=2)
            v_lower = mul(mul(below, load(F, (s, FV), rows), da=True, rows=2), uf, rows=2)
            if f == FX:
                store(S, (FZ,), rows, add(upper, back_x(lower)))
                store(S, (FV,), rows, add(v_upper, back_x(v_lower)))
            else:
                store(L, (1,), up, lower)
                store(L, (2,), up, v_lower)
                store(S, (FZ,), rows, add(load(S, (FZ,), rows, 2), upper))
                store(S, (FV,), rows, add(load(S, (FV,), rows, 2), v_upper))

        each_half(body)
        if f == FY:
            unwrap(1)
            unwrap(2)

    def z_links(s, last):
        for f, k in ((FZ, 1), (FV, 2)):
            for part in range(2):
                rows = halves[part]
                total = add(load(S, (f,), rows, 2), load(L, (k,), rows, 2))
                store(F, (s + 1, f), rows, mixed(load(F, (s, f), rows, 2), total, 0.125))
                if last:
                    onward(s + 1, f, part)
        wrap(F, s + 1, FZ)
        wrap(F, s + 1, FV)

    for copy in near[2:]:
        copy.wait()
    other = pl.ds(pl.multiple_of(o * half, half), half)
    arrived(F.at[0, 0:3, :, :, :, other], r_own)
    wrap(F, 0, FX)
    wrap(F, 0, FZ)
    in_plane(0)
    for k in range(2):
        arrived(F.at[0, FV, :, 0:2, :, halves[k]], r_v + k)

    def complete(rows, up):
        store(F, (0, FV), rows, load2(F, (0, FV), rows))

    each_half(complete)
    wrap(F, 0, FV)

    r_next = new_recv(4)

    def onward(s, f, k):
        remote(
            F.at[s, f, :, 0:2, :, halves[k]], UP.at[f, :, :, :, halves[k]], r_next + f,
            ta=wrapped(j + h + ta - 1, ta), gy=o,
        )

    r_now = {FX: r_x, FY: r_y}
    for s in range(STEPS):
        last = s == STEPS - 1
        r_then = {f: new_recv(2) for f in (FX, FY)} if not last else {}
        for f in (FX, FY):
            for k in range(2):
                arrived(H.at[s, :, f, :, :, :, halves[k]], r_now[f] + k)
                across(s, f, k)
                if last:
                    onward(s + 1, f, k)
                else:
                    out = F.at[s + 1, f, :, 0:2, :, halves[k]]
                    for side_k, to in ((0, zm), (1, zp)):
                        remote(
                            out, H.at[s + 1, side_k, f, :, :, :, halves[k]],
                            r_then[f] + k, gz=to,
                        )
            if f == FX:
                wrap(F, s + 1, FX)
            else:
                hear_x(last)
            if last:
                hear_z()
            z_staples(s, f)
        r_now = r_then
        if s == STEPS - 2:
            for t in range(2):
                remote(plane(None, t), two(TH, 1), r_t + h, gz=zp, gy=t)
        z_links(s, last)
        if not last:
            in_plane(s + 1)

    n = STEPS
    arrived(T.at[:, :, :, other], r_ownt)
    wrap(T)
    for k in range(2):
        arrived(TH.at[:, :, :, :, halves[k]], r_t + k)

    def before(rows, up):
        t = load(T, (), rows)
        ux, uy = load(F, (n, FX), rows), load(F, (n, FY), rows)
        store(M, (0,), rows, mul(ux, ahead_x(t), rows=2))
        store(M, (1,), rows, mul(ux, t, da=True, rows=2))
        store(M, (2,), rows, mul(uy, load(T, (), up), rows=2))
        store(M, (3,), rows, mul(uy, t, da=True, rows=2))
        store(M, (4,), rows, mul(load(F, (n, FZ), rows), load2(TH, (0,), rows), rows=2))
        store(
            M, (5,), rows, mul(load(F, (n, FV), rows), load2(TH, (1,), rows), da=True, rows=2)
        )

    each_half(before)
    hear_z()
    arrived(UP.at[FX], r_next + FX)
    arrived(UP.at[FY], r_next + FY)

    def along_xy(rows, up):
        ux, uy = load2(UP, (FX,), rows), load2(UP, (FY,), rows)
        total = add(
            mul(load(M, (0,), rows, 2), ux, db=True, rows=2),
            back_x(mul(load(M, (1,), rows, 2), ux, rows=2)),
            mul(load(M, (2,), rows, 2), uy, db=True, rows=2),
        )
        store(S, (0,), rows, total)
        store(L, (0,), up, mul(load(M, (3,), rows, 2), uy, rows=2))

    each_half(along_xy)
    hear_z()
    unwrap(0)
    arrived(UP.at[FZ], r_next + FZ)
    arrived(UP.at[FV], r_next + FV)

    def finish(k, carry):
        r0 = pl.multiple_of(k * half, half)
        rows = pl.ds(r0, half)
        uz, uv = load2(UP, (FZ,), rows), load2(UP, (FV,), rows)
        total = add(
            load(S, (0,), rows, 2),
            load(L, (0,), rows, 2),
            mul(load(M, (4,), rows, 2), uz, db=True, rows=2),
            mul(load(M, (5,), rows, 2), uv, rows=2),
        )
        done = mixed(load(T, (), rows, 2), total, 0.5 / 6.0)
        for part in range(2):
            for a in range(2):
                for b in range(3):
                    sm[pl.ds(r0 * 16 + part * 6 + a * 3 + b, half, 16), :] = done[part][a][b]
        return carry

    lax.fori_loop(0, 2, finish, 0)

    lanes = sm.shape[-1]
    sm3, ar3 = sm.reshape(full, 16, lanes), ar.reshape(own * nd, 16, lanes)
    ar4 = ar.reshape(own, nd, 16, lanes)
    r_row, r_out = new_recv(), new_recv()
    away = sorted(range(1, ta), key=lambda k: -min(k, ta - k))
    home = pl.ds(j * own, own)

    def to_product(k, **kw):
        jd = wrapped(j + k, ta) if k else j
        remote(
            sm3.at[pl.ds(jd * own, own), 0:12], ar4.at[:, me, 0:12], r_row, ta=jd, gy=1, **kw
        )

    for k in away:
        to_product(k)

    @pl.when(h == 0)
    def _():
        to_product(0, cores=(0,))

    hear_z()

    def slices(start, rows):
        at = lambda c: ar[pl.ds(start + c, rows, 32), :]
        return third_row(
            tuple([[at(part * 6 + a * 3 + b) for b in range(3)] for a in range(2)] for part in range(2))
        )

    def pick(first, rows):
        vs = [tree[pl.ds(c * full + first, rows, 2), :] for c in range(18)]
        return tuple(
            [[vs[part * 9 + a * 3 + b] for b in range(3)] for a in range(3)] for part in range(2)
        )

    @pl.when(h == 1)
    def _():
        for r in range(own):
            ar3[r * nd + me] = sm3[j * own + r]
        arrived(ar4.at[:, 0 : nd - 1, 0:12], r_row)
        rows = own * nd // 2
        lhs, rhs = slices(0, rows), slices(16, rows)
        while rows > own:
            flat = [v for part in mul(lhs, rhs) for line in part for v in line]
            for c, v in enumerate(flat):
                tree[pl.ds(c * full, rows), :] = v
            rows //= 2
            lhs, rhs = pick(0, rows), pick(1, rows)
        re = im = None
        for a in range(3):
            for b in range(3):
                lr, li, rr, ri = lhs[0][a][b], lhs[1][a][b], rhs[0][b][a], rhs[1][b][a]
                t_re, t_im = lr * rr - li * ri, lr * ri + li * rr
                re = t_re if re is None else re + t_re
                im = t_im if im is None else im + t_im
        for r in range(own):
            pb[r, 0:1, :] = re[r : r + 1] / 3.0
            pb[r, 1:2, :] = im[r : r + 1] / 3.0
        for k in away:
            for c in range(2):
                remote(pb, bc.at[home], r_out, cores=(1,), ta=wrapped(j + k, ta), gy=c)
        remote(pb, bc.at[home], r_out, cores=(1,), gy=0)
        bc[home] = pb[...]
        arrived(bc.at[pl.ds(0, full - own)], r_out)

    @pl.when(h == 0)
    def _():
        arrived(bc, r_out)

    hear_z(True)
    sums = jnp.sum(bc[...], axis=0)
    zs[z] = sums
    r_sum = new_recv()
    for k in sorted(range(1, gz), key=lambda k: -min(k, gz - k)):
        remote(zs.at[z], zs.at[z], r_sum, gz=wrapped(z + k, gz))
    for k in range(half):
        pol[:, 0, k, :] = bc[h * half + k]
    arrived(zs.at[pl.ds(0, gz - 1)], r_sum)
    totals = jnp.sum(zs[...], axis=0)
    sites = float(full * gz * sp.shape[-1])
    mean[...] = jnp.broadcast_to(jnp.sum(totals, axis=1, keepdims=True) / sites, totals.shape)

    def all_sent(c):
        lines = F.reshape(math.prod(F.shape[:-1]), lanes).at[pl.ds(0, rows_sent[c])]
        pltpu.make_async_copy(lines, lines, send_sem).wait()

    for c in range(2):
        pl.when(h == c)(functools.partial(all_sent, c))


def solution(mesh):
    ta, gz = mesh.shape["ta"], mesh.shape["gz"]

    def body(sp, tl):
        half, lanes = sp.shape[-2:]
        full = 2 * half
        pad = full + 8
        own = full // ta

        def vmem(*dims):
            return pltpu.VMEM((*dims, lanes), F32)

        n_recv = 2 + 2 + 2 + 2 + 2 + 4 + 4 * (STEPS - 1) + 3
        polyakov, means = pl.pallas_call(
            functools.partial(kernel, ta, gz, half),
            out_shape=(
                jax.ShapeDtypeStruct((2, 1, half, lanes), F32),
                jax.ShapeDtypeStruct((2, lanes), F32),
            ),
            in_specs=[pl.BlockSpec(memory_space=pltpu.HBM)] * 2,
            out_specs=(pl.BlockSpec(memory_space=pltpu.VMEM),) * 2,
            scratch_shapes=[
                pltpu.VMEM(sp.shape, F32),
                pltpu.VMEM(tl.shape, F32),
                vmem(STEPS + 1, 4, 2, 3, 3, pad),
                vmem(2, 3, 3, pad),
                vmem(STEPS, 2, 2, 2, 2, 3, full),
                vmem(2, 2, 2, 3, full),
                vmem(4, 2, 2, 3, full),
                vmem(4, 2, 2, 3, full),
                vmem(3, 2, 2, 3, pad),
                vmem(2, 2, 3, 3, full),
                vmem(6, 2, 2, 3, full),
                vmem(full * 16),
                vmem(2 * full * 16),
                vmem(18 * full),
                vmem(own, 2),
                vmem(full, 2),
                vmem(gz, 2),
                pltpu.SemaphoreType.DMA((4,)),
                pltpu.SemaphoreType.DMA,
                pltpu.SemaphoreType.DMA((n_recv,)),
                pltpu.SemaphoreType.REGULAR((max(ta // 2, 1),)),
                pltpu.SemaphoreType.REGULAR((max(gz // 2, 1),)),
            ],
            compiler_params=pltpu.CompilerParams(
                collective_id=0, has_side_effects=True, vmem_limit_bytes=56_450_000
            ),
        )(sp, tl)
        return polyakov, means[:, 0]

    return jax.shard_map(
        body,
        mesh=mesh,
        in_specs=(
            P("cfg", None, None, None, "ta", "gz", "gy", None),
            P("cfg", None, None, "ta", "gz", "gy", None),
        ),
        out_specs=(P("cfg", "gz", "gy", None), P("cfg")),
        check_vma=False,
    )
```

```python
import functools
import math

import jax
import jax.numpy as jnp
from jax import lax
from jax.experimental import pallas as pl
from jax.experimental.pallas import tpu as pltpu
from jax.sharding import PartitionSpec as P

MESH = pl.DeviceIdType.MESH
F32 = jnp.float32
STEPS = 3
FLOOR = 0.25
FX, FY, FZ, FV = 0, 1, 2, 3


def third_row(m):
    (a_re, b_re), (a_im, b_im) = m[0][:2], m[1][:2]
    re, im = [], []
    for k in range(3):
        p, q = (k + 1) % 3, (k + 2) % 3
        re.append(
            a_re[p] * b_re[q] - a_im[p] * b_im[q] - (a_re[q] * b_re[p] - a_im[q] * b_im[p])
        )
        im.append(
            (a_re[q] * b_im[p] + a_im[q] * b_re[p]) - (a_re[p] * b_im[q] + a_im[p] * b_re[q])
        )
    return [m[0][0], m[0][1], re], [m[1][0], m[1][1], im]


def load(ref, lead, rows, count=3):
    return tuple(
        [[ref[(*lead, part, i, j, rows)] for j in range(3)] for i in range(count)]
        for part in range(2)
    )


def load2(ref, lead, rows):
    return third_row(load(ref, lead, rows, 2))


def store(ref, lead, rows, m):
    for part in range(2):
        for i, row in enumerate(m[part]):
            for j, v in enumerate(row):
                ref[(*lead, part, i, j, rows)] = v


def mapped(fn, *ms):
    return tuple(
        [[fn(*vs) for vs in zip(*rows)] for rows in zip(*[m[part] for m in ms])]
        for part in range(2)
    )


def add(*ms):
    return mapped(lambda *vs: functools.reduce(lambda a, b: a + b, vs), *ms)


def ahead_x(m):
    return mapped(lambda v: pltpu.roll(v, v.shape[-1] - 1, 1), m)


def back_x(m):
    return mapped(lambda v: pltpu.roll(v, 1, 1), m)


def mul(a, b, da=False, db=False, rows=3):
    out_re, out_im = [], []
    for i in range(rows):
        row_re, row_im = [], []
        for k in range(3):
            re = im = None
            for j in range(3):
                ar, ai = (a[0][j][i], a[1][j][i]) if da else (a[0][i][j], a[1][i][j])
                br, bi = (b[0][k][j], b[1][k][j]) if db else (b[0][j][k], b[1][j][k])
                rr, ii, ri, ir = ar * br, ai * bi, ar * bi, ai * br
                tr = rr + ii if da != db else rr - ii
                if da and db:
                    ti = -(ri + ir)
                elif da:
                    ti = ri - ir
                elif db:
                    ti = ir - ri
                else:
                    ti = ri + ir
                re = tr if re is None else re + tr
                im = ti if im is None else im + ti
            row_re.append(re)
            row_im.append(im)
        out_re.append(row_re)
        out_im.append(row_im)
    return out_re, out_im


def normalized(re, im):
    weight = sum(v * v for v in re) + sum(v * v for v in im)
    scale = lax.rsqrt(jnp.maximum(weight, FLOOR))
    return [v * scale for v in re], [v * scale for v in im]


def project(re, im):
    u_re, u_im = normalized(re[0], im[0])
    in_re = sum(u_re[j] * re[1][j] + u_im[j] * im[1][j] for j in range(3))
    in_im = sum(u_re[j] * im[1][j] - u_im[j] * re[1][j] for j in range(3))
    w_re = [re[1][j] - (in_re * u_re[j] - in_im * u_im[j]) for j in range(3)]
    w_im = [im[1][j] - (in_re * u_im[j] + in_im * u_re[j]) for j in range(3)]
    v_re, v_im = normalized(w_re, w_im)
    return third_row(([u_re, v_re], [u_im, v_im]))


def mixed(link, staples, weight):
    re = [[0.5 * link[0][i][j] + weight * staples[0][i][j] for j in range(3)] for i in range(2)]
    im = [[0.5 * link[1][i][j] + weight * staples[1][i][j] for j in range(3)] for i in range(2)]
    return project(re, im)


def kernel(
    ta, gz, half,
    sp, tl, pol, mean,
    SP, TL, F, T, H, TH, UP, TB, THB, YP, YQ, Q, S, L, AB, M, sm, ar, tree, pb, bc, zs,
    local_sem, send_sem, recv_sem, ready_x, ready_z,
):
    def wrapped(v, n):
        return jnp.where(v >= n, v - n, v)

    j, z, h = lax.axis_index("ta"), lax.axis_index("gz"), lax.axis_index("gy")
    o = 1 - h
    zp, zm = wrapped(z + 1, gz), wrapped(z + gz - 1, gz)
    full = 2 * half
    nd = 2 * ta
    own = full // ta
    me = 2 * j + h
    mine = pl.ds(pl.multiple_of(h * half, half), half)
    halves = [pl.ds(k * half, half) for k in range(2)]

    rows_sent = [0, 0]
    n_recv = [0]

    def remote(src, dst, recv_index, cores=(0, 1), **where):
        pltpu.make_async_remote_copy(
            src_ref=src, dst_ref=dst, send_sem=send_sem, recv_sem=recv_sem.at[recv_index],
            device_id=where, device_id_type=MESH,
        ).start()
        for c in cores:
            rows_sent[c] += math.prod(src.shape[:-1])

    def arrived(dst, recv_index):
        pltpu.make_async_remote_copy(
            src_ref=dst, dst_ref=dst, send_sem=send_sem, recv_sem=recv_sem.at[recv_index],
            device_id={"gy": o}, device_id_type=MESH,
        ).wait_recv()

    def new_recv(n=1):
        k = n_recv[0]
        n_recv[0] += n
        return k

    near = [
        pltpu.make_async_copy(sp, SP, local_sem.at[2]),
        pltpu.make_async_copy(tl, TL, local_sem.at[3]),
        pltpu.make_async_copy(sp.at[:, :, :, :, h, 0], F.at[0, 0:3, :, :, :, mine], local_sem.at[0]),
        pltpu.make_async_copy(tl.at[:, :, :, h, 0], T.at[:, :, :, mine], local_sem.at[1]),
    ]
    for copy in near:
        copy.start()

    barrier = pltpu.get_barrier_semaphore()
    around = sorted({(0, 1 % gz), (0, gz - 1), (1 % ta, 0), (ta - 1, 0)} - {(0, 0)})

    def place(dx, dz):
        return {"ta": wrapped(j + dx, ta), "gz": wrapped(z + dz, gz)}

    def signal(sem, **where):
        pl.semaphore_signal(sem, inc=1, device_id=where, device_id_type=MESH)

    signal(barrier, gy=o)
    for dx, dz in around:
        for c in range(2):
            signal(barrier, **place(dx, dz), gy=c)
    near[0].wait()
    pl.semaphore_wait(barrier, 1 + 2 * len(around))

    def relay(sem, rounds, sides):
        done = [0]

        def go(last=False):
            while True:
                if 0 < done[0] <= rounds:
                    pl.semaphore_wait(sem.at[done[0] - 1], len(sides))
                done[0] += 1
                if done[0] <= rounds:
                    for where in sides:
                        signal(sem.at[done[0] - 1], **where)
                if not last or done[0] > rounds:
                    return

        return go

    hear_x = relay(
        ready_x, ta // 2 - 1, [{"ta": wrapped(j + k, ta)} for k in sorted({1 % ta, ta - 1} - {0})]
    )
    hear_z = relay(
        ready_z, gz // 2 - STEPS, [{"gz": wrapped(z + k, gz)} for k in sorted({1 % gz, gz - 1} - {0})]
    )

    r_v, r_x, r_y, r_t = new_recv(2), new_recv(2), new_recv(2), new_recv(2)
    r_own, r_ownt = new_recv(), new_recv()

    def plane(f, t):
        return SP.at[f, :, 0:2, :, t, 0] if f is not None else TL.at[:, 0:2, :, t, 0]

    def two(ref, *lead):
        return ref.at[(*lead, slice(None), slice(0, 2), slice(None), mine)]

    for t in range(2):
        remote(plane(FZ, t), two(F, 0, FV), r_v + h, gz=zp, gy=t)
    remote(SP.at[:, :, :, :, o, 0], F.at[0, 0:3, :, :, :, mine], r_own, gy=o)
    for f, r in ((FX, r_x), (FY, r_y)):
        for t in range(2):
            remote(plane(f, t), two(H, 0, 0, f), r + h, gz=zm, gy=t)
            remote(plane(f, t), two(H, 0, 1, f), r + h, gz=zp, gy=t)
    near[1].wait()
    remote(TL.at[:, :, :, o, 0], T.at[:, :, :, mine], r_ownt, gy=o)
    for t in range(2):
        remote(plane(None, t), two(TH, 0), r_t + h, gz=zm, gy=t)
    hear_x()

    def each_half(body):
        def run(k, carry):
            r0 = pl.multiple_of(k * half, half)
            body(pl.ds(r0, half), pl.ds(r0 + 1, half))
            return carry

        lax.fori_loop(0, 2, run, 0)

    def wrap(ref, *lead):
        ref[(*lead, slice(None), slice(None), slice(None), pl.ds(full, 1))] = ref[
            (*lead, slice(None), slice(None), slice(None), pl.ds(0, 1))
        ]

    def unwrap(k):
        L[k, :, :, :, pl.ds(0, 1)] = L[k, :, :, :, pl.ds(full, 1)]

    def in_plane(s):
        def body(rows, up):
            ux, uy = load(F, (s, FX), rows), load(F, (s, FY), rows)
            uy_x, ux_y = ahead_x(uy), load(F, (s, FX), up)
            c, d = mul(ux, uy_x), mul(uy, ux_y)
            store(S, (FX,), rows, mul(d, uy_x, db=True, rows=2))
            store(L, (0,), up, mul(uy, c, da=True, rows=2))
            store(
                S, (FY,), rows,
                add(mul(c, ux_y, db=True, rows=2), back_x(mul(ux, d, da=True, rows=2))),
            )

        each_half(body)
        unwrap(0)

    def side(ref, s, f, rows, up):
        return ahead_x(load(ref, (s, f), rows)) if up is None else load(ref, (s, f), up)

    def across(s, f, k):
        def body(rows, up):
            up = None if f == FX else up
            uz, uz_f = load(F, (s, FZ), rows), side(F, s, FZ, rows, up)
            a = mul(uz, load2(H, (s, 0, f), rows))
            store(AB, (0,), rows, a)
            total = add(load(S, (f,), rows, 2), mul(a, uz_f, db=True, rows=2))
            uv, uv_f = load(F, (s, FV), rows), side(F, s, FV, rows, up)
            b = mul(load2(H, (s, 1, f), rows), uv_f)
            store(AB, (1,), rows, b)
            total = add(total, mul(uv, b, da=True, rows=2))
            if f == FX:
                total = add(total, load(L, (0,), rows, 2))
            store(F, (s + 1, f), rows, mixed(load(F, (s, f), rows, 2), total, 0.125))

        body(halves[k], pl.ds(k * half + 1, half))

    def z_staples(s, f):
        def body(rows, up):
            shift = None if f == FX else up
            uf = load(F, (s, f), rows)
            b = mul(uf, side(F, s, FZ, rows, shift), rows=2)
            upper = mul(b, load2(H, (s, 0, f), rows), db=True, rows=2)
            lower = mul(uf, load(AB, (0,), rows), da=True, rows=2)
            below = load2(H, (s, 1, f), rows)
            v_upper = mul(load(AB, (1,), rows), uf, db=True, rows=2)
            v_lower = mul(mul(below, load(F, (s, FV), rows), da=True, rows=2), uf, rows=2)
            if f == FX:
                store(S, (FZ,), rows, add(upper, back_x(lower)))
                store(S, (FV,), rows, add(v_upper, back_x(v_lower)))
            else:
                store(L, (1,), up, lower)
                store(L, (2,), up, v_lower)
                store(S, (FZ,), rows, add(load(S, (FZ,), rows, 2), upper))
                store(S, (FV,), rows, add(load(S, (FV,), rows, 2), v_upper))

        each_half(body)
        if f == FY:
            unwrap(1)
            unwrap(2)

    def z_links(s, last):
        for f, k in ((FZ, 1), (FV, 2)):
            for part in range(2):
                rows = halves[part]
                total = add(load(S, (f,), rows, 2), load(L, (k,), rows, 2))
                store(F, (s + 1, f), rows, mixed(load(F, (s, f), rows, 2), total, 0.125))
                if last:
                    onward(s + 1, f, part)
        wrap(F, s + 1, FZ)
        wrap(F, s + 1, FV)

    for copy in near[2:]:
        copy.wait()
    other = pl.ds(pl.multiple_of(o * half, half), half)
    arrived(F.at[0, 0:3, :, :, :, other], r_own)
    wrap(F, 0, FX)
    wrap(F, 0, FZ)
    in_plane(0)
    for k in range(2):
        arrived(F.at[0, FV, :, 0:2, :, halves[k]], r_v + k)

    def complete(rows, up):
        store(F, (0, FV), rows, load2(F, (0, FV), rows))

    each_half(complete)
    wrap(F, 0, FV)

    r_next = [new_recv(5), new_recv(5)]
    r_tb, r_thb = new_recv(), new_recv()
    beside = [{"ta": wrapped(j + h + ta - 1, ta), "gy": o}, {"ta": wrapped(j + h, ta), "gy": o}]
    inner = pl.ds(half, half)

    def onward(s, f, k):
        remote(
            F.at[s, f, :, 0:2, :, halves[k]], UP.at[k, f, :, :, :, inner], r_next[k] + f, **beside[k]
        )

    def entries():
        return [(part, a, b) for part in range(2) for a in range(2) for b in range(3)]

    def onward_row(s, k):
        row = full - 1 if k == 0 else half - 1
        for c, (part, a, b) in enumerate(entries()):
            YP[k, pl.ds(c, 1), :] = F[s, FY, part, a, b, pl.ds(row, 1), :]
        remote(YP.at[k, 0:12], YQ.at[k, 0:12], r_next[k] + 4, **beside[k])

    r_now = {FX: r_x, FY: r_y}
    for s in range(STEPS):
        last = s == STEPS - 1
        r_then = {f: new_recv(2) for f in (FX, FY)} if not last else {}
        for f in (FX, FY):
            for k in range(2):
                arrived(H.at[s, :, f, :, :, :, halves[k]], r_now[f] + k)
                across(s, f, k)
                if last:
                    onward(s + 1, f, k)
                else:
                    out = F.at[s + 1, f, :, 0:2, :, halves[k]]
                    for side_k, to in ((0, zm), (1, zp)):
                        remote(
                            out, H.at[s + 1, side_k, f, :, :, :, halves[k]],
                            r_then[f] + k, gz=to,
                        )
            if f == FX:
                wrap(F, s + 1, FX)
            else:
                if last:
                    for k in range(2):
                        onward_row(s + 1, k)
                hear_x(last)
            if last:
                hear_z()
            z_staples(s, f)
        r_now = r_then
        if s == 0:
            arrived(T.at[:, :, :, other], r_ownt)
            wrap(T)
            remote(T.at[:, 0:2, :, 0:full], TB.at[:, :, :, 0:full], r_tb, **beside[1])
        if s == STEPS - 2:
            for t in range(2):
                remote(plane(None, t), two(TH, 1), r_t + h, gz=zp, gy=t)

            @pl.when(h == 1)
            def _():
                for side_k, to in ((0, zm), (1, zp)):
                    for t in range(2):
                        remote(
                            plane(None, t), THB.at[side_k], r_thb, cores=(1,),
                            ta=wrapped(j + t, ta), gz=to, gy=1 - t,
                        )
        z_links(s, last)
        if not last:
            in_plane(s + 1)

    n = STEPS
    r0, r1 = halves
    before1 = pl.ds(half - 1, half)
    for k in range(2):
        arrived(TH.at[:, :, :, :, halves[k]], r_t + k)

    def lower_y(rows, up):
        store(M, (3,), up, mul(load(F, (n, FY), rows), load(T, (), rows), da=True, rows=2))

    each_half(lower_y)
    M[3, :, :, :, pl.ds(0, 1)] = M[3, :, :, :, pl.ds(full, 1)]
    t = load(T, (), r0)
    ux, uy = load(F, (n, FX), r0), load(F, (n, FY), r0)
    store(M, (0,), r0, mul(ux, ahead_x(t), rows=2))
    store(M, (1,), r0, mul(ux, t, da=True, rows=2))
    store(M, (2,), r0, mul(uy, load(T, (), pl.ds(1, half)), rows=2))
    store(M, (4,), r0, mul(load(F, (n, FZ), r0), load2(TH, (0,), r0), rows=2))
    store(M, (5,), r0, mul(load(F, (n, FV), r0), load2(TH, (1,), r0), da=True, rows=2))

    arrived(TB.at[:, :, :, 0:full], r_tb)
    wrap(TB)
    arrived(THB, r_thb)
    t = load2(TB, (), r1)
    ux = load(F, (n, FX), r1)
    store(Q, (0,), r0, mul(ahead_x(t), ux, db=True))
    store(Q, (1,), r0, mul(t, ux))
    store(Q, (2,), r0, mul(load2(TB, (), pl.ds(half + 1, half)), load(F, (n, FY), r1), db=True))
    store(Q, (3,), r0, mul(load2(TB, (), before1), load(F, (n, FY), before1)))
    store(Q, (4,), r0, mul(load2(THB, (0,), r0), load(F, (n, FZ), r1), db=True))
    store(Q, (5,), r0, mul(load2(THB, (1,), r0), load(F, (n, FV), r1)))
    hear_z()

    def came(k, f):
        arrived(UP.at[k, f, :, :, :, inner], r_next[k] + f)

    def row_came(k):
        arrived(YQ.at[k, 0:12], r_next[k] + 4)
        for c, (part, a, b) in enumerate(entries()):
            UP[k, FY, part, a, b, pl.ds(half - 1, 1), :] = YQ[k, pl.ds(c, 1), :]

    for k in range(2):
        came(k, FX)
        came(k, FY)
        row_came(k)
        if k == 0:
            ux = load2(UP, (0, FX), inner)
            total = add(
                mul(load(M, (0,), r0, 2), ux, db=True, rows=2),
                back_x(mul(load(M, (1,), r0, 2), ux, rows=2)),
                mul(load(M, (2,), r0, 2), load2(UP, (0, FY), inner), db=True, rows=2),
                mul(load(M, (3,), r0, 2), load2(UP, (0, FY), before1), rows=2),
            )
        else:
            ux = load2(UP, (1, FX), inner)
            total = add(
                mul(ux, load(Q, (0,), r0), rows=2),
                back_x(mul(ux, load(Q, (1,), r0), da=True, rows=2)),
                mul(load2(UP, (1, FY), inner), load(Q, (2,), r0), rows=2),
                mul(load2(UP, (1, FY), before1), load(Q, (3,), r0), da=True, rows=2),
            )
        store(S, (0,), halves[k], total)
        if k == 0:
            hear_z()

    for k in range(2):
        came(k, FZ)
        came(k, FV)
        uz, uv = load2(UP, (k, FZ), inner), load2(UP, (k, FV), inner)
        if k == 0:
            link = load(T, (), r0, 2)
            total = add(
                load(S, (0,), r0, 2),
                mul(load(M, (4,), r0, 2), uz, db=True, rows=2),
                mul(load(M, (5,), r0, 2), uv, rows=2),
            )
        else:
            link = load(TB, (), r1, 2)
            total = add(
                load(S, (0,), r1, 2),
                mul(uz, load(Q, (4,), r0), rows=2),
                mul(uv, load(Q, (5,), r0), da=True, rows=2),
            )
        done = mixed(link, total, 0.5 / 6.0)
        for c, (part, a, b) in enumerate(entries()):
            sm[pl.ds(k * half * 16 + c, half, 16), :] = done[part][a][b]

    lanes = sm.shape[-1]
    sm3, ar3 = sm.reshape(full, 16, lanes), ar.reshape(own * nd, 16, lanes)
    ar4 = ar.reshape(own, nd, 16, lanes)
    r_row, r_out = new_recv(), new_recv()
    away = sorted(range(1, ta), key=lambda k: -min(k, ta - k))
    home = pl.ds(j * own, own)

    def slice_of(jd):
        return jnp.where(jd * own < half, me, wrapped(me + nd - 1, nd))

    def to_product(k, **kw):
        jd = wrapped(j + k, ta) if k else j
        remote(
            sm3.at[pl.ds(jd * own, own), 0:12], ar4.at[:, slice_of(jd), 0:12], r_row,
            ta=jd, gy=1, **kw,
        )

    for k in away:
        to_product(k)

    @pl.when(h == 0)
    def _():
        to_product(0, cores=(0,))

    hear_z()

    def slices(start, rows):
        at = lambda c: ar[pl.ds(start + c, rows, 32), :]
        return third_row(
            tuple([[at(part * 6 + a * 3 + b) for b in range(3)] for a in range(2)] for part in range(2))
        )

    def pick(first, rows):
        vs = [tree[pl.ds(c * full + first, rows, 2), :] for c in range(18)]
        return tuple(
            [[vs[part * 9 + a * 3 + b] for b in range(3)] for a in range(3)] for part in range(2)
        )

    @pl.when(h == 1)
    def _():
        for r in range(own):
            ar3[r * nd + slice_of(j)] = sm3[j * own + r]
        arrived(ar4.at[:, 0 : nd - 1, 0:12], r_row)
        rows = own * nd // 2
        lhs, rhs = slices(0, rows), slices(16, rows)
        while rows > own:
            flat = [v for part in mul(lhs, rhs) for line in part for v in line]
            for c, v in enumerate(flat):
                tree[pl.ds(c * full, rows), :] = v
            rows //= 2
            lhs, rhs = pick(0, rows), pick(1, rows)
        re = im = None
        for a in range(3):
            for b in range(3):
                lr, li, rr, ri = lhs[0][a][b], lhs[1][a][b], rhs[0][b][a], rhs[1][b][a]
                t_re, t_im = lr * rr - li * ri, lr * ri + li * rr
                re = t_re if re is None else re + t_re
                im = t_im if im is None else im + t_im
        for r in range(own):
            pb[r, 0:1, :] = re[r : r + 1] / 3.0
            pb[r, 1:2, :] = im[r : r + 1] / 3.0
        for k in away:
            for c in range(2):
                remote(pb, bc.at[home], r_out, cores=(1,), ta=wrapped(j + k, ta), gy=c)
        remote(pb, bc.at[home], r_out, cores=(1,), gy=0)
        bc[home] = pb[...]
        arrived(bc.at[pl.ds(0, full - own)], r_out)

    @pl.when(h == 0)
    def _():
        arrived(bc, r_out)

    hear_z(True)
    sums = jnp.sum(bc[...], axis=0)
    zs[z] = sums
    r_sum = new_recv()
    for k in sorted(range(1, gz), key=lambda k: min(k, gz - k)):
        remote(zs.at[z], zs.at[z], r_sum, gz=wrapped(z + k, gz))
    for k in range(half):
        pol[:, 0, k, :] = bc[h * half + k]
    arrived(zs.at[pl.ds(0, gz - 1)], r_sum)
    totals = jnp.sum(zs[...], axis=0)
    sites = float(full * gz * sp.shape[-1])
    mean[...] = jnp.broadcast_to(jnp.sum(totals, axis=1, keepdims=True) / sites, totals.shape)

    def all_sent(c):
        lines = F.reshape(math.prod(F.shape[:-1]), lanes).at[pl.ds(0, rows_sent[c])]
        pltpu.make_async_copy(lines, lines, send_sem).wait()

    for c in range(2):
        pl.when(h == c)(functools.partial(all_sent, c))


def solution(mesh):
    ta, gz = mesh.shape["ta"], mesh.shape["gz"]

    def body(sp, tl):
        half, lanes = sp.shape[-2:]
        full = 2 * half
        pad = full + 8
        own = full // ta

        def vmem(*dims):
            return pltpu.VMEM((*dims, lanes), F32)

        n_recv = 2 + 2 + 2 + 2 + 2 + 12 + 4 * (STEPS - 1) + 3
        polyakov, means = pl.pallas_call(
            functools.partial(kernel, ta, gz, half),
            out_shape=(
                jax.ShapeDtypeStruct((2, 1, half, lanes), F32),
                jax.ShapeDtypeStruct((2, lanes), F32),
            ),
            in_specs=[pl.BlockSpec(memory_space=pltpu.HBM)] * 2,
            out_specs=(pl.BlockSpec(memory_space=pltpu.VMEM),) * 2,
            scratch_shapes=[
                pltpu.VMEM(sp.shape, F32),
                pltpu.VMEM(tl.shape, F32),
                vmem(STEPS + 1, 4, 2, 3, 3, pad),
                vmem(2, 3, 3, pad),
                vmem(STEPS, 2, 2, 2, 2, 3, full),
                vmem(2, 2, 2, 3, full),
                vmem(2, 4, 2, 2, 3, full),
                vmem(2, 2, 3, pad),
                vmem(2, 2, 2, 3, half),
                vmem(2, 16),
                vmem(2, 16),
                vmem(6, 2, 3, 3, half),
                vmem(4, 2, 2, 3, full),
                vmem(3, 2, 2, 3, pad),
                vmem(2, 2, 3, 3, full),
                vmem(6, 2, 2, 3, pad),
                vmem(full * 16),
                vmem(2 * full * 16),
                vmem(18 * full),
                vmem(own, 2),
                vmem(full, 2),
                vmem(gz, 2),
                pltpu.SemaphoreType.DMA((4,)),
                pltpu.SemaphoreType.DMA,
                pltpu.SemaphoreType.DMA((n_recv,)),
                pltpu.SemaphoreType.REGULAR((max(ta // 2, 1),)),
                pltpu.SemaphoreType.REGULAR((max(gz // 2, 1),)),
            ],
            compiler_params=pltpu.CompilerParams(
                collective_id=0, has_side_effects=True, vmem_limit_bytes=56_450_000
            ),
        )(sp, tl)
        return polyakov, means[:, 0]

    return jax.shard_map(
        body,
        mesh=mesh,
        in_specs=(
            P("cfg", None, None, None, "ta", "gz", "gy", None),
            P("cfg", None, None, "ta", "gz", "gy", None),
        ),
        out_specs=(P("cfg", "gz", "gy", None), P("cfg")),
        check_vma=False,
    )
```

```python
import functools
import math

import jax
import jax.numpy as jnp
from jax import lax
from jax.experimental import pallas as pl
from jax.experimental.pallas import tpu as pltpu
from jax.sharding import PartitionSpec as P

MESH = pl.DeviceIdType.MESH
F32 = jnp.float32
STEPS = 3
FLOOR = 0.25
FX, FY, FZ, FV = 0, 1, 2, 3


def third_row(m):
    (a_re, b_re), (a_im, b_im) = m[0][:2], m[1][:2]
    re, im = [], []
    for k in range(3):
        p, q = (k + 1) % 3, (k + 2) % 3
        re.append(
            a_re[p] * b_re[q] - a_im[p] * b_im[q] - (a_re[q] * b_re[p] - a_im[q] * b_im[p])
        )
        im.append(
            (a_re[q] * b_im[p] + a_im[q] * b_re[p]) - (a_re[p] * b_im[q] + a_im[p] * b_re[q])
        )
    return [m[0][0], m[0][1], re], [m[1][0], m[1][1], im]


def load(ref, lead, rows, count=3):
    return tuple(
        [[ref[(*lead, part, i, j, rows)] for j in range(3)] for i in range(count)]
        for part in range(2)
    )


def load2(ref, lead, rows):
    return third_row(load(ref, lead, rows, 2))


def store(ref, lead, rows, m):
    for part in range(2):
        for i, row in enumerate(m[part]):
            for j, v in enumerate(row):
                ref[(*lead, part, i, j, rows)] = v


def mapped(fn, *ms):
    return tuple(
        [[fn(*vs) for vs in zip(*rows)] for rows in zip(*[m[part] for m in ms])]
        for part in range(2)
    )


def add(*ms):
    return mapped(lambda *vs: functools.reduce(lambda a, b: a + b, vs), *ms)


def ahead_x(m):
    return mapped(lambda v: pltpu.roll(v, v.shape[-1] - 1, 1), m)


def back_x(m):
    return mapped(lambda v: pltpu.roll(v, 1, 1), m)


def mul(a, b, da=False, db=False, rows=3):
    out_re, out_im = [], []
    for i in range(rows):
        row_re, row_im = [], []
        for k in range(3):
            re = im = None
            for j in range(3):
                ar, ai = (a[0][j][i], a[1][j][i]) if da else (a[0][i][j], a[1][i][j])
                br, bi = (b[0][k][j], b[1][k][j]) if db else (b[0][j][k], b[1][j][k])
                rr, ii, ri, ir = ar * br, ai * bi, ar * bi, ai * br
                tr = rr + ii if da != db else rr - ii
                if da and db:
                    ti = -(ri + ir)
                elif da:
                    ti = ri - ir
                elif db:
                    ti = ir - ri
                else:
                    ti = ri + ir
                re = tr if re is None else re + tr
                im = ti if im is None else im + ti
            row_re.append(re)
            row_im.append(im)
        out_re.append(row_re)
        out_im.append(row_im)
    return out_re, out_im


def normalized(re, im):
    weight = sum(v * v for v in re) + sum(v * v for v in im)
    scale = lax.rsqrt(jnp.maximum(weight, FLOOR))
    return [v * scale for v in re], [v * scale for v in im]


def project(re, im):
    u_re, u_im = normalized(re[0], im[0])
    in_re = sum(u_re[j] * re[1][j] + u_im[j] * im[1][j] for j in range(3))
    in_im = sum(u_re[j] * im[1][j] - u_im[j] * re[1][j] for j in range(3))
    w_re = [re[1][j] - (in_re * u_re[j] - in_im * u_im[j]) for j in range(3)]
    w_im = [im[1][j] - (in_re * u_im[j] + in_im * u_re[j]) for j in range(3)]
    v_re, v_im = normalized(w_re, w_im)
    return third_row(([u_re, v_re], [u_im, v_im]))


def mixed(link, staples, weight):
    re = [[0.5 * link[0][i][j] + weight * staples[0][i][j] for j in range(3)] for i in range(2)]
    im = [[0.5 * link[1][i][j] + weight * staples[1][i][j] for j in range(3)] for i in range(2)]
    return project(re, im)


def kernel(
    ta, gz, half,
    sp, tl, pol, mean,
    SP, TL, F, T, H, TH, UP, TB, THB, YP, YQ, Q, S, L, AB, M, sm, ar, tree, pb, bc, zs,
    local_sem, send_sem, recv_sem, ready_x, ready_z,
):
    def wrapped(v, n):
        return jnp.where(v >= n, v - n, v)

    j, z, h = lax.axis_index("ta"), lax.axis_index("gz"), lax.axis_index("gy")
    o = 1 - h
    zp, zm = wrapped(z + 1, gz), wrapped(z + gz - 1, gz)
    full = 2 * half
    nd = 2 * ta
    own = full // ta
    me = 2 * j + h
    mine = pl.ds(pl.multiple_of(h * half, half), half)
    halves = [pl.ds(k * half, half) for k in range(2)]

    rows_sent = [0, 0]
    n_recv = [0]

    def remote(src, dst, recv_index, cores=(0, 1), **where):
        pltpu.make_async_remote_copy(
            src_ref=src, dst_ref=dst, send_sem=send_sem, recv_sem=recv_sem.at[recv_index],
            device_id=where, device_id_type=MESH,
        ).start()
        for c in cores:
            rows_sent[c] += math.prod(src.shape[:-1])

    def arrived(dst, recv_index):
        pltpu.make_async_remote_copy(
            src_ref=dst, dst_ref=dst, send_sem=send_sem, recv_sem=recv_sem.at[recv_index],
            device_id={"gy": o}, device_id_type=MESH,
        ).wait_recv()

    def new_recv(n=1):
        k = n_recv[0]
        n_recv[0] += n
        return k

    near = [
        pltpu.make_async_copy(sp, SP, local_sem.at[2]),
        pltpu.make_async_copy(tl, TL, local_sem.at[3]),
        pltpu.make_async_copy(sp.at[:, :, :, :, h, 0], F.at[0, 0:3, :, :, :, mine], local_sem.at[0]),
        pltpu.make_async_copy(tl.at[:, :, :, h, 0], T.at[:, :, :, mine], local_sem.at[1]),
    ]
    for copy in near:
        copy.start()

    barrier = pltpu.get_barrier_semaphore()
    around = sorted({(0, 1 % gz), (0, gz - 1), (1 % ta, 0), (ta - 1, 0)} - {(0, 0)})

    def place(dx, dz):
        return {"ta": wrapped(j + dx, ta), "gz": wrapped(z + dz, gz)}

    def signal(sem, **where):
        pl.semaphore_signal(sem, inc=1, device_id=where, device_id_type=MESH)

    signal(barrier, gy=o)
    for dx, dz in around:
        for c in range(2):
            signal(barrier, **place(dx, dz), gy=c)
    near[0].wait()
    pl.semaphore_wait(barrier, 1 + 2 * len(around))

    def relay(sem, rounds, sides):
        done = [0]

        def go(last=False):
            while True:
                if 0 < done[0] <= rounds:
                    pl.semaphore_wait(sem.at[done[0] - 1], len(sides))
                done[0] += 1
                if done[0] <= rounds:
                    for where in sides:
                        signal(sem.at[done[0] - 1], **where)
                if not last or done[0] > rounds:
                    return

        return go

    hear_x = relay(
        ready_x, ta // 2 - 1, [{"ta": wrapped(j + k, ta)} for k in sorted({1 % ta, ta - 1} - {0})]
    )
    hear_z = relay(
        ready_z, gz // 2 - 1, [{"gz": wrapped(z + k, gz)} for k in sorted({1 % gz, gz - 1} - {0})]
    )

    r_v, r_x, r_y, r_t = new_recv(2), new_recv(2), new_recv(2), new_recv(2)
    r_own, r_ownt = new_recv(), new_recv()

    def plane(f, t):
        return SP.at[f, :, 0:2, :, t, 0] if f is not None else TL.at[:, 0:2, :, t, 0]

    def two(ref, *lead):
        return ref.at[(*lead, slice(None), slice(0, 2), slice(None), mine)]

    for t in range(2):
        remote(plane(FZ, t), two(F, 0, FV), r_v + h, gz=zp, gy=t)
    remote(SP.at[:, :, :, :, o, 0], F.at[0, 0:3, :, :, :, mine], r_own, gy=o)
    for f, r in ((FX, r_x), (FY, r_y)):
        for t in range(2):
            remote(plane(f, t), two(H, 0, 0, f), r + h, gz=zm, gy=t)
            remote(plane(f, t), two(H, 0, 1, f), r + h, gz=zp, gy=t)
    near[1].wait()
    remote(TL.at[:, :, :, o, 0], T.at[:, :, :, mine], r_ownt, gy=o)
    for t in range(2):
        remote(plane(None, t), two(TH, 0), r_t + h, gz=zm, gy=t)
    hear_x()
    hear_z()

    def each_half(body):
        def run(k, carry):
            r0 = pl.multiple_of(k * half, half)
            body(pl.ds(r0, half), pl.ds(r0 + 1, half))
            return carry

        lax.fori_loop(0, 2, run, 0)

    def wrap(ref, *lead):
        ref[(*lead, slice(None), slice(None), slice(None), pl.ds(full, 1))] = ref[
            (*lead, slice(None), slice(None), slice(None), pl.ds(0, 1))
        ]

    def unwrap(k):
        L[k, :, :, :, pl.ds(0, 1)] = L[k, :, :, :, pl.ds(full, 1)]

    def in_plane(s):
        def body(rows, up):
            ux, uy = load(F, (s, FX), rows), load(F, (s, FY), rows)
            uy_x, ux_y = ahead_x(uy), load(F, (s, FX), up)
            c, d = mul(ux, uy_x), mul(uy, ux_y)
            store(S, (FX,), rows, mul(d, uy_x, db=True, rows=2))
            store(L, (0,), up, mul(uy, c, da=True, rows=2))
            store(
                S, (FY,), rows,
                add(mul(c, ux_y, db=True, rows=2), back_x(mul(ux, d, da=True, rows=2))),
            )

        each_half(body)
        unwrap(0)

    def side(ref, s, f, rows, up):
        return ahead_x(load(ref, (s, f), rows)) if up is None else load(ref, (s, f), up)

    def across(s, f, k):
        def body(rows, up):
            up = None if f == FX else up
            uz, uz_f = load(F, (s, FZ), rows), side(F, s, FZ, rows, up)
            a = mul(uz, load2(H, (s, 0, f), rows))
            store(AB, (0,), rows, a)
            total = add(load(S, (f,), rows, 2), mul(a, uz_f, db=True, rows=2))
            uv, uv_f = load(F, (s, FV), rows), side(F, s, FV, rows, up)
            b = mul(load2(H, (s, 1, f), rows), uv_f)
            store(AB, (1,), rows, b)
            total = add(total, mul(uv, b, da=True, rows=2))
            if f == FX:
                total = add(total, load(L, (0,), rows, 2))
            store(F, (s + 1, f), rows, mixed(load(F, (s, f), rows, 2), total, 0.125))

        body(halves[k], pl.ds(k * half + 1, half))

    def z_staples(s, f):
        def body(rows, up):
            shift = None if f == FX else up
            uf = load(F, (s, f), rows)
            b = mul(uf, side(F, s, FZ, rows, shift), rows=2)
            upper = mul(b, load2(H, (s, 0, f), rows), db=True, rows=2)
            lower = mul(uf, load(AB, (0,), rows), da=True, rows=2)
            below = load2(H, (s, 1, f), rows)
            v_upper = mul(load(AB, (1,), rows), uf, db=True, rows=2)
            v_lower = mul(mul(below, load(F, (s, FV), rows), da=True, rows=2), uf, rows=2)
            if f == FX:
                store(S, (FZ,), rows, add(upper, back_x(lower)))
                store(S, (FV,), rows, add(v_upper, back_x(v_lower)))
            else:
                store(L, (1,), up, lower)
                store(L, (2,), up, v_lower)
                store(S, (FZ,), rows, add(load(S, (FZ,), rows, 2), upper))
                store(S, (FV,), rows, add(load(S, (FV,), rows, 2), v_upper))

        each_half(body)
        if f == FY:
            unwrap(1)
            unwrap(2)

    def z_links(s, last):
        for f, k in ((FZ, 1), (FV, 2)):
            for part in range(2):
                rows = halves[part]
                total = add(load(S, (f,), rows, 2), load(L, (k,), rows, 2))
                store(F, (s + 1, f), rows, mixed(load(F, (s, f), rows, 2), total, 0.125))
                if last:
                    onward(s + 1, f, part)
        wrap(F, s + 1, FZ)
        wrap(F, s + 1, FV)

    for copy in near[2:]:
        copy.wait()
    other = pl.ds(pl.multiple_of(o * half, half), half)
    arrived(F.at[0, 0:3, :, :, :, other], r_own)
    wrap(F, 0, FX)
    wrap(F, 0, FZ)
    in_plane(0)
    hear_z()
    for k in range(2):
        arrived(F.at[0, FV, :, 0:2, :, halves[k]], r_v + k)

    def complete(rows, up):
        store(F, (0, FV), rows, load2(F, (0, FV), rows))

    each_half(complete)
    wrap(F, 0, FV)

    r_next = [new_recv(5), new_recv(5)]
    r_tb, r_thb = new_recv(), new_recv()
    beside = [{"ta": wrapped(j + h + ta - 1, ta), "gy": o}, {"ta": wrapped(j + h, ta), "gy": o}]
    inner = pl.ds(half, half)

    def onward(s, f, k):
        remote(
            F.at[s, f, :, 0:2, :, halves[k]], UP.at[k, f, :, :, :, inner], r_next[k] + f, **beside[k]
        )

    def entries():
        return [(part, a, b) for part in range(2) for a in range(2) for b in range(3)]

    def onward_row(s, k):
        row = full - 1 if k == 0 else half - 1
        for c, (part, a, b) in enumerate(entries()):
            YP[k, pl.ds(c, 1), :] = F[s, FY, part, a, b, pl.ds(row, 1), :]
        remote(YP.at[k, 0:12], YQ.at[k, 0:12], r_next[k] + 4, **beside[k])

    r_now = {FX: r_x, FY: r_y}
    for s in range(STEPS):
        last = s == STEPS - 1
        r_then = {f: new_recv(2) for f in (FX, FY)} if not last else {}
        for f in (FX, FY):
            hear_z(last and f == FY)
            if f == FY:
                hear_x(last)
            for k in range(2):
                arrived(H.at[s, :, f, :, :, :, halves[k]], r_now[f] + k)
                across(s, f, k)
                if last:
                    onward(s + 1, f, k)
                else:
                    out = F.at[s + 1, f, :, 0:2, :, halves[k]]
                    for side_k, to in ((0, zm), (1, zp)):
                        remote(
                            out, H.at[s + 1, side_k, f, :, :, :, halves[k]],
                            r_then[f] + k, gz=to,
                        )
            if f == FX:
                wrap(F, s + 1, FX)
            else:
                if last:
                    for k in range(2):
                        onward_row(s + 1, k)
            z_staples(s, f)
        r_now = r_then
        if s == 0:
            arrived(T.at[:, :, :, other], r_ownt)
            wrap(T)
            remote(T.at[:, 0:2, :, 0:full], TB.at[:, :, :, 0:full], r_tb, **beside[1])
        if s == STEPS - 2:
            @pl.when(h == 1)
            def _():
                for side_k, to in ((0, zm), (1, zp)):
                    for t in range(2):
                        remote(
                            plane(None, t), THB.at[side_k], r_thb, cores=(1,),
                            ta=wrapped(j + t, ta), gz=to, gy=1 - t,
                        )

            for t in range(2):
                remote(plane(None, t), two(TH, 1), r_t + h, gz=zp, gy=t)
        z_links(s, last)
        if not last:
            in_plane(s + 1)

    n = STEPS
    r0, r1 = halves
    before1 = pl.ds(half - 1, half)

    def lower_y(rows, up):
        store(M, (3,), up, mul(load(F, (n, FY), rows), load(T, (), rows), da=True, rows=2))

    each_half(lower_y)
    M[3, :, :, :, pl.ds(0, 1)] = M[3, :, :, :, pl.ds(full, 1)]
    t = load(T, (), r0)
    ux, uy = load(F, (n, FX), r0), load(F, (n, FY), r0)
    store(M, (0,), r0, mul(ux, ahead_x(t), rows=2))
    store(M, (1,), r0, mul(ux, t, da=True, rows=2))
    store(M, (2,), r0, mul(uy, load(T, (), pl.ds(1, half)), rows=2))

    arrived(TB.at[:, :, :, 0:full], r_tb)
    wrap(TB)
    t = load2(TB, (), r1)
    ux = load(F, (n, FX), r1)
    store(Q, (0,), r0, mul(ahead_x(t), ux, db=True))
    store(Q, (1,), r0, mul(t, ux))
    store(Q, (2,), r0, mul(load2(TB, (), pl.ds(half + 1, half)), load(F, (n, FY), r1), db=True))
    store(Q, (3,), r0, mul(load2(TB, (), before1), load(F, (n, FY), before1)))

    def came(k, f):
        arrived(UP.at[k, f, :, :, :, inner], r_next[k] + f)

    def row_came(k):
        arrived(YQ.at[k, 0:12], r_next[k] + 4)
        for c, (part, a, b) in enumerate(entries()):
            UP[k, FY, part, a, b, pl.ds(half - 1, 1), :] = YQ[k, pl.ds(c, 1), :]

    for k in range(2):
        came(k, FX)
        came(k, FY)
        row_came(k)
        if k == 0:
            ux = load2(UP, (0, FX), inner)
            total = add(
                mul(load(M, (0,), r0, 2), ux, db=True, rows=2),
                back_x(mul(load(M, (1,), r0, 2), ux, rows=2)),
                mul(load(M, (2,), r0, 2), load2(UP, (0, FY), inner), db=True, rows=2),
                mul(load(M, (3,), r0, 2), load2(UP, (0, FY), before1), rows=2),
            )
        else:
            ux = load2(UP, (1, FX), inner)
            total = add(
                mul(ux, load(Q, (0,), r0), rows=2),
                back_x(mul(ux, load(Q, (1,), r0), da=True, rows=2)),
                mul(load2(UP, (1, FY), inner), load(Q, (2,), r0), rows=2),
                mul(load2(UP, (1, FY), before1), load(Q, (3,), r0), da=True, rows=2),
            )
        store(S, (0,), halves[k], total)

    arrived(THB, r_thb)
    store(Q, (4,), r0, mul(load2(THB, (0,), r0), load(F, (n, FZ), r1), db=True))
    store(Q, (5,), r0, mul(load2(THB, (1,), r0), load(F, (n, FV), r1)))
    for k in range(2):
        arrived(TH.at[:, :, :, :, halves[k]], r_t + k)
    store(M, (4,), r0, mul(load(F, (n, FZ), r0), load2(TH, (0,), r0), rows=2))
    store(M, (5,), r0, mul(load(F, (n, FV), r0), load2(TH, (1,), r0), da=True, rows=2))

    for k in range(2):
        came(k, FZ)
        came(k, FV)
        uz, uv = load2(UP, (k, FZ), inner), load2(UP, (k, FV), inner)
        if k == 0:
            link = load(T, (), r0, 2)
            total = add(
                load(S, (0,), r0, 2),
                mul(load(M, (4,), r0, 2), uz, db=True, rows=2),
                mul(load(M, (5,), r0, 2), uv, rows=2),
            )
        else:
            link = load(TB, (), r1, 2)
            total = add(
                load(S, (0,), r1, 2),
                mul(uz, load(Q, (4,), r0), rows=2),
                mul(uv, load(Q, (5,), r0), da=True, rows=2),
            )
        done = mixed(link, total, 0.5 / 6.0)
        for c, (part, a, b) in enumerate(entries()):
            sm[pl.ds(k * half * 16 + c, half, 16), :] = done[part][a][b]

    lanes = sm.shape[-1]
    sm3, ar3 = sm.reshape(full, 16, lanes), ar.reshape(own * nd, 16, lanes)
    ar4 = ar.reshape(own, nd, 16, lanes)
    r_row, r_out = new_recv(), new_recv()
    away = sorted(range(1, ta), key=lambda k: -min(k, ta - k))
    home = pl.ds(j * own, own)

    def slice_of(jd):
        return jnp.where(jd * own < half, me, wrapped(me + nd - 1, nd))

    def to_product(k, **kw):
        jd = wrapped(j + k, ta) if k else j
        remote(
            sm3.at[pl.ds(jd * own, own), 0:12], ar4.at[:, slice_of(jd), 0:12], r_row,
            ta=jd, gy=1, **kw,
        )

    for k in away:
        to_product(k)

    @pl.when(h == 0)
    def _():
        to_product(0, cores=(0,))

    def slices(start, rows):
        at = lambda c: ar[pl.ds(start + c, rows, 32), :]
        return third_row(
            tuple([[at(part * 6 + a * 3 + b) for b in range(3)] for a in range(2)] for part in range(2))
        )

    def pick(first, rows):
        vs = [tree[pl.ds(c * full + first, rows, 2), :] for c in range(18)]
        return tuple(
            [[vs[part * 9 + a * 3 + b] for b in range(3)] for a in range(3)] for part in range(2)
        )

    @pl.when(h == 1)
    def _():
        for r in range(own):
            ar3[r * nd + slice_of(j)] = sm3[j * own + r]
        arrived(ar4.at[:, 0 : nd - 1, 0:12], r_row)
        rows = own * nd // 2
        lhs, rhs = slices(0, rows), slices(16, rows)
        while rows > own:
            flat = [v for part in mul(lhs, rhs) for line in part for v in line]
            for c, v in enumerate(flat):
                tree[pl.ds(c * full, rows), :] = v
            rows //= 2
            lhs, rhs = pick(0, rows), pick(1, rows)
        re = im = None
        for a in range(3):
            for b in range(3):
                lr, li, rr, ri = lhs[0][a][b], lhs[1][a][b], rhs[0][b][a], rhs[1][b][a]
                t_re, t_im = lr * rr - li * ri, lr * ri + li * rr
                re = t_re if re is None else re + t_re
                im = t_im if im is None else im + t_im
        for r in range(own):
            pb[r, 0:1, :] = re[r : r + 1] / 3.0
            pb[r, 1:2, :] = im[r : r + 1] / 3.0
        for k in away:
            for c in range(2):
                remote(pb, bc.at[home], r_out, cores=(1,), ta=wrapped(j + k, ta), gy=c)
        remote(pb, bc.at[home], r_out, cores=(1,), gy=0)
        bc[home] = pb[...]
        arrived(bc.at[pl.ds(0, full - own)], r_out)

    @pl.when(h == 0)
    def _():
        arrived(bc, r_out)

    sums = jnp.sum(bc[...], axis=0)
    zs[z] = sums
    r_sum = new_recv()
    for k in sorted(range(1, gz), key=lambda k: min(k, gz - k)):
        remote(zs.at[z], zs.at[z], r_sum, gz=wrapped(z + k, gz))
    for k in range(half):
        pol[:, 0, k, :] = bc[h * half + k]
    arrived(zs.at[pl.ds(0, gz - 1)], r_sum)
    totals = jnp.sum(zs[...], axis=0)
    sites = float(full * gz * sp.shape[-1])
    mean[...] = jnp.broadcast_to(jnp.sum(totals, axis=1, keepdims=True) / sites, totals.shape)

    def all_sent(c):
        lines = F.reshape(math.prod(F.shape[:-1]), lanes).at[pl.ds(0, rows_sent[c])]
        pltpu.make_async_copy(lines, lines, send_sem).wait()

    for c in range(2):
        pl.when(h == c)(functools.partial(all_sent, c))


def solution(mesh):
    ta, gz = mesh.shape["ta"], mesh.shape["gz"]

    def body(sp, tl):
        half, lanes = sp.shape[-2:]
        full = 2 * half
        pad = full + 8
        own = full // ta

        def vmem(*dims):
            return pltpu.VMEM((*dims, lanes), F32)

        n_recv = 2 + 2 + 2 + 2 + 2 + 12 + 4 * (STEPS - 1) + 3
        polyakov, means = pl.pallas_call(
            functools.partial(kernel, ta, gz, half),
            out_shape=(
                jax.ShapeDtypeStruct((2, 1, half, lanes), F32),
                jax.ShapeDtypeStruct((2, lanes), F32),
            ),
            in_specs=[pl.BlockSpec(memory_space=pltpu.HBM)] * 2,
            out_specs=(pl.BlockSpec(memory_space=pltpu.VMEM),) * 2,
            scratch_shapes=[
                pltpu.VMEM(sp.shape, F32),
                pltpu.VMEM(tl.shape, F32),
                vmem(STEPS + 1, 4, 2, 3, 3, pad),
                vmem(2, 3, 3, pad),
                vmem(STEPS, 2, 2, 2, 2, 3, full),
                vmem(2, 2, 2, 3, full),
                vmem(2, 4, 2, 2, 3, full),
                vmem(2, 2, 3, pad),
                vmem(2, 2, 2, 3, half),
                vmem(2, 16),
                vmem(2, 16),
                vmem(6, 2, 3, 3, half),
                vmem(4, 2, 2, 3, full),
                vmem(3, 2, 2, 3, pad),
                vmem(2, 2, 3, 3, full),
                vmem(6, 2, 2, 3, pad),
                vmem(full * 16),
                vmem(2 * full * 16),
                vmem(18 * full),
                vmem(own, 2),
                vmem(full, 2),
                vmem(gz, 2),
                pltpu.SemaphoreType.DMA((4,)),
                pltpu.SemaphoreType.DMA,
                pltpu.SemaphoreType.DMA((n_recv,)),
                pltpu.SemaphoreType.REGULAR((max(ta // 2, 1),)),
                pltpu.SemaphoreType.REGULAR((max(gz // 2, 1),)),
            ],
            compiler_params=pltpu.CompilerParams(
                collective_id=0, has_side_effects=True, vmem_limit_bytes=56_450_000
            ),
        )(sp, tl)
        return polyakov, means[:, 0]

    return jax.shard_map(
        body,
        mesh=mesh,
        in_specs=(
            P("cfg", None, None, None, "ta", "gz", "gy", None),
            P("cfg", None, None, "ta", "gz", "gy", None),
        ),
        out_specs=(P("cfg", "gz", "gy", None), P("cfg")),
        check_vma=False,
    )
```

```python
import functools
import math

import jax
import jax.numpy as jnp
from jax import lax
from jax.experimental import pallas as pl
from jax.experimental.pallas import tpu as pltpu
from jax.sharding import PartitionSpec as P

MESH = pl.DeviceIdType.MESH
F32 = jnp.float32
STEPS = 3
FLOOR = 0.25
FX, FY, FZ, FV = 0, 1, 2, 3


def third_row(m):
    (a_re, b_re), (a_im, b_im) = m[0][:2], m[1][:2]
    re, im = [], []
    for k in range(3):
        p, q = (k + 1) % 3, (k + 2) % 3
        re.append(
            a_re[p] * b_re[q] - a_im[p] * b_im[q] - (a_re[q] * b_re[p] - a_im[q] * b_im[p])
        )
        im.append(
            (a_re[q] * b_im[p] + a_im[q] * b_re[p]) - (a_re[p] * b_im[q] + a_im[p] * b_re[q])
        )
    return [m[0][0], m[0][1], re], [m[1][0], m[1][1], im]


def load(ref, lead, rows, count=3):
    return tuple(
        [[ref[(*lead, part, i, j, rows)] for j in range(3)] for i in range(count)]
        for part in range(2)
    )


def load2(ref, lead, rows):
    return third_row(load(ref, lead, rows, 2))


def store(ref, lead, rows, m):
    for part in range(2):
        for i, row in enumerate(m[part]):
            for j, v in enumerate(row):
                ref[(*lead, part, i, j, rows)] = v


def mapped(fn, *ms):
    return tuple(
        [[fn(*vs) for vs in zip(*rows)] for rows in zip(*[m[part] for m in ms])]
        for part in range(2)
    )


def add(*ms):
    return mapped(lambda *vs: functools.reduce(lambda a, b: a + b, vs), *ms)


def ahead_x(m):
    return mapped(lambda v: pltpu.roll(v, v.shape[-1] - 1, 1), m)


def back_x(m):
    return mapped(lambda v: pltpu.roll(v, 1, 1), m)


def mul(a, b, da=False, db=False, rows=3):
    out_re, out_im = [], []
    for i in range(rows):
        row_re, row_im = [], []
        for k in range(3):
            re = im = None
            for j in range(3):
                ar, ai = (a[0][j][i], a[1][j][i]) if da else (a[0][i][j], a[1][i][j])
                br, bi = (b[0][k][j], b[1][k][j]) if db else (b[0][j][k], b[1][j][k])
                rr, ii, ri, ir = ar * br, ai * bi, ar * bi, ai * br
                tr = rr + ii if da != db else rr - ii
                if da and db:
                    ti = -(ri + ir)
                elif da:
                    ti = ri - ir
                elif db:
                    ti = ir - ri
                else:
                    ti = ri + ir
                re = tr if re is None else re + tr
                im = ti if im is None else im + ti
            row_re.append(re)
            row_im.append(im)
        out_re.append(row_re)
        out_im.append(row_im)
    return out_re, out_im


def normalized(re, im):
    weight = sum(v * v for v in re) + sum(v * v for v in im)
    scale = lax.rsqrt(jnp.maximum(weight, FLOOR))
    return [v * scale for v in re], [v * scale for v in im]


def project(re, im):
    u_re, u_im = normalized(re[0], im[0])
    in_re = sum(u_re[j] * re[1][j] + u_im[j] * im[1][j] for j in range(3))
    in_im = sum(u_re[j] * im[1][j] - u_im[j] * re[1][j] for j in range(3))
    w_re = [re[1][j] - (in_re * u_re[j] - in_im * u_im[j]) for j in range(3)]
    w_im = [im[1][j] - (in_re * u_im[j] + in_im * u_re[j]) for j in range(3)]
    v_re, v_im = normalized(w_re, w_im)
    return third_row(([u_re, v_re], [u_im, v_im]))


def mixed(link, staples, weight):
    re = [[0.5 * link[0][i][j] + weight * staples[0][i][j] for j in range(3)] for i in range(2)]
    im = [[0.5 * link[1][i][j] + weight * staples[1][i][j] for j in range(3)] for i in range(2)]
    return project(re, im)


def kernel(
    ta, gz, half,
    sp, tl, pol, mean,
    SP, TL, F, T, H, TH, UP, TB, THB, YP, YQ, Q, S, L, AB, M, sm, ar, tree, pb, bc, zs,
    local_sem, send_sem, recv_sem, ready_x, ready_z,
):
    def wrapped(v, n):
        return jnp.where(v >= n, v - n, v)

    j, z, h = lax.axis_index("ta"), lax.axis_index("gz"), lax.axis_index("gy")
    o = 1 - h
    zp, zm = wrapped(z + 1, gz), wrapped(z + gz - 1, gz)
    full = 2 * half
    nd = 2 * ta
    own = full // ta
    me = 2 * j + h
    mine = pl.ds(pl.multiple_of(h * half, half), half)
    halves = [pl.ds(k * half, half) for k in range(2)]

    rows_sent = [0, 0]
    n_recv = [0]

    def remote(src, dst, recv_index, cores=(0, 1), **where):
        pltpu.make_async_remote_copy(
            src_ref=src, dst_ref=dst, send_sem=send_sem, recv_sem=recv_sem.at[recv_index],
            device_id=where, device_id_type=MESH,
        ).start()
        for c in cores:
            rows_sent[c] += math.prod(src.shape[:-1])

    def arrived(dst, recv_index):
        pltpu.make_async_remote_copy(
            src_ref=dst, dst_ref=dst, send_sem=send_sem, recv_sem=recv_sem.at[recv_index],
            device_id={"gy": o}, device_id_type=MESH,
        ).wait_recv()

    def new_recv(n=1):
        k = n_recv[0]
        n_recv[0] += n
        return k

    near = [
        pltpu.make_async_copy(sp, SP, local_sem.at[2]),
        pltpu.make_async_copy(tl, TL, local_sem.at[3]),
        pltpu.make_async_copy(sp.at[:, :, :, :, h, 0], F.at[0, 0:3, :, :, :, mine], local_sem.at[0]),
        pltpu.make_async_copy(tl.at[:, :, :, h, 0], T.at[:, :, :, mine], local_sem.at[1]),
    ]
    for copy in near:
        copy.start()

    barrier = pltpu.get_barrier_semaphore()
    around = sorted({(0, 1 % gz), (0, gz - 1), (1 % ta, 0), (ta - 1, 0)} - {(0, 0)})

    def place(dx, dz):
        return {"ta": wrapped(j + dx, ta), "gz": wrapped(z + dz, gz)}

    def signal(sem, **where):
        pl.semaphore_signal(sem, inc=1, device_id=where, device_id_type=MESH)

    signal(barrier, gy=o)
    for dx, dz in around:
        for c in range(2):
            signal(barrier, **place(dx, dz), gy=c)
    near[0].wait()
    pl.semaphore_wait(barrier, 1 + 2 * len(around))

    def relay(sem, axis, here, size):
        reach = [1]
        waiting = [None]

        def go():
            if waiting[0] is not None:
                pl.semaphore_wait(sem.at[waiting[0][0]], waiting[0][1])
                waiting[0] = None
            if 2 * reach[0] <= size:
                n = reach[0]
                sides = sorted({n % size, (size - n) % size} - {0})
                if n < size // 2:
                    index = n.bit_length() - 1
                    for k in sides:
                        signal(sem.at[index], **{axis: wrapped(here + k, size)})
                    waiting[0] = (index, len(sides))
                    reach[0] = 2 * n

        return go

    hear_x = relay(ready_x, "ta", j, ta)
    hear_z = relay(ready_z, "gz", z, gz)

    r_v, r_x, r_y, r_t = new_recv(2), new_recv(2), new_recv(2), new_recv(2)
    r_own, r_ownt = new_recv(), new_recv()

    def plane(f, t):
        return SP.at[f, :, 0:2, :, t, 0] if f is not None else TL.at[:, 0:2, :, t, 0]

    def two(ref, *lead):
        return ref.at[(*lead, slice(None), slice(0, 2), slice(None), mine)]

    for t in range(2):
        remote(plane(FZ, t), two(F, 0, FV), r_v + h, gz=zp, gy=t)
    remote(SP.at[:, :, :, :, o, 0], F.at[0, 0:3, :, :, :, mine], r_own, gy=o)
    for f, r in ((FX, r_x), (FY, r_y)):
        for t in range(2):
            remote(plane(f, t), two(H, 0, 0, f), r + h, gz=zm, gy=t)
            remote(plane(f, t), two(H, 0, 1, f), r + h, gz=zp, gy=t)
    near[1].wait()
    remote(TL.at[:, :, :, o, 0], T.at[:, :, :, mine], r_ownt, gy=o)
    for t in range(2):
        remote(plane(None, t), two(TH, 0), r_t + h, gz=zm, gy=t)
    hear_x()
    hear_z()

    def each_half(body):
        def run(k, carry):
            r0 = pl.multiple_of(k * half, half)
            body(pl.ds(r0, half), pl.ds(r0 + 1, half))
            return carry

        lax.fori_loop(0, 2, run, 0)

    def wrap(ref, *lead):
        ref[(*lead, slice(None), slice(None), slice(None), pl.ds(full, 1))] = ref[
            (*lead, slice(None), slice(None), slice(None), pl.ds(0, 1))
        ]

    def unwrap(k):
        L[k, :, :, :, pl.ds(0, 1)] = L[k, :, :, :, pl.ds(full, 1)]

    def in_plane(s):
        def body(rows, up):
            ux, uy = load(F, (s, FX), rows), load(F, (s, FY), rows)
            uy_x, ux_y = ahead_x(uy), load(F, (s, FX), up)
            c, d = mul(ux, uy_x), mul(uy, ux_y)
            store(S, (FX,), rows, mul(d, uy_x, db=True, rows=2))
            store(L, (0,), up, mul(uy, c, da=True, rows=2))
            store(
                S, (FY,), rows,
                add(mul(c, ux_y, db=True, rows=2), back_x(mul(ux, d, da=True, rows=2))),
            )

        each_half(body)
        unwrap(0)

    def side(ref, s, f, rows, up):
        return ahead_x(load(ref, (s, f), rows)) if up is None else load(ref, (s, f), up)

    def span(k):
        r0 = pl.multiple_of(k * half, half)
        return pl.ds(r0, half), pl.ds(r0 + 1, half)

    def across(s, f, rows, up):
        def body(rows, up):
            up = None if f == FX else up
            uz, uz_f = load(F, (s, FZ), rows), side(F, s, FZ, rows, up)
            a = mul(uz, load2(H, (s, 0, f), rows))
            store(AB, (0,), rows, a)
            total = add(load(S, (f,), rows, 2), mul(a, uz_f, db=True, rows=2))
            uv, uv_f = load(F, (s, FV), rows), side(F, s, FV, rows, up)
            b = mul(load2(H, (s, 1, f), rows), uv_f)
            store(AB, (1,), rows, b)
            total = add(total, mul(uv, b, da=True, rows=2))
            if f == FX:
                total = add(total, load(L, (0,), rows, 2))
            store(F, (s + 1, f), rows, mixed(load(F, (s, f), rows, 2), total, 0.125))

        body(rows, up)

    def z_staples(s, f):
        def body(rows, up):
            shift = None if f == FX else up
            uf = load(F, (s, f), rows)
            b = mul(uf, side(F, s, FZ, rows, shift), rows=2)
            upper = mul(b, load2(H, (s, 0, f), rows), db=True, rows=2)
            lower = mul(uf, load(AB, (0,), rows), da=True, rows=2)
            below = load2(H, (s, 1, f), rows)
            v_upper = mul(load(AB, (1,), rows), uf, db=True, rows=2)
            v_lower = mul(mul(below, load(F, (s, FV), rows), da=True, rows=2), uf, rows=2)
            if f == FX:
                store(S, (FZ,), rows, add(upper, back_x(lower)))
                store(S, (FV,), rows, add(v_upper, back_x(v_lower)))
            else:
                store(L, (1,), up, lower)
                store(L, (2,), up, v_lower)
                store(S, (FZ,), rows, add(load(S, (FZ,), rows, 2), upper))
                store(S, (FV,), rows, add(load(S, (FV,), rows, 2), v_upper))

        each_half(body)
        if f == FY:
            unwrap(1)
            unwrap(2)

    def z_links(s, last):
        for part in (h, o):
            rows, _ = span(part)
            for f, k in ((FZ, 1), (FV, 2)):
                total = add(load(S, (f,), rows, 2), load(L, (k,), rows, 2))
                store(F, (s + 1, f), rows, mixed(load(F, (s, f), rows, 2), total, 0.125))
                if last:
                    onward(s + 1, f, part, rows)
        wrap(F, s + 1, FZ)
        wrap(F, s + 1, FV)

    for copy in near[2:]:
        copy.wait()
    other = pl.ds(pl.multiple_of(o * half, half), half)
    arrived(F.at[0, 0:3, :, :, :, other], r_own)
    wrap(F, 0, FX)
    wrap(F, 0, FZ)
    in_plane(0)
    for k in range(2):
        arrived(F.at[0, FV, :, 0:2, :, halves[k]], r_v + k)

    def complete(rows, up):
        store(F, (0, FV), rows, load2(F, (0, FV), rows))

    each_half(complete)
    wrap(F, 0, FV)

    r_next = new_recv(10)
    r_tb, r_thb = new_recv(), new_recv()
    beside = [{"ta": wrapped(j + h + ta - 1, ta), "gy": o}, {"ta": wrapped(j + h, ta), "gy": o}]
    inner = pl.ds(half, half)

    def onward(s, f, k, rows):
        to = {"ta": jnp.where(k == 0, beside[0]["ta"], beside[1]["ta"]), "gy": o}
        remote(
            F.at[s, f, :, 0:2, :, rows], UP.at[k, f, :, :, :, inner], r_next + 5 * k + f, **to
        )

    def entries():
        return [(part, a, b) for part in range(2) for a in range(2) for b in range(3)]

    def onward_row(s, k):
        row = full - 1 if k == 0 else half - 1
        for c, (part, a, b) in enumerate(entries()):
            YP[k, pl.ds(c, 1), :] = F[s, FY, part, a, b, pl.ds(row, 1), :]
        remote(YP.at[k, 0:12], YQ.at[k, 0:12], r_next + 5 * k + 4, **beside[k])

    r_now = {FX: r_x, FY: r_y}
    for s in range(STEPS):
        last = s == STEPS - 1
        r_then = {f: new_recv(2) for f in (FX, FY)} if not last else {}
        for f in (FX, FY):
            (hear_z if f == FX else hear_x)()
            for k in (h, o):
                rows, up = span(k)
                arrived(H.at[s, :, f, :, :, :, rows], r_now[f] + k)
                across(s, f, rows, up)
                if last:
                    onward(s + 1, f, k, rows)
                else:
                    out = F.at[s + 1, f, :, 0:2, :, rows]
                    for side_k, to in ((0, zm), (1, zp)):
                        remote(
                            out, H.at[s + 1, side_k, f, :, :, :, rows], r_then[f] + k, gz=to
                        )
            if f == FX:
                wrap(F, s + 1, FX)
            else:
                if last:
                    for k in range(2):
                        onward_row(s + 1, k)
            z_staples(s, f)
        r_now = r_then
        if s == 0:
            arrived(T.at[:, :, :, other], r_ownt)
            wrap(T)
            remote(T.at[:, 0:2, :, 0:full], TB.at[:, :, :, 0:full], r_tb, **beside[1])
        if s == STEPS - 2:
            @pl.when(h == 1)
            def _():
                for side_k, to in ((0, zm), (1, zp)):
                    for t in range(2):
                        remote(
                            plane(None, t), THB.at[side_k], r_thb, cores=(1,),
                            ta=wrapped(j + t, ta), gz=to, gy=1 - t,
                        )

            for t in range(2):
                remote(plane(None, t), two(TH, 1), r_t + h, gz=zp, gy=t)
        z_links(s, last)
        if not last:
            in_plane(s + 1)

    n = STEPS
    r0, r1 = halves
    before1 = pl.ds(half - 1, half)

    def lower_y(rows, up):
        store(M, (3,), up, mul(load(F, (n, FY), rows), load(T, (), rows), da=True, rows=2))

    each_half(lower_y)
    M[3, :, :, :, pl.ds(0, 1)] = M[3, :, :, :, pl.ds(full, 1)]
    t = load(T, (), r0)
    ux, uy = load(F, (n, FX), r0), load(F, (n, FY), r0)
    store(M, (0,), r0, mul(ux, ahead_x(t), rows=2))
    store(M, (1,), r0, mul(ux, t, da=True, rows=2))
    store(M, (2,), r0, mul(uy, load(T, (), pl.ds(1, half)), rows=2))

    arrived(TB.at[:, :, :, 0:full], r_tb)
    wrap(TB)
    t = load2(TB, (), r1)
    ux = load(F, (n, FX), r1)
    store(Q, (0,), r0, mul(ahead_x(t), ux, db=True))
    store(Q, (1,), r0, mul(t, ux))
    store(Q, (2,), r0, mul(load2(TB, (), pl.ds(half + 1, half)), load(F, (n, FY), r1), db=True))
    store(Q, (3,), r0, mul(load2(TB, (), before1), load(F, (n, FY), before1)))

    def came(k, f):
        arrived(UP.at[k, f, :, :, :, inner], r_next + 5 * k + f)

    def row_came(k):
        arrived(YQ.at[k, 0:12], r_next + 5 * k + 4)
        for c, (part, a, b) in enumerate(entries()):
            UP[k, FY, part, a, b, pl.ds(half - 1, 1), :] = YQ[k, pl.ds(c, 1), :]

    for k in range(2):
        came(k, FX)
        came(k, FY)
        row_came(k)
        if k == 0:
            ux = load2(UP, (0, FX), inner)
            total = add(
                mul(load(M, (0,), r0, 2), ux, db=True, rows=2),
                back_x(mul(load(M, (1,), r0, 2), ux, rows=2)),
                mul(load(M, (2,), r0, 2), load2(UP, (0, FY), inner), db=True, rows=2),
                mul(load(M, (3,), r0, 2), load2(UP, (0, FY), before1), rows=2),
            )
        else:
            ux = load2(UP, (1, FX), inner)
            total = add(
                mul(ux, load(Q, (0,), r0), rows=2),
                back_x(mul(ux, load(Q, (1,), r0), da=True, rows=2)),
                mul(load2(UP, (1, FY), inner), load(Q, (2,), r0), rows=2),
                mul(load2(UP, (1, FY), before1), load(Q, (3,), r0), da=True, rows=2),
            )
        store(S, (0,), halves[k], total)

    arrived(THB, r_thb)
    store(Q, (4,), r0, mul(load2(THB, (0,), r0), load(F, (n, FZ), r1), db=True))
    store(Q, (5,), r0, mul(load2(THB, (1,), r0), load(F, (n, FV), r1)))
    for k in range(2):
        arrived(TH.at[:, :, :, :, halves[k]], r_t + k)
    store(M, (4,), r0, mul(load(F, (n, FZ), r0), load2(TH, (0,), r0), rows=2))
    store(M, (5,), r0, mul(load(F, (n, FV), r0), load2(TH, (1,), r0), da=True, rows=2))

    for k in range(2):
        came(k, FZ)
        came(k, FV)
        uz, uv = load2(UP, (k, FZ), inner), load2(UP, (k, FV), inner)
        if k == 0:
            link = load(T, (), r0, 2)
            total = add(
                load(S, (0,), r0, 2),
                mul(load(M, (4,), r0, 2), uz, db=True, rows=2),
                mul(load(M, (5,), r0, 2), uv, rows=2),
            )
        else:
            link = load(TB, (), r1, 2)
            total = add(
                load(S, (0,), r1, 2),
                mul(uz, load(Q, (4,), r0), rows=2),
                mul(uv, load(Q, (5,), r0), da=True, rows=2),
            )
        done = mixed(link, total, 0.5 / 6.0)
        for c, (part, a, b) in enumerate(entries()):
            sm[pl.ds(k * half * 16 + c, half, 16), :] = done[part][a][b]

    lanes = sm.shape[-1]
    sm3, ar3 = sm.reshape(full, 16, lanes), ar.reshape(own * nd, 16, lanes)
    ar4 = ar.reshape(own, nd, 16, lanes)
    r_row, r_out = new_recv(), new_recv()
    away = sorted(range(1, ta), key=lambda k: -min(k, ta - k))
    home = pl.ds(j * own, own)

    def slice_of(jd):
        return jnp.where(jd * own < half, me, wrapped(me + nd - 1, nd))

    def to_product(k, **kw):
        jd = wrapped(j + k, ta) if k else j
        remote(
            sm3.at[pl.ds(jd * own, own), 0:12], ar4.at[:, slice_of(jd), 0:12], r_row,
            ta=jd, gy=1, **kw,
        )

    for k in away:
        to_product(k)

    @pl.when(h == 0)
    def _():
        to_product(0, cores=(0,))

    def slices(start, rows):
        at = lambda c: ar[pl.ds(start + c, rows, 32), :]
        return third_row(
            tuple([[at(part * 6 + a * 3 + b) for b in range(3)] for a in range(2)] for part in range(2))
        )

    def pick(first, rows):
        vs = [tree[pl.ds(c * full + first, rows, 2), :] for c in range(18)]
        return tuple(
            [[vs[part * 9 + a * 3 + b] for b in range(3)] for a in range(3)] for part in range(2)
        )

    @pl.when(h == 1)
    def _():
        for r in range(own):
            ar3[r * nd + slice_of(j)] = sm3[j * own + r]
        arrived(ar4.at[:, 0 : nd - 1, 0:12], r_row)
        rows = own * nd // 2
        lhs, rhs = slices(0, rows), slices(16, rows)
        while rows > own:
            flat = [v for part in mul(lhs, rhs) for line in part for v in line]
            for c, v in enumerate(flat):
                tree[pl.ds(c * full, rows), :] = v
            rows //= 2
            lhs, rhs = pick(0, rows), pick(1, rows)
        re = im = None
        for a in range(3):
            for b in range(3):
                lr, li, rr, ri = lhs[0][a][b], lhs[1][a][b], rhs[0][b][a], rhs[1][b][a]
                t_re, t_im = lr * rr - li * ri, lr * ri + li * rr
                re = t_re if re is None else re + t_re
                im = t_im if im is None else im + t_im
        for r in range(own):
            pb[r, 0:1, :] = re[r : r + 1] / 3.0
            pb[r, 1:2, :] = im[r : r + 1] / 3.0
        for k in away:
            for c in range(2):
                remote(pb, bc.at[home], r_out, cores=(1,), ta=wrapped(j + k, ta), gy=c)
        remote(pb, bc.at[home], r_out, cores=(1,), gy=0)
        bc[home] = pb[...]
        arrived(bc.at[pl.ds(0, full - own)], r_out)

    @pl.when(h == 0)
    def _():
        arrived(bc, r_out)

    sums = jnp.sum(bc[...], axis=0)
    zs[z] = sums
    r_sum = new_recv()
    for k in sorted(range(1, gz), key=lambda k: min(k, gz - k)):
        remote(zs.at[z], zs.at[z], r_sum, gz=wrapped(z + k, gz))
    for k in range(half):
        pol[:, 0, k, :] = bc[h * half + k]
    arrived(zs.at[pl.ds(0, gz - 1)], r_sum)
    totals = jnp.sum(zs[...], axis=0)
    sites = float(full * gz * sp.shape[-1])
    mean[...] = jnp.broadcast_to(jnp.sum(totals, axis=1, keepdims=True) / sites, totals.shape)

    def all_sent(c):
        lines = F.reshape(math.prod(F.shape[:-1]), lanes).at[pl.ds(0, rows_sent[c])]
        pltpu.make_async_copy(lines, lines, send_sem).wait()

    for c in range(2):
        pl.when(h == c)(functools.partial(all_sent, c))


def solution(mesh):
    ta, gz = mesh.shape["ta"], mesh.shape["gz"]

    def body(sp, tl):
        half, lanes = sp.shape[-2:]
        full = 2 * half
        pad = full + 8
        own = full // ta

        def vmem(*dims):
            return pltpu.VMEM((*dims, lanes), F32)

        n_recv = 2 + 2 + 2 + 2 + 2 + 12 + 4 * (STEPS - 1) + 3
        polyakov, means = pl.pallas_call(
            functools.partial(kernel, ta, gz, half),
            out_shape=(
                jax.ShapeDtypeStruct((2, 1, half, lanes), F32),
                jax.ShapeDtypeStruct((2, lanes), F32),
            ),
            in_specs=[pl.BlockSpec(memory_space=pltpu.HBM)] * 2,
            out_specs=(pl.BlockSpec(memory_space=pltpu.VMEM),) * 2,
            scratch_shapes=[
                pltpu.VMEM(sp.shape, F32),
                pltpu.VMEM(tl.shape, F32),
                vmem(STEPS + 1, 4, 2, 3, 3, pad),
                vmem(2, 3, 3, pad),
                vmem(STEPS, 2, 2, 2, 2, 3, full),
                vmem(2, 2, 2, 3, full),
                vmem(2, 4, 2, 2, 3, full),
                vmem(2, 2, 3, pad),
                vmem(2, 2, 2, 3, half),
                vmem(2, 16),
                vmem(2, 16),
                vmem(6, 2, 3, 3, half),
                vmem(4, 2, 2, 3, full),
                vmem(3, 2, 2, 3, pad),
                vmem(2, 2, 3, 3, full),
                vmem(6, 2, 2, 3, pad),
                vmem(full * 16),
                vmem(2 * full * 16),
                vmem(18 * full),
                vmem(own, 2),
                vmem(full, 2),
                vmem(gz, 2),
                pltpu.SemaphoreType.DMA((4,)),
                pltpu.SemaphoreType.DMA,
                pltpu.SemaphoreType.DMA((n_recv,)),
                pltpu.SemaphoreType.REGULAR((max(ta // 2, 1),)),
                pltpu.SemaphoreType.REGULAR((max(gz // 2, 1),)),
            ],
            compiler_params=pltpu.CompilerParams(
                collective_id=0, has_side_effects=True, vmem_limit_bytes=56_450_000
            ),
        )(sp, tl)
        return polyakov, means[:, 0]

    return jax.shard_map(
        body,
        mesh=mesh,
        in_specs=(
            P("cfg", None, None, None, "ta", "gz", "gy", None),
            P("cfg", None, None, "ta", "gz", "gy", None),
        ),
        out_specs=(P("cfg", "gz", "gy", None), P("cfg")),
        check_vma=False,
    )
```

```python
import functools
import math

import jax
import jax.numpy as jnp
from jax import lax
from jax.experimental import pallas as pl
from jax.experimental.pallas import tpu as pltpu
from jax.sharding import PartitionSpec as P

MESH = pl.DeviceIdType.MESH
F32 = jnp.float32
STEPS = 3
FLOOR = 0.25
FX, FY, FZ, FV = 0, 1, 2, 3


def third_row(m):
    (a_re, b_re), (a_im, b_im) = m[0][:2], m[1][:2]
    re, im = [], []
    for k in range(3):
        p, q = (k + 1) % 3, (k + 2) % 3
        re.append(
            a_re[p] * b_re[q] - a_im[p] * b_im[q] - (a_re[q] * b_re[p] - a_im[q] * b_im[p])
        )
        im.append(
            (a_re[q] * b_im[p] + a_im[q] * b_re[p]) - (a_re[p] * b_im[q] + a_im[p] * b_re[q])
        )
    return [m[0][0], m[0][1], re], [m[1][0], m[1][1], im]


def load(ref, lead, rows, count=3):
    return tuple(
        [[ref[(*lead, part, i, j, rows)] for j in range(3)] for i in range(count)]
        for part in range(2)
    )


def load2(ref, lead, rows):
    return third_row(load(ref, lead, rows, 2))


def store(ref, lead, rows, m):
    for part in range(2):
        for i, row in enumerate(m[part]):
            for j, v in enumerate(row):
                ref[(*lead, part, i, j, rows)] = v


def mapped(fn, *ms):
    return tuple(
        [[fn(*vs) for vs in zip(*rows)] for rows in zip(*[m[part] for m in ms])]
        for part in range(2)
    )


def add(*ms):
    return mapped(lambda *vs: functools.reduce(lambda a, b: a + b, vs), *ms)


def ahead_x(m):
    return mapped(lambda v: pltpu.roll(v, v.shape[-1] - 1, 1), m)


def back_x(m):
    return mapped(lambda v: pltpu.roll(v, 1, 1), m)


def mul(a, b, da=False, db=False, rows=3):
    out_re, out_im = [], []
    for i in range(rows):
        row_re, row_im = [], []
        for k in range(3):
            re = im = None
            for j in range(3):
                ar, ai = (a[0][j][i], a[1][j][i]) if da else (a[0][i][j], a[1][i][j])
                br, bi = (b[0][k][j], b[1][k][j]) if db else (b[0][j][k], b[1][j][k])
                rr, ii, ri, ir = ar * br, ai * bi, ar * bi, ai * br
                tr = rr + ii if da != db else rr - ii
                if da and db:
                    ti = -(ri + ir)
                elif da:
                    ti = ri - ir
                elif db:
                    ti = ir - ri
                else:
                    ti = ri + ir
                re = tr if re is None else re + tr
                im = ti if im is None else im + ti
            row_re.append(re)
            row_im.append(im)
        out_re.append(row_re)
        out_im.append(row_im)
    return out_re, out_im


def normalized(re, im):
    weight = sum(v * v for v in re) + sum(v * v for v in im)
    scale = lax.rsqrt(jnp.maximum(weight, FLOOR))
    return [v * scale for v in re], [v * scale for v in im]


def project(re, im):
    u_re, u_im = normalized(re[0], im[0])
    in_re = sum(u_re[j] * re[1][j] + u_im[j] * im[1][j] for j in range(3))
    in_im = sum(u_re[j] * im[1][j] - u_im[j] * re[1][j] for j in range(3))
    w_re = [re[1][j] - (in_re * u_re[j] - in_im * u_im[j]) for j in range(3)]
    w_im = [im[1][j] - (in_re * u_im[j] + in_im * u_re[j]) for j in range(3)]
    v_re, v_im = normalized(w_re, w_im)
    return third_row(([u_re, v_re], [u_im, v_im]))


def mixed(link, staples, weight):
    re = [[0.5 * link[0][i][j] + weight * staples[0][i][j] for j in range(3)] for i in range(2)]
    im = [[0.5 * link[1][i][j] + weight * staples[1][i][j] for j in range(3)] for i in range(2)]
    return project(re, im)


def kernel(
    ta, gz, half,
    sp, tl, pol, mean,
    SP, TL, F, T, H, TH, UP, TB, THB, YP, YQ, Q, S, L, AB, M, sm, ar, tree, pb, bc, zs,
    local_sem, send_sem, recv_sem, ready_x, ready_z,
):
    def wrapped(v, n):
        return jnp.where(v >= n, v - n, v)

    j, z, h = lax.axis_index("ta"), lax.axis_index("gz"), lax.axis_index("gy")
    o = 1 - h
    zp, zm = wrapped(z + 1, gz), wrapped(z + gz - 1, gz)
    full = 2 * half
    nd = 2 * ta
    own = full // ta
    me = 2 * j + h
    mine = pl.ds(pl.multiple_of(h * half, half), half)
    halves = [pl.ds(k * half, half) for k in range(2)]

    rows_sent = [0, 0]
    n_recv = [0]

    def remote(src, dst, recv_index, cores=(0, 1), **where):
        pltpu.make_async_remote_copy(
            src_ref=src, dst_ref=dst, send_sem=send_sem, recv_sem=recv_sem.at[recv_index],
            device_id=where, device_id_type=MESH,
        ).start()
        for c in cores:
            rows_sent[c] += math.prod(src.shape[:-1])

    def arrived(dst, recv_index):
        pltpu.make_async_remote_copy(
            src_ref=dst, dst_ref=dst, send_sem=send_sem, recv_sem=recv_sem.at[recv_index],
            device_id={"gy": o}, device_id_type=MESH,
        ).wait_recv()

    def new_recv(n=1):
        k = n_recv[0]
        n_recv[0] += n
        return k

    near = [
        pltpu.make_async_copy(sp, SP, local_sem.at[2]),
        pltpu.make_async_copy(tl, TL, local_sem.at[3]),
        pltpu.make_async_copy(sp.at[:, :, :, :, h, 0], F.at[0, 0:3, :, :, :, mine], local_sem.at[0]),
        pltpu.make_async_copy(tl.at[:, :, :, h, 0], T.at[:, :, :, mine], local_sem.at[1]),
    ]
    for copy in near:
        copy.start()

    barrier = pltpu.get_barrier_semaphore()
    around = sorted({(0, 1 % gz), (0, gz - 1), (1 % ta, 0), (ta - 1, 0)} - {(0, 0)})

    def place(dx, dz):
        return {"ta": wrapped(j + dx, ta), "gz": wrapped(z + dz, gz)}

    def signal(sem, **where):
        pl.semaphore_signal(sem, inc=1, device_id=where, device_id_type=MESH)

    signal(barrier, gy=o)
    for dx, dz in around:
        for c in range(2):
            signal(barrier, **place(dx, dz), gy=c)
    near[0].wait()
    pl.semaphore_wait(barrier, 1 + 2 * len(around))

    def relay(sem, axis, here, size):
        reach = [1]
        waiting = [None]

        def go():
            if waiting[0] is not None:
                pl.semaphore_wait(sem.at[waiting[0][0]], waiting[0][1])
                waiting[0] = None
            if 2 * reach[0] <= size:
                n = reach[0]
                sides = sorted({n % size, (size - n) % size} - {0})
                if n < size // 2:
                    index = n.bit_length() - 1
                    for k in sides:
                        signal(sem.at[index], **{axis: wrapped(here + k, size)})
                    waiting[0] = (index, len(sides))
                    reach[0] = 2 * n

        return go

    hear_x = relay(ready_x, "ta", j, ta)
    hear_z = relay(ready_z, "gz", z, gz)

    r_v, r_x, r_y, r_t = new_recv(2), new_recv(2), new_recv(2), new_recv(2)
    r_own, r_ownt = new_recv(), new_recv()

    def plane(f, t):
        return SP.at[f, :, 0:2, :, t, 0] if f is not None else TL.at[:, 0:2, :, t, 0]

    def two(ref, *lead):
        return ref.at[(*lead, slice(None), slice(0, 2), slice(None), mine)]

    for t in range(2):
        remote(plane(FZ, t), two(F, 0, FV), r_v + h, gz=zp, gy=t)
    remote(SP.at[:, :, :, :, o, 0], F.at[0, 0:3, :, :, :, mine], r_own, gy=o)
    for f, r in ((FX, r_x), (FY, r_y)):
        for t in range(2):
            remote(plane(f, t), two(H, 0, 0, f), r + h, gz=zm, gy=t)
            remote(plane(f, t), two(H, 0, 1, f), r + h, gz=zp, gy=t)
    near[1].wait()
    remote(TL.at[:, :, :, o, 0], T.at[:, :, :, mine], r_ownt, gy=o)
    for t in range(2):
        remote(plane(None, t), two(TH, 0), r_t + h, gz=zm, gy=t)
    hear_x()
    hear_z()

    def each_half(body):
        def run(k, carry):
            r0 = pl.multiple_of(k * half, half)
            body(pl.ds(r0, half), pl.ds(r0 + 1, half))
            return carry

        lax.fori_loop(0, 2, run, 0)

    def wrap(ref, *lead):
        ref[(*lead, slice(None), slice(None), slice(None), pl.ds(full, 1))] = ref[
            (*lead, slice(None), slice(None), slice(None), pl.ds(0, 1))
        ]

    def unwrap(k):
        L[k, :, :, :, pl.ds(0, 1)] = L[k, :, :, :, pl.ds(full, 1)]

    def in_plane(s):
        def body(rows, up):
            ux, uy = load(F, (s, FX), rows), load(F, (s, FY), rows)
            uy_x, ux_y = ahead_x(uy), load(F, (s, FX), up)
            c, d = mul(ux, uy_x), mul(uy, ux_y)
            store(S, (FX,), rows, mul(d, uy_x, db=True, rows=2))
            store(L, (0,), up, mul(uy, c, da=True, rows=2))
            store(
                S, (FY,), rows,
                add(mul(c, ux_y, db=True, rows=2), back_x(mul(ux, d, da=True, rows=2))),
            )

        each_half(body)
        unwrap(0)

    def side(ref, s, f, rows, up):
        return ahead_x(load(ref, (s, f), rows)) if up is None else load(ref, (s, f), up)

    def span(k):
        r0 = pl.multiple_of(k * half, half)
        return pl.ds(r0, half), pl.ds(r0 + 1, half)

    def across(s, f, rows, up):
        def body(rows, up):
            up = None if f == FX else up
            uz, uz_f = load(F, (s, FZ), rows), side(F, s, FZ, rows, up)
            a = mul(uz, load2(H, (s, 0, f), rows))
            store(AB, (0,), rows, a)
            total = add(load(S, (f,), rows, 2), mul(a, uz_f, db=True, rows=2))
            uv, uv_f = load(F, (s, FV), rows), side(F, s, FV, rows, up)
            b = mul(load2(H, (s, 1, f), rows), uv_f)
            store(AB, (1,), rows, b)
            total = add(total, mul(uv, b, da=True, rows=2))
            if f == FX:
                total = add(total, load(L, (0,), rows, 2))
            store(F, (s + 1, f), rows, mixed(load(F, (s, f), rows, 2), total, 0.125))

        body(rows, up)

    def z_staples(s, f):
        def body(rows, up):
            shift = None if f == FX else up
            uf = load(F, (s, f), rows)
            b = mul(uf, side(F, s, FZ, rows, shift), rows=2)
            upper = mul(b, load2(H, (s, 0, f), rows), db=True, rows=2)
            lower = mul(uf, load(AB, (0,), rows), da=True, rows=2)
            below = load2(H, (s, 1, f), rows)
            v_upper = mul(load(AB, (1,), rows), uf, db=True, rows=2)
            v_lower = mul(mul(below, load(F, (s, FV), rows), da=True, rows=2), uf, rows=2)
            if f == FX:
                store(S, (FZ,), rows, add(upper, back_x(lower)))
                store(S, (FV,), rows, add(v_upper, back_x(v_lower)))
            else:
                store(L, (1,), up, lower)
                store(L, (2,), up, v_lower)
                store(S, (FZ,), rows, add(load(S, (FZ,), rows, 2), upper))
                store(S, (FV,), rows, add(load(S, (FV,), rows, 2), v_upper))

        each_half(body)
        if f == FY:
            unwrap(1)
            unwrap(2)

    def z_links(s, last):
        for part in (h, o):
            rows, _ = span(part)
            for f, k in ((FZ, 1), (FV, 2)):
                total = add(load(S, (f,), rows, 2), load(L, (k,), rows, 2))
                store(F, (s + 1, f), rows, mixed(load(F, (s, f), rows, 2), total, 0.125))
                if last:
                    onward(s + 1, f, part, rows)
        wrap(F, s + 1, FZ)
        wrap(F, s + 1, FV)

    for copy in near[2:]:
        copy.wait()
    other = pl.ds(pl.multiple_of(o * half, half), half)
    arrived(F.at[0, 0:3, :, :, :, other], r_own)
    wrap(F, 0, FX)
    wrap(F, 0, FZ)
    in_plane(0)
    for k in range(2):
        arrived(F.at[0, FV, :, 0:2, :, halves[k]], r_v + k)

    def complete(rows, up):
        store(F, (0, FV), rows, load2(F, (0, FV), rows))

    each_half(complete)
    wrap(F, 0, FV)

    r_next = new_recv(10)
    r_tb, r_thb = new_recv(), new_recv()
    beside = [{"ta": wrapped(j + h + ta - 1, ta), "gy": o}, {"ta": wrapped(j + h, ta), "gy": o}]
    inner = pl.ds(half, half)

    def onward(s, f, k, rows):
        to = {"ta": jnp.where(k == 0, beside[0]["ta"], beside[1]["ta"]), "gy": o}
        remote(
            F.at[s, f, :, 0:2, :, rows], UP.at[k, f, :, :, :, inner], r_next + 5 * k + f, **to
        )

    def entries():
        return [(part, a, b) for part in range(2) for a in range(2) for b in range(3)]

    def onward_row(s, k):
        row = full - 1 if k == 0 else half - 1
        for c, (part, a, b) in enumerate(entries()):
            YP[k, pl.ds(c, 1), :] = F[s, FY, part, a, b, pl.ds(row, 1), :]
        remote(YP.at[k, 0:12], YQ.at[k, 0:12], r_next + 5 * k + 4, **beside[k])

    r_now = {FX: r_x, FY: r_y}
    for s in range(STEPS):
        last = s == STEPS - 1
        r_then = {f: new_recv(2) for f in (FX, FY)} if not last else {}
        for f in (FX, FY):
            (hear_z if f == FX else hear_x)()
            for k in (h, o):
                rows, up = span(k)
                arrived(H.at[s, :, f, :, :, :, rows], r_now[f] + k)
                across(s, f, rows, up)
                if last:
                    onward(s + 1, f, k, rows)
                else:
                    out = F.at[s + 1, f, :, 0:2, :, rows]
                    for side_k, to in ((0, zm), (1, zp)):
                        remote(
                            out, H.at[s + 1, side_k, f, :, :, :, rows], r_then[f] + k, gz=to
                        )
            if f == FX:
                wrap(F, s + 1, FX)
            else:
                if last:
                    for k in range(2):
                        onward_row(s + 1, k)
            z_staples(s, f)
        r_now = r_then
        if s == 0:
            arrived(T.at[:, :, :, other], r_ownt)
            wrap(T)
            remote(T.at[:, 0:2, :, 0:full], TB.at[:, :, :, 0:full], r_tb, **beside[1])
        if s == STEPS - 2:
            @pl.when(h == 1)
            def _():
                for side_k, to in ((0, zm), (1, zp)):
                    for t in range(2):
                        remote(
                            plane(None, t), THB.at[side_k], r_thb, cores=(1,),
                            ta=wrapped(j + t, ta), gz=to, gy=1 - t,
                        )

            for t in range(2):
                remote(plane(None, t), two(TH, 1), r_t + h, gz=zp, gy=t)
        z_links(s, last)
        if not last:
            in_plane(s + 1)

    n = STEPS
    r0, r1 = halves
    before1 = pl.ds(half - 1, half)

    def lower_y(rows, up):
        store(M, (3,), up, mul(load(F, (n, FY), rows), load(T, (), rows), da=True, rows=2))

    each_half(lower_y)
    M[3, :, :, :, pl.ds(0, 1)] = M[3, :, :, :, pl.ds(full, 1)]
    t = load(T, (), r0)
    ux, uy = load(F, (n, FX), r0), load(F, (n, FY), r0)
    store(M, (0,), r0, mul(ux, ahead_x(t), rows=2))
    store(M, (1,), r0, mul(ux, t, da=True, rows=2))
    store(M, (2,), r0, mul(uy, load(T, (), pl.ds(1, half)), rows=2))

    arrived(TB.at[:, :, :, 0:full], r_tb)
    wrap(TB)
    t = load2(TB, (), r1)
    ux = load(F, (n, FX), r1)
    store(Q, (0,), r0, mul(ahead_x(t), ux, db=True))
    store(Q, (1,), r0, mul(t, ux))
    store(Q, (2,), r0, mul(load2(TB, (), pl.ds(half + 1, half)), load(F, (n, FY), r1), db=True))
    store(Q, (3,), r0, mul(load2(TB, (), before1), load(F, (n, FY), before1)))

    def came(k, f):
        arrived(UP.at[k, f, :, :, :, inner], r_next + 5 * k + f)

    def row_came(k):
        arrived(YQ.at[k, 0:12], r_next + 5 * k + 4)
        for c, (part, a, b) in enumerate(entries()):
            UP[k, FY, part, a, b, pl.ds(half - 1, 1), :] = YQ[k, pl.ds(c, 1), :]

    def first_half(part):
        if part == 0:
            came(0, FX)
            came(0, FY)
            row_came(0)
            ux = load2(UP, (0, FX), inner)
            total = add(
                mul(load(M, (0,), r0, 2), ux, db=True, rows=2),
                back_x(mul(load(M, (1,), r0, 2), ux, rows=2)),
                mul(load(M, (2,), r0, 2), load2(UP, (0, FY), inner), db=True, rows=2),
                mul(load(M, (3,), r0, 2), load2(UP, (0, FY), before1), rows=2),
            )
            store(S, (0,), r0, total)
            for k in range(2):
                arrived(TH.at[:, :, :, :, halves[k]], r_t + k)
            store(M, (4,), r0, mul(load(F, (n, FZ), r0), load2(TH, (0,), r0), rows=2))
            store(M, (5,), r0, mul(load(F, (n, FV), r0), load2(TH, (1,), r0), da=True, rows=2))
        else:
            came(0, FZ)
            came(0, FV)
            total = add(
                load(S, (0,), r0, 2),
                mul(load(M, (4,), r0, 2), load2(UP, (0, FZ), inner), db=True, rows=2),
                mul(load(M, (5,), r0, 2), load2(UP, (0, FV), inner), rows=2),
            )
            smoothed(0, load(T, (), r0, 2), total)

    def second_half(part):
        if part == 0:
            came(1, FX)
            came(1, FY)
            row_came(1)
            ux = load2(UP, (1, FX), inner)
            total = add(
                mul(ux, load(Q, (0,), r0), rows=2),
                back_x(mul(ux, load(Q, (1,), r0), da=True, rows=2)),
                mul(load2(UP, (1, FY), inner), load(Q, (2,), r0), rows=2),
                mul(load2(UP, (1, FY), before1), load(Q, (3,), r0), da=True, rows=2),
            )
            store(S, (0,), r1, total)
            arrived(THB, r_thb)
            store(Q, (4,), r0, mul(load2(THB, (0,), r0), load(F, (n, FZ), r1), db=True))
            store(Q, (5,), r0, mul(load2(THB, (1,), r0), load(F, (n, FV), r1)))
        else:
            came(1, FZ)
            came(1, FV)
            total = add(
                load(S, (0,), r1, 2),
                mul(load2(UP, (1, FZ), inner), load(Q, (4,), r0), rows=2),
                mul(load2(UP, (1, FV), inner), load(Q, (5,), r0), da=True, rows=2),
            )
            smoothed(1, load(TB, (), r1, 2), total)

    def smoothed(k, link, total):
        done = mixed(link, total, 0.5 / 6.0)
        for c, (part, a, b) in enumerate(entries()):
            sm[pl.ds(k * half * 16 + c, half, 16), :] = done[part][a][b]

    lanes = sm.shape[-1]
    sm3, ar3 = sm.reshape(full, 16, lanes), ar.reshape(own * nd, 16, lanes)
    ar4 = ar.reshape(own, nd, 16, lanes)
    r_row, r_out = new_recv(), new_recv()
    away = sorted(range(1, ta), key=lambda k: -min(k, ta - k))
    home = pl.ds(j * own, own)

    def slice_of(jd):
        return jnp.where(jd * own < half, me, wrapped(me + nd - 1, nd))

    def to_products(k, c):
        here, part = wrapped(j, ta // 2), ta // 2
        for i in range(part):
            jd = k * part + wrapped(here + i, part)

            def go(jd=jd):
                remote(
                    sm3.at[pl.ds(jd * own, own), 0:12], ar4.at[:, slice_of(jd), 0:12], r_row,
                    cores=(c,), ta=jd, gy=1,
                )

            if c == 0:
                go()
            else:
                pl.when(jd != j)(go)

    @pl.when(h == 0)
    def _():
        first_half(0)
        first_half(1)
        to_products(0, 0)
        second_half(0)
        second_half(1)
        to_products(1, 0)

    @pl.when(h == 1)
    def _():
        second_half(0)
        second_half(1)
        to_products(1, 1)
        first_half(0)
        first_half(1)
        to_products(0, 1)

    rows_sent[1] -= own * 12

    def slices(start, rows):
        at = lambda c: ar[pl.ds(start + c, rows, 32), :]
        return third_row(
            tuple([[at(part * 6 + a * 3 + b) for b in range(3)] for a in range(2)] for part in range(2))
        )

    def pick(first, rows):
        vs = [tree[pl.ds(c * full + first, rows, 2), :] for c in range(18)]
        return tuple(
            [[vs[part * 9 + a * 3 + b] for b in range(3)] for a in range(3)] for part in range(2)
        )

    @pl.when(h == 1)
    def _():
        for r in range(own):
            ar3[r * nd + slice_of(j)] = sm3[j * own + r]
        arrived(ar4.at[:, 0 : nd - 1, 0:12], r_row)
        rows = own * nd // 2
        lhs, rhs = slices(0, rows), slices(16, rows)
        while rows > own:
            flat = [v for part in mul(lhs, rhs) for line in part for v in line]
            for c, v in enumerate(flat):
                tree[pl.ds(c * full, rows), :] = v
            rows //= 2
            lhs, rhs = pick(0, rows), pick(1, rows)
        re = im = None
        for a in range(3):
            for b in range(3):
                lr, li, rr, ri = lhs[0][a][b], lhs[1][a][b], rhs[0][b][a], rhs[1][b][a]
                t_re, t_im = lr * rr - li * ri, lr * ri + li * rr
                re = t_re if re is None else re + t_re
                im = t_im if im is None else im + t_im
        for r in range(own):
            pb[r, 0:1, :] = re[r : r + 1] / 3.0
            pb[r, 1:2, :] = im[r : r + 1] / 3.0
        for k in away:
            for c in range(2):
                remote(pb, bc.at[home], r_out, cores=(1,), ta=wrapped(j + k, ta), gy=c)
        remote(pb, bc.at[home], r_out, cores=(1,), gy=0)
        bc[home] = pb[...]
        arrived(bc.at[pl.ds(0, full - own)], r_out)

    @pl.when(h == 0)
    def _():
        arrived(bc, r_out)

    sums = jnp.sum(bc[...], axis=0)
    zs[z] = sums
    r_sum = new_recv()
    for k in sorted(range(1, gz), key=lambda k: min(k, gz - k)):
        remote(zs.at[z], zs.at[z], r_sum, gz=wrapped(z + k, gz))
    for k in range(half):
        pol[:, 0, k, :] = bc[h * half + k]
    arrived(zs.at[pl.ds(0, gz - 1)], r_sum)
    totals = jnp.sum(zs[...], axis=0)
    sites = float(full * gz * sp.shape[-1])
    totals = jnp.sum(totals, axis=1, keepdims=True) / sites
    lane = lax.broadcasted_iota(jnp.int32, (1, lanes), 1)
    mean[...] = jnp.where(lane == 0, totals[0:1], totals[1:2])

    def all_sent(c):
        lines = F.reshape(math.prod(F.shape[:-1]), lanes).at[pl.ds(0, rows_sent[c])]
        pltpu.make_async_copy(lines, lines, send_sem).wait()

    for c in range(2):
        pl.when(h == c)(functools.partial(all_sent, c))


def write_out(polyakov, means, polyakov_out, means_out):
    polyakov_out[...] = polyakov[...]
    means_out[...] = means[0, 0:2]


def solution(mesh):
    ta, gz = mesh.shape["ta"], mesh.shape["gz"]

    def body(sp, tl):
        half, lanes = sp.shape[-2:]
        full = 2 * half
        pad = full + 8
        own = full // ta

        def vmem(*dims):
            return pltpu.VMEM((*dims, lanes), F32)

        n_recv = 2 + 2 + 2 + 2 + 2 + 12 + 4 * (STEPS - 1) + 3
        polyakov, means = pl.pallas_call(
            functools.partial(kernel, ta, gz, half),
            out_shape=(
                jax.ShapeDtypeStruct((2, 1, half, lanes), F32),
                jax.ShapeDtypeStruct((1, lanes), F32),
            ),
            in_specs=[pl.BlockSpec(memory_space=pltpu.HBM)] * 2,
            out_specs=(pl.BlockSpec(memory_space=pltpu.VMEM),) * 2,
            scratch_shapes=[
                pltpu.VMEM(sp.shape, F32),
                pltpu.VMEM(tl.shape, F32),
                vmem(STEPS + 1, 4, 2, 3, 3, pad),
                vmem(2, 3, 3, pad),
                vmem(STEPS, 2, 2, 2, 2, 3, full),
                vmem(2, 2, 2, 3, full),
                vmem(2, 4, 2, 2, 3, full),
                vmem(2, 2, 3, pad),
                vmem(2, 2, 2, 3, half),
                vmem(2, 16),
                vmem(2, 16),
                vmem(6, 2, 3, 3, half),
                vmem(4, 2, 2, 3, full),
                vmem(3, 2, 2, 3, pad),
                vmem(2, 2, 3, 3, full),
                vmem(6, 2, 2, 3, pad),
                vmem(full * 16),
                vmem(2 * full * 16),
                vmem(18 * full),
                vmem(own, 2),
                vmem(full, 2),
                vmem(gz, 2),
                pltpu.SemaphoreType.DMA((4,)),
                pltpu.SemaphoreType.DMA,
                pltpu.SemaphoreType.DMA((n_recv,)),
                pltpu.SemaphoreType.REGULAR((max(ta // 2, 1),)),
                pltpu.SemaphoreType.REGULAR((max(gz // 2, 1),)),
            ],
            compiler_params=pltpu.CompilerParams(
                collective_id=0, has_side_effects=True, vmem_limit_bytes=56_450_000
            ),
        )(sp, tl)
        return pl.pallas_call(
            write_out,
            out_shape=(
                jax.ShapeDtypeStruct(polyakov.shape, F32),
                jax.ShapeDtypeStruct((2,), F32),
            ),
            in_specs=[pl.BlockSpec(memory_space=pltpu.VMEM)] * 2,
            out_specs=(pl.BlockSpec(memory_space=pltpu.VMEM),) * 2,
            compiler_params=pltpu.CompilerParams(vmem_limit_bytes=1024 * 1024),
        )(polyakov, means)

    return jax.shard_map(
        body,
        mesh=mesh,
        in_specs=(
            P("cfg", None, None, None, "ta", "gz", "gy", None),
            P("cfg", None, None, "ta", "gz", "gy", None),
        ),
        out_specs=(P("cfg", "gz", "gy", None), P("cfg")),
        check_vma=False,
    )
```

```python
import functools
import math

import jax
import jax.numpy as jnp
from jax import lax
from jax.experimental import pallas as pl
from jax.experimental.pallas import tpu as pltpu
from jax.sharding import PartitionSpec as P

MESH = pl.DeviceIdType.MESH
F32 = jnp.float32
STEPS = 3
FLOOR = 0.25
FX, FY, FZ, FV = 0, 1, 2, 3


def third_row(m):
    (a_re, b_re), (a_im, b_im) = m[0][:2], m[1][:2]
    re, im = [], []
    for k in range(3):
        p, q = (k + 1) % 3, (k + 2) % 3
        re.append(
            a_re[p] * b_re[q] - a_im[p] * b_im[q] - (a_re[q] * b_re[p] - a_im[q] * b_im[p])
        )
        im.append(
            (a_re[q] * b_im[p] + a_im[q] * b_re[p]) - (a_re[p] * b_im[q] + a_im[p] * b_re[q])
        )
    return [m[0][0], m[0][1], re], [m[1][0], m[1][1], im]


def load(ref, lead, rows, count=3):
    return tuple(
        [[ref[(*lead, part, i, j, rows)] for j in range(3)] for i in range(count)]
        for part in range(2)
    )


def load2(ref, lead, rows):
    return third_row(load(ref, lead, rows, 2))


def store(ref, lead, rows, m):
    for part in range(2):
        for i, row in enumerate(m[part]):
            for j, v in enumerate(row):
                ref[(*lead, part, i, j, rows)] = v


def mapped(fn, *ms):
    return tuple(
        [[fn(*vs) for vs in zip(*rows)] for rows in zip(*[m[part] for m in ms])]
        for part in range(2)
    )


def add(*ms):
    return mapped(lambda *vs: functools.reduce(lambda a, b: a + b, vs), *ms)


def ahead_x(m):
    return mapped(lambda v: pltpu.roll(v, v.shape[-1] - 1, 1), m)


def back_x(m):
    return mapped(lambda v: pltpu.roll(v, 1, 1), m)


def mul(a, b, da=False, db=False, rows=3):
    out_re, out_im = [], []
    for i in range(rows):
        row_re, row_im = [], []
        for k in range(3):
            re = im = None
            for j in range(3):
                ar, ai = (a[0][j][i], a[1][j][i]) if da else (a[0][i][j], a[1][i][j])
                br, bi = (b[0][k][j], b[1][k][j]) if db else (b[0][j][k], b[1][j][k])
                rr, ii, ri, ir = ar * br, ai * bi, ar * bi, ai * br
                tr = rr + ii if da != db else rr - ii
                if da and db:
                    ti = -(ri + ir)
                elif da:
                    ti = ri - ir
                elif db:
                    ti = ir - ri
                else:
                    ti = ri + ir
                re = tr if re is None else re + tr
                im = ti if im is None else im + ti
            row_re.append(re)
            row_im.append(im)
        out_re.append(row_re)
        out_im.append(row_im)
    return out_re, out_im


def normalized(re, im):
    weight = sum(v * v for v in re) + sum(v * v for v in im)
    scale = lax.rsqrt(jnp.maximum(weight, FLOOR))
    return [v * scale for v in re], [v * scale for v in im]


def project(re, im):
    u_re, u_im = normalized(re[0], im[0])
    in_re = sum(u_re[j] * re[1][j] + u_im[j] * im[1][j] for j in range(3))
    in_im = sum(u_re[j] * im[1][j] - u_im[j] * re[1][j] for j in range(3))
    w_re = [re[1][j] - (in_re * u_re[j] - in_im * u_im[j]) for j in range(3)]
    w_im = [im[1][j] - (in_re * u_im[j] + in_im * u_re[j]) for j in range(3)]
    v_re, v_im = normalized(w_re, w_im)
    return third_row(([u_re, v_re], [u_im, v_im]))


def mixed(link, staples, weight):
    re = [[0.5 * link[0][i][j] + weight * staples[0][i][j] for j in range(3)] for i in range(2)]
    im = [[0.5 * link[1][i][j] + weight * staples[1][i][j] for j in range(3)] for i in range(2)]
    return project(re, im)


def kernel(
    ta, gz, half,
    sp, tl, pol, mean,
    SP, TL, F, T, H, TH, UP, TB, THB, YP, YQ, Q, S, L, AB, M, sm, ar, tree, pb, bc, zs,
    local_sem, send_sem, recv_sem, ready_x, ready_z,
):
    def wrapped(v, n):
        return jnp.where(v >= n, v - n, v)

    j, z, h = lax.axis_index("ta"), lax.axis_index("gz"), lax.axis_index("gy")
    o = 1 - h
    zp, zm = wrapped(z + 1, gz), wrapped(z + gz - 1, gz)
    full = 2 * half
    nd = 2 * ta
    own = full // ta
    me = 2 * j + h
    mine = pl.ds(pl.multiple_of(h * half, half), half)
    halves = [pl.ds(k * half, half) for k in range(2)]

    rows_sent = [0, 0]
    n_recv = [0]

    def remote(src, dst, recv_index, cores=(0, 1), **where):
        pltpu.make_async_remote_copy(
            src_ref=src, dst_ref=dst, send_sem=send_sem, recv_sem=recv_sem.at[recv_index],
            device_id=where, device_id_type=MESH,
        ).start()
        for c in cores:
            rows_sent[c] += math.prod(src.shape[:-1])

    def arrived(dst, recv_index):
        pltpu.make_async_remote_copy(
            src_ref=dst, dst_ref=dst, send_sem=send_sem, recv_sem=recv_sem.at[recv_index],
            device_id={"gy": o}, device_id_type=MESH,
        ).wait_recv()

    def new_recv(n=1):
        k = n_recv[0]
        n_recv[0] += n
        return k

    near = [
        pltpu.make_async_copy(sp, SP, local_sem.at[2]),
        pltpu.make_async_copy(tl, TL, local_sem.at[3]),
        pltpu.make_async_copy(sp.at[:, :, :, :, h, 0], F.at[0, 0:3, :, :, :, mine], local_sem.at[0]),
        pltpu.make_async_copy(tl.at[:, :, :, h, 0], T.at[:, :, :, mine], local_sem.at[1]),
    ]
    for copy in near:
        copy.start()

    barrier = pltpu.get_barrier_semaphore()
    around = sorted({(0, 1 % gz), (0, gz - 1), (1 % ta, 0), (ta - 1, 0)} - {(0, 0)})

    def place(dx, dz):
        return {"ta": wrapped(j + dx, ta), "gz": wrapped(z + dz, gz)}

    def signal(sem, **where):
        pl.semaphore_signal(sem, inc=1, device_id=where, device_id_type=MESH)

    signal(barrier, gy=o)
    for dx, dz in around:
        for c in range(2):
            signal(barrier, **place(dx, dz), gy=c)
    near[0].wait()
    pl.semaphore_wait(barrier, 1 + 2 * len(around))

    def relay(sem, axis, here, size):
        reach = [1]
        waiting = [None]

        def go():
            if waiting[0] is not None:
                pl.semaphore_wait(sem.at[waiting[0][0]], waiting[0][1])
                waiting[0] = None
            if 2 * reach[0] <= size:
                n = reach[0]
                sides = sorted({n % size, (size - n) % size} - {0})
                if n < size // 2:
                    index = n.bit_length() - 1
                    for k in sides:
                        signal(sem.at[index], **{axis: wrapped(here + k, size)})
                    waiting[0] = (index, len(sides))
                    reach[0] = 2 * n

        return go

    hear_x = relay(ready_x, "ta", j, ta)
    hear_z = relay(ready_z, "gz", z, gz)

    r_v, r_x, r_y, r_t = new_recv(2), new_recv(2), new_recv(2), new_recv(2)
    r_own, r_ownt = new_recv(), new_recv()

    def plane(f, t):
        return SP.at[f, :, 0:2, :, t, 0] if f is not None else TL.at[:, 0:2, :, t, 0]

    def two(ref, *lead):
        return ref.at[(*lead, slice(None), slice(0, 2), slice(None), mine)]

    for t in range(2):
        remote(plane(FZ, t), two(F, 0, FV), r_v + h, gz=zp, gy=t)
        remote(plane(FX, t), two(H, 0, 0, FX), r_x + h, gz=zm, gy=t)
        remote(plane(FX, t), two(H, 0, 1, FX), r_x + h, gz=zp, gy=t)
        if t == 0:
            remote(SP.at[:, :, :, :, o, 0], F.at[0, 0:3, :, :, :, mine], r_own, gy=o)
    for t in range(2):
        remote(plane(FY, t), two(H, 0, 0, FY), r_y + h, gz=zm, gy=t)
        remote(plane(FY, t), two(H, 0, 1, FY), r_y + h, gz=zp, gy=t)
    near[1].wait()
    remote(TL.at[:, :, :, o, 0], T.at[:, :, :, mine], r_ownt, gy=o)
    for t in range(2):
        remote(plane(None, t), two(TH, 0), r_t + h, gz=zm, gy=t)
    hear_x()
    hear_z()

    def each_half(body):
        def run(k, carry):
            r0 = pl.multiple_of(k * half, half)
            body(pl.ds(r0, half), pl.ds(r0 + 1, half))
            return carry

        lax.fori_loop(0, 2, run, 0)

    def wrap(ref, *lead):
        ref[(*lead, slice(None), slice(None), slice(None), pl.ds(full, 1))] = ref[
            (*lead, slice(None), slice(None), slice(None), pl.ds(0, 1))
        ]

    def unwrap(k):
        L[k, :, :, :, pl.ds(0, 1)] = L[k, :, :, :, pl.ds(full, 1)]

    def in_plane(s):
        def body(rows, up):
            ux, uy = load(F, (s, FX), rows), load(F, (s, FY), rows)
            uy_x, ux_y = ahead_x(uy), load(F, (s, FX), up)
            c, d = mul(ux, uy_x), mul(uy, ux_y)
            store(S, (FX,), rows, mul(d, uy_x, db=True, rows=2))
            store(L, (0,), up, mul(uy, c, da=True, rows=2))
            store(
                S, (FY,), rows,
                add(mul(c, ux_y, db=True, rows=2), back_x(mul(ux, d, da=True, rows=2))),
            )

        each_half(body)
        unwrap(0)

    def side(ref, s, f, rows, up):
        return ahead_x(load(ref, (s, f), rows)) if up is None else load(ref, (s, f), up)

    def span(k):
        r0 = pl.multiple_of(k * half, half)
        return pl.ds(r0, half), pl.ds(r0 + 1, half)

    def across(s, f, rows, up):
        def body(rows, up):
            up = None if f == FX else up
            uz, uz_f = load(F, (s, FZ), rows), side(F, s, FZ, rows, up)
            a = mul(uz, load2(H, (s, 0, f), rows))
            store(AB, (0,), rows, a)
            total = add(load(S, (f,), rows, 2), mul(a, uz_f, db=True, rows=2))
            uv, uv_f = load(F, (s, FV), rows), side(F, s, FV, rows, up)
            b = mul(load2(H, (s, 1, f), rows), uv_f)
            store(AB, (1,), rows, b)
            total = add(total, mul(uv, b, da=True, rows=2))
            if f == FX:
                total = add(total, load(L, (0,), rows, 2))
            store(F, (s + 1, f), rows, mixed(load(F, (s, f), rows, 2), total, 0.125))

        body(rows, up)

    def z_staples(s, f):
        def body(rows, up):
            shift = None if f == FX else up
            uf = load(F, (s, f), rows)
            b = mul(uf, side(F, s, FZ, rows, shift), rows=2)
            upper = mul(b, load2(H, (s, 0, f), rows), db=True, rows=2)
            lower = mul(uf, load(AB, (0,), rows), da=True, rows=2)
            below = load2(H, (s, 1, f), rows)
            v_upper = mul(load(AB, (1,), rows), uf, db=True, rows=2)
            v_lower = mul(mul(below, load(F, (s, FV), rows), da=True, rows=2), uf, rows=2)
            if f == FX:
                store(S, (FZ,), rows, add(upper, back_x(lower)))
                store(S, (FV,), rows, add(v_upper, back_x(v_lower)))
            else:
                store(L, (1,), up, lower)
                store(L, (2,), up, v_lower)
                store(S, (FZ,), rows, add(load(S, (FZ,), rows, 2), upper))
                store(S, (FV,), rows, add(load(S, (FV,), rows, 2), v_upper))

        each_half(body)
        if f == FY:
            unwrap(1)
            unwrap(2)

    def z_links(s, last):
        for part in (h, o):
            rows, _ = span(part)
            for f, k in ((FZ, 1), (FV, 2)):
                total = add(load(S, (f,), rows, 2), load(L, (k,), rows, 2))
                store(F, (s + 1, f), rows, mixed(load(F, (s, f), rows, 2), total, 0.125))
                if last:
                    onward(s + 1, f, part, rows)
        wrap(F, s + 1, FZ)
        wrap(F, s + 1, FV)

    for copy in near[2:]:
        copy.wait()
    other = pl.ds(pl.multiple_of(o * half, half), half)
    arrived(F.at[0, 0:3, :, :, :, other], r_own)
    wrap(F, 0, FX)
    wrap(F, 0, FZ)
    in_plane(0)
    for k in range(2):
        arrived(F.at[0, FV, :, 0:2, :, halves[k]], r_v + k)

    def complete(rows, up):
        store(F, (0, FV), rows, load2(F, (0, FV), rows))

    each_half(complete)
    wrap(F, 0, FV)

    r_next = new_recv(10)
    r_tb, r_thb = new_recv(), new_recv()
    beside = [{"ta": wrapped(j + h + ta - 1, ta), "gy": o}, {"ta": wrapped(j + h, ta), "gy": o}]
    inner = pl.ds(half, half)

    def onward(s, f, k, rows):
        to = {"ta": jnp.where(k == 0, beside[0]["ta"], beside[1]["ta"]), "gy": o}
        remote(
            F.at[s, f, :, 0:2, :, rows], UP.at[k, f, :, :, :, inner], r_next + 5 * k + f, **to
        )

    def entries():
        return [(part, a, b) for part in range(2) for a in range(2) for b in range(3)]

    def onward_row(s, k):
        row = full - 1 if k == 0 else half - 1
        for c, (part, a, b) in enumerate(entries()):
            YP[k, pl.ds(c, 1), :] = F[s, FY, part, a, b, pl.ds(row, 1), :]
        remote(YP.at[k, 0:12], YQ.at[k, 0:12], r_next + 5 * k + 4, **beside[k])

    r_now = {FX: r_x, FY: r_y}
    for s in range(STEPS):
        last = s == STEPS - 1
        r_then = {f: new_recv(2) for f in (FX, FY)} if not last else {}
        for f in (FX, FY):
            (hear_z if f == FX else hear_x)()
            for k in (h, o):
                rows, up = span(k)
                arrived(H.at[s, :, f, :, :, :, rows], r_now[f] + k)
                across(s, f, rows, up)
                if last:
                    onward(s + 1, f, k, rows)
                else:
                    out = F.at[s + 1, f, :, 0:2, :, rows]
                    for side_k, to in ((0, zm), (1, zp)):
                        remote(
                            out, H.at[s + 1, side_k, f, :, :, :, rows], r_then[f] + k, gz=to
                        )
            if f == FX:
                wrap(F, s + 1, FX)
            else:
                if last:
                    for k in range(2):
                        onward_row(s + 1, k)
            z_staples(s, f)
        r_now = r_then
        if s == 0:
            arrived(T.at[:, :, :, other], r_ownt)
            wrap(T)
            remote(T.at[:, 0:2, :, 0:full], TB.at[:, :, :, 0:full], r_tb, **beside[1])
        if s == STEPS - 2:
            @pl.when(h == 1)
            def _():
                for side_k, to in ((0, zm), (1, zp)):
                    for t in range(2):
                        remote(
                            plane(None, t), THB.at[side_k], r_thb, cores=(1,),
                            ta=wrapped(j + t, ta), gz=to, gy=1 - t,
                        )

            for t in range(2):
                remote(plane(None, t), two(TH, 1), r_t + h, gz=zp, gy=t)
        z_links(s, last)
        if not last:
            in_plane(s + 1)

    n = STEPS
    r0, r1 = halves
    before1 = pl.ds(half - 1, half)

    def lower_y(rows, up):
        store(M, (3,), up, mul(load(F, (n, FY), rows), load(T, (), rows), da=True, rows=2))

    each_half(lower_y)
    M[3, :, :, :, pl.ds(0, 1)] = M[3, :, :, :, pl.ds(full, 1)]
    t = load(T, (), r0)
    ux, uy = load(F, (n, FX), r0), load(F, (n, FY), r0)
    store(M, (0,), r0, mul(ux, ahead_x(t), rows=2))
    store(M, (1,), r0, mul(ux, t, da=True, rows=2))
    store(M, (2,), r0, mul(uy, load(T, (), pl.ds(1, half)), rows=2))

    arrived(TB.at[:, :, :, 0:full], r_tb)
    wrap(TB)
    t = load2(TB, (), r1)
    ux = load(F, (n, FX), r1)
    store(Q, (0,), r0, mul(ahead_x(t), ux, db=True))
    store(Q, (1,), r0, mul(t, ux))
    store(Q, (2,), r0, mul(load2(TB, (), pl.ds(half + 1, half)), load(F, (n, FY), r1), db=True))
    store(Q, (3,), r0, mul(load2(TB, (), before1), load(F, (n, FY), before1)))

    def came(k, f):
        arrived(UP.at[k, f, :, :, :, inner], r_next + 5 * k + f)

    def row_came(k):
        arrived(YQ.at[k, 0:12], r_next + 5 * k + 4)
        for c, (part, a, b) in enumerate(entries()):
            UP[k, FY, part, a, b, pl.ds(half - 1, 1), :] = YQ[k, pl.ds(c, 1), :]

    def first_half(part):
        if part == 0:
            came(0, FX)
            came(0, FY)
            row_came(0)
            ux = load2(UP, (0, FX), inner)
            total = add(
                mul(load(M, (0,), r0, 2), ux, db=True, rows=2),
                back_x(mul(load(M, (1,), r0, 2), ux, rows=2)),
                mul(load(M, (2,), r0, 2), load2(UP, (0, FY), inner), db=True, rows=2),
                mul(load(M, (3,), r0, 2), load2(UP, (0, FY), before1), rows=2),
            )
            store(S, (0,), r0, total)
            for k in range(2):
                arrived(TH.at[:, :, :, :, halves[k]], r_t + k)
            store(M, (4,), r0, mul(load(F, (n, FZ), r0), load2(TH, (0,), r0), rows=2))
            store(M, (5,), r0, mul(load(F, (n, FV), r0), load2(TH, (1,), r0), da=True, rows=2))
        else:
            came(0, FZ)
            came(0, FV)
            total = add(
                load(S, (0,), r0, 2),
                mul(load(M, (4,), r0, 2), load2(UP, (0, FZ), inner), db=True, rows=2),
                mul(load(M, (5,), r0, 2), load2(UP, (0, FV), inner), rows=2),
            )
            smoothed(0, load(T, (), r0, 2), total)

    def second_half(part):
        if part == 0:
            came(1, FX)
            came(1, FY)
            row_came(1)
            ux = load2(UP, (1, FX), inner)
            total = add(
                mul(ux, load(Q, (0,), r0), rows=2),
                back_x(mul(ux, load(Q, (1,), r0), da=True, rows=2)),
                mul(load2(UP, (1, FY), inner), load(Q, (2,), r0), rows=2),
                mul(load2(UP, (1, FY), before1), load(Q, (3,), r0), da=True, rows=2),
            )
            store(S, (0,), r1, total)
            arrived(THB, r_thb)
            store(Q, (4,), r0, mul(load2(THB, (0,), r0), load(F, (n, FZ), r1), db=True))
            store(Q, (5,), r0, mul(load2(THB, (1,), r0), load(F, (n, FV), r1)))
        else:
            came(1, FZ)
            came(1, FV)
            total = add(
                load(S, (0,), r1, 2),
                mul(load2(UP, (1, FZ), inner), load(Q, (4,), r0), rows=2),
                mul(load2(UP, (1, FV), inner), load(Q, (5,), r0), da=True, rows=2),
            )
            smoothed(1, load(TB, (), r1, 2), total)

    def smoothed(k, link, total):
        done = mixed(link, total, 0.5 / 6.0)
        for c, (part, a, b) in enumerate(entries()):
            sm[pl.ds(k * half * 16 + c, half, 16), :] = done[part][a][b]

    lanes = sm.shape[-1]
    sm3, ar3 = sm.reshape(full, 16, lanes), ar.reshape(own * nd, 16, lanes)
    ar4 = ar.reshape(own, nd, 16, lanes)
    r_row, r_out = new_recv(), new_recv()
    away = sorted(range(1, ta), key=lambda k: -min(k, ta - k))
    home = pl.ds(j * own, own)

    def slice_of(jd):
        return jnp.where(jd * own < half, me, wrapped(me + nd - 1, nd))

    def to_products(k, c):
        here, part = wrapped(j, ta // 2), ta // 2
        for i in range(part):
            jd = k * part + wrapped(here + i, part)

            def go(jd=jd):
                remote(
                    sm3.at[pl.ds(jd * own, own), 0:12], ar4.at[:, slice_of(jd), 0:12], r_row,
                    cores=(c,), ta=jd, gy=1,
                )

            if c == 0:
                go()
            else:
                pl.when(jd != j)(go)

    @pl.when(h == 0)
    def _():
        first_half(0)
        first_half(1)
        to_products(0, 0)
        second_half(0)
        second_half(1)
        to_products(1, 0)

    @pl.when(h == 1)
    def _():
        second_half(0)
        second_half(1)
        to_products(1, 1)
        first_half(0)
        first_half(1)
        to_products(0, 1)

    rows_sent[1] -= own * 12

    def slices(start, rows):
        at = lambda c: ar[pl.ds(start + c, rows, 32), :]
        return third_row(
            tuple([[at(part * 6 + a * 3 + b) for b in range(3)] for a in range(2)] for part in range(2))
        )

    def pick(first, rows):
        vs = [tree[pl.ds(c * full + first, rows, 2), :] for c in range(18)]
        return tuple(
            [[vs[part * 9 + a * 3 + b] for b in range(3)] for a in range(3)] for part in range(2)
        )

    @pl.when(h == 1)
    def _():
        for r in range(own):
            ar3[r * nd + slice_of(j)] = sm3[j * own + r]
        arrived(ar4.at[:, 0 : nd - 1, 0:12], r_row)
        rows = own * nd // 2
        lhs, rhs = slices(0, rows), slices(16, rows)
        while rows > own:
            flat = [v for part in mul(lhs, rhs) for line in part for v in line]
            for c, v in enumerate(flat):
                tree[pl.ds(c * full, rows), :] = v
            rows //= 2
            lhs, rhs = pick(0, rows), pick(1, rows)
        re = im = None
        for a in range(3):
            for b in range(3):
                lr, li, rr, ri = lhs[0][a][b], lhs[1][a][b], rhs[0][b][a], rhs[1][b][a]
                t_re, t_im = lr * rr - li * ri, lr * ri + li * rr
                re = t_re if re is None else re + t_re
                im = t_im if im is None else im + t_im
        for r in range(own):
            pb[r, 0:1, :] = re[r : r + 1] / 3.0
            pb[r, 1:2, :] = im[r : r + 1] / 3.0
        for k in away:
            for c in range(2):
                remote(pb, bc.at[home], r_out, cores=(1,), ta=wrapped(j + k, ta), gy=c)
        remote(pb, bc.at[home], r_out, cores=(1,), gy=0)
        bc[home] = pb[...]
        arrived(bc.at[pl.ds(0, full - own)], r_out)

    @pl.when(h == 0)
    def _():
        arrived(bc, r_out)

    sums = jnp.sum(bc[...], axis=0)
    zs[z] = sums
    r_sum = new_recv()
    for k in sorted(range(1, gz), key=lambda k: min(k, gz - k)):
        remote(zs.at[z], zs.at[z], r_sum, gz=wrapped(z + k, gz))
    for k in range(half):
        pol[:, 0, k, :] = bc[h * half + k]
    arrived(zs.at[pl.ds(0, gz - 1)], r_sum)
    totals = jnp.sum(zs[...], axis=0)
    sites = float(full * gz * sp.shape[-1])
    totals = jnp.sum(totals, axis=1, keepdims=True) / sites
    lane = lax.broadcasted_iota(jnp.int32, (1, lanes), 1)
    mean[...] = jnp.where(lane == 0, totals[0:1], totals[1:2])

    def all_sent(c):
        lines = F.reshape(math.prod(F.shape[:-1]), lanes).at[pl.ds(0, rows_sent[c])]
        pltpu.make_async_copy(lines, lines, send_sem).wait()

    for c in range(2):
        pl.when(h == c)(functools.partial(all_sent, c))


def write_out(polyakov, means, polyakov_out, means_out):
    polyakov_out[...] = polyakov[...]
    means_out[...] = means[0, 0:2]


def solution(mesh):
    ta, gz = mesh.shape["ta"], mesh.shape["gz"]

    def body(sp, tl):
        half, lanes = sp.shape[-2:]
        full = 2 * half
        pad = full + 8
        own = full // ta

        def vmem(*dims):
            return pltpu.VMEM((*dims, lanes), F32)

        n_recv = 2 + 2 + 2 + 2 + 2 + 12 + 4 * (STEPS - 1) + 3
        polyakov, means = pl.pallas_call(
            functools.partial(kernel, ta, gz, half),
            out_shape=(
                jax.ShapeDtypeStruct((2, 1, half, lanes), F32),
                jax.ShapeDtypeStruct((1, lanes), F32),
            ),
            in_specs=[pl.BlockSpec(memory_space=pltpu.HBM)] * 2,
            out_specs=(pl.BlockSpec(memory_space=pltpu.VMEM),) * 2,
            scratch_shapes=[
                pltpu.VMEM(sp.shape, F32),
                pltpu.VMEM(tl.shape, F32),
                vmem(STEPS + 1, 4, 2, 3, 3, pad),
                vmem(2, 3, 3, pad),
                vmem(STEPS, 2, 2, 2, 2, 3, full),
                vmem(2, 2, 2, 3, full),
                vmem(2, 4, 2, 2, 3, full),
                vmem(2, 2, 3, pad),
                vmem(2, 2, 2, 3, half),
                vmem(2, 16),
                vmem(2, 16),
                vmem(6, 2, 3, 3, half),
                vmem(4, 2, 2, 3, full),
                vmem(3, 2, 2, 3, pad),
                vmem(2, 2, 3, 3, full),
                vmem(6, 2, 2, 3, pad),
                vmem(full * 16),
                vmem(2 * full * 16),
                vmem(18 * full),
                vmem(own, 2),
                vmem(full, 2),
                vmem(gz, 2),
                pltpu.SemaphoreType.DMA((4,)),
                pltpu.SemaphoreType.DMA,
                pltpu.SemaphoreType.DMA((n_recv,)),
                pltpu.SemaphoreType.REGULAR((max(ta // 2, 1),)),
                pltpu.SemaphoreType.REGULAR((max(gz // 2, 1),)),
            ],
            compiler_params=pltpu.CompilerParams(
                collective_id=0, has_side_effects=True, vmem_limit_bytes=56_450_000
            ),
        )(sp, tl)
        return pl.pallas_call(
            write_out,
            out_shape=(
                jax.ShapeDtypeStruct(polyakov.shape, F32),
                jax.ShapeDtypeStruct((2,), F32),
            ),
            in_specs=[pl.BlockSpec(memory_space=pltpu.VMEM)] * 2,
            out_specs=(pl.BlockSpec(memory_space=pltpu.VMEM),) * 2,
            compiler_params=pltpu.CompilerParams(vmem_limit_bytes=1024 * 1024),
        )(polyakov, means)

    return jax.shard_map(
        body,
        mesh=mesh,
        in_specs=(
            P("cfg", None, None, None, "ta", "gz", "gy", None),
            P("cfg", None, None, "ta", "gz", "gy", None),
        ),
        out_specs=(P("cfg", "gz", "gy", None), P("cfg")),
        check_vma=False,
    )
```
